32 devices in a mesh: fsdp: 16 (over z, y, core), tp: 2 (over x).
Axes of the slice: x: 2, y: 2, z: 4, core: 2. Of those that a mesh axis runs over, the one named last changes fastest.
Arguments:
- frames: bfloat16 [4096, 768], P('fsdp'), may hold values from -6 to 6
- cotangent: bfloat16 [4096, 768], P('fsdp'), may hold values from -6 to 6
- w_qkv: float32 [2, 768, 3, 768], P(None, 'fsdp', None, 'tp'), may hold values from -0.21875 to 0.21875
- w_out: float32 [2, 768, 768], P(None, 'tp', 'fsdp'), may hold values from -0.4375 to 0.4375
- w_up: float32 [2, 768, 3072], P(None, 'fsdp', 'tp'), may hold values from -0.21875 to 0.21875
- w_down: float32 [2, 3072, 768], P(None, 'tp', 'fsdp'), may hold values from -0.109375 to 0.109375
- b_qv: float32 [2, 2, 12, 64], P(None, None, 'tp', 'fsdp'), may hold values from -1.5 to 1.5
- b_up: float32 [2, 48, 64], P(None, 'tp', 'fsdp'), may hold values from -1.5 to 1.5
- vectors: float32 [2, 6, 768], P(None, None, 'fsdp'), may hold values from -0.6 to 1.5, as said below
- first_qkv: float32 [2, 768, 3, 768], P(None, 'fsdp', None, 'tp'), may hold values from -12 to 12
- first_out: float32 [2, 768, 768], P(None, 'tp', 'fsdp'), may hold values from -12 to 12
- first_up: float32 [2, 768, 3072], P(None, 'fsdp', 'tp'), may hold values from -12 to 12
- first_down: float32 [2, 3072, 768], P(None, 'tp', 'fsdp'), may hold values from -12 to 12
- first_bqv: float32 [2, 2, 12, 64], P(None, None, 'tp', 'fsdp'), may hold values from -12 to 12
- first_bup: float32 [2, 48, 64], P(None, 'tp', 'fsdp'), may hold values from -12 to 12
- first_vec: float32 [2, 6, 768], P(None, None, 'fsdp'), may hold values from -12 to 12
- second_qkv: float32 [2, 768, 3, 768], P(None, 'fsdp', None, 'tp'), may hold values from 0.4096 to 4.096
- second_out: float32 [2, 768, 768], P(None, 'tp', 'fsdp'), may hold values from 0.4096 to 4.096
- second_up: float32 [2, 768, 3072], P(None, 'fsdp', 'tp'), may hold values from 0.4096 to 4.096
- second_down: float32 [2, 3072, 768], P(None, 'tp', 'fsdp'), may hold values from 0.4096 to 4.096
- second_bqv: float32 [2, 2, 12, 64], P(None, None, 'tp', 'fsdp'), may hold values from 0.4096 to 4.096
- second_bup: float32 [2, 48, 64], P(None, 'tp', 'fsdp'), may hold values from 0.4096 to 4.096
- second_vec: float32 [2, 6, 768], P(None, None, 'fsdp'), may hold values from 0.4096 to 4.096
Outputs:
- output: bfloat16 [4096, 768], P('fsdp')
- grad_input: float32 [4096, 768], P('fsdp')
- grad_qkv: float32 [2, 768, 3, 768], P(None, 'fsdp', None, 'tp')
- grad_out: float32 [2, 768, 768], P(None, 'tp', 'fsdp')
- grad_up: float32 [2, 768, 3072], P(None, 'fsdp', 'tp')
- grad_down: float32 [2, 3072, 768], P(None, 'tp', 'fsdp')
- grad_bqv: float32 [2, 2, 12, 64], P(None, None, 'tp', 'fsdp')
- grad_bup: float32 [2, 48, 64], P(None, 'tp', 'fsdp')
- grad_vec: float32 [2, 6, 768], P(None, None, 'fsdp')
- next_qkv: float32 [2, 768, 3, 768], P(None, 'fsdp', None, 'tp')
- next_out: float32 [2, 768, 768], P(None, 'tp', 'fsdp')
- next_up: float32 [2, 768, 3072], P(None, 'fsdp', 'tp')
- next_down: float32 [2, 3072, 768], P(None, 'tp', 'fsdp')
- next_bqv: float32 [2, 2, 12, 64], P(None, None, 'tp', 'fsdp')
- next_bup: float32 [2, 48, 64], P(None, 'tp', 'fsdp')
- next_vec: float32 [2, 6, 768], P(None, None, 'fsdp')
- next_first_qkv: float32 [2, 768, 3, 768], P(None, 'fsdp', None, 'tp')
- next_first_out: float32 [2, 768, 768], P(None, 'tp', 'fsdp')
- next_first_up: float32 [2, 768, 3072], P(None, 'fsdp', 'tp')
- next_first_down: float32 [2, 3072, 768], P(None, 'tp', 'fsdp')
- next_first_bqv: float32 [2, 2, 12, 64], P(None, None, 'tp', 'fsdp')
- next_first_bup: float32 [2, 48, 64], P(None, 'tp', 'fsdp')
- next_first_vec: float32 [2, 6, 768], P(None, None, 'fsdp')
- next_second_qkv: float32 [2, 768, 3, 768], P(None, 'fsdp', None, 'tp')
- next_second_out: float32 [2, 768, 768], P(None, 'tp', 'fsdp')
- next_second_up: float32 [2, 768, 3072], P(None, 'fsdp', 'tp')
- next_second_down: float32 [2, 3072, 768], P(None, 'tp', 'fsdp')
- next_second_bqv: float32 [2, 2, 12, 64], P(None, None, 'tp', 'fsdp')
- next_second_bup: float32 [2, 48, 64], P(None, 'tp', 'fsdp')
- next_second_vec: float32 [2, 6, 768], P(None, None, 'fsdp')
The draws below stay inside these ranges and needn't reach their ends.
Inputs may be any that keep to these rules, and one draw needn't show every extreme that they name: `vectors`: rows 0 and 2 of each layer (norm gains) lie in 0.5 to 1.5, the other rows in -0.6 to 0.6.
All inputs are finite; a program needn't handle non-finite values.
Results may differ from the reference program's by a relative error of at most 0.017.
Values may be sent and summed in bfloat16 or wider, within the bound.
A program may use at most 128 MiB of HBM per device.

```python
import math
from functools import partial
import jax
import jax.numpy as jnp
from jax import lax

D = 768
H = 12
HD = 64
FF = 3072
SEQ = 256
LAYERS = 2
STEP = 3
TOKENS = 4096


def draw_vectors(key, part):
    key_gain = jax.random.fold_in(key, 11)
    key_shift = jax.random.fold_in(key, 23)
    gains = jax.random.uniform(key_gain, (LAYERS, 6, D), jnp.float32, 0.5, 1.5)
    shifts = jax.random.uniform(key_shift, (LAYERS, 6, D), jnp.float32, -0.6, 0.6)
    row_number = jnp.arange(6).reshape(1, 6, 1)
    picked = (row_number == 0) | (row_number == 2)
    return jnp.where(picked, gains, shifts)


def block_levels(rng, dims, cuts, low, high):
    def one(dim, blocks):
        draws = jax.random.uniform(jax.random.fold_in(jax.random.fold_in(rng, 6), dim), (blocks,), jnp.float32, low / len(cuts), high / len(cuts))
        return jnp.repeat(jnp.exp(draws), dims[dim] // blocks).reshape((-1,) + (1,) * (len(dims) - dim - 1))

    factor_of = one(*cuts[0])
    for cut in cuts[1:]:
        factor_of = factor_of * one(*cut)
    return factor_of


def noise(rng, extent, spread, bound, split=(), dtype=jnp.bfloat16):
    level = block_levels(rng, extent, split, -0.22, 0.18) if split else 1.0
    values = jax.random.normal(rng, extent, jnp.float32) * spread * level
    return jnp.minimum(jnp.maximum(values, -bound), bound).astype(dtype)


def setup_inputs(seed: int = 0) -> dict:
    splits = jax.random.split(jax.random.key(seed), 24)
    return {
        "frames": noise(splits[0], (TOKENS, D), 1.0, 6.0, ((0, 16),)),
        "cotangent": noise(splits[1], (TOKENS, D), 1.0, 6.0, ((0, 16),)),
        "w_qkv": noise(splits[2], (LAYERS, D, 3, D), D ** -0.5, 0.21875, ((1, 16), (3, 2)), jnp.float32),
        "w_out": noise(splits[3], (LAYERS, D, D), (D // 4) ** -0.5, 0.4375, ((1, 2), (2, 16)), jnp.float32),
        "w_up": noise(splits[4], (LAYERS, D, FF), D ** -0.5, 0.21875, ((1, 16), (2, 2)), jnp.float32),
        "w_down": noise(splits[5], (LAYERS, FF, D), FF ** -0.5, 0.109375, ((1, 2), (2, 16)), jnp.float32),
        "b_qv": noise(splits[6], (LAYERS, 2, H, HD), 0.3, 1.5, ((2, 2), (3, 16)), jnp.float32),
        "b_up": noise(splits[7], (LAYERS, FF // HD, HD), 0.3, 1.5, ((1, 2), (2, 16)), jnp.float32),
        "vectors": draw_vectors(jax.random.fold_in(splits[23], 71), 0),
        "first_qkv": noise(splits[9], (LAYERS, D, 3, D), (0.03 * TOKENS ** 0.5), 12.0, ((1, 16), (3, 2)), jnp.float32),
        "first_out": noise(splits[10], (LAYERS, D, D), (0.03 * TOKENS ** 0.5), 12.0, ((1, 2), (2, 16)), jnp.float32),
        "first_up": noise(splits[11], (LAYERS, D, FF), (0.03 * TOKENS ** 0.5), 12.0, ((1, 16), (2, 2)), jnp.float32),
        "first_down": noise(splits[12], (LAYERS, FF, D), (0.03 * TOKENS ** 0.5), 12.0, ((1, 2), (2, 16)), jnp.float32),
        "first_bqv": noise(splits[13], (LAYERS, 2, H, HD), (0.03 * TOKENS ** 0.5), 12.0, ((2, 2), (3, 16)), jnp.float32),
        "first_bup": noise(splits[14], (LAYERS, FF // HD, HD), (0.03 * TOKENS ** 0.5), 12.0, ((1, 2), (2, 16)), jnp.float32),
        "first_vec": noise(splits[15], (LAYERS, 6, D), (0.03 * TOKENS ** 0.5), 12.0, ((2, 16),), jnp.float32),
        "second_qkv": jnp.clip(jnp.exp(math.log(4.096) - 2.3025852 * jax.random.uniform(splits[16], (LAYERS, D, 3, D), jnp.float32) ** block_levels(splits[16], (LAYERS, D, 3, D), ((1, 16), (3, 2)), -0.2, 0.2)), 0.4096, 4.096),
        "second_out": jnp.clip(jnp.exp(math.log(4.096) - 2.3025852 * jax.random.uniform(splits[17], (LAYERS, D, D), jnp.float32) ** block_levels(splits[17], (LAYERS, D, D), ((1, 2), (2, 16)), -0.2, 0.2)), 0.4096, 4.096),
        "second_up": jnp.clip(jnp.exp(math.log(4.096) - 2.3025852 * jax.random.uniform(splits[18], (LAYERS, D, FF), jnp.float32) ** block_levels(splits[18], (LAYERS, D, FF), ((1, 16), (2, 2)), -0.2, 0.2)), 0.4096, 4.096),
        "second_down": jnp.clip(jnp.exp(math.log(4.096) - 2.3025852 * jax.random.uniform(splits[19], (LAYERS, FF, D), jnp.float32) ** block_levels(splits[19], (LAYERS, FF, D), ((1, 2), (2, 16)), -0.2, 0.2)), 0.4096, 4.096),
        "second_bqv": jnp.clip(jnp.exp(math.log(4.096) - 2.3025852 * jax.random.uniform(splits[20], (LAYERS, 2, H, HD), jnp.float32) ** block_levels(splits[20], (LAYERS, 2, H, HD), ((2, 2), (3, 16)), -0.2, 0.2)), 0.4096, 4.096),
        "second_bup": jnp.clip(jnp.exp(math.log(4.096) - 2.3025852 * jax.random.uniform(splits[21], (LAYERS, FF // HD, HD), jnp.float32) ** block_levels(splits[21], (LAYERS, FF // HD, HD), ((1, 2), (2, 16)), -0.2, 0.2)), 0.4096, 4.096),
        "second_vec": jnp.clip(jnp.exp(math.log(4.096) - 2.3025852 * jax.random.uniform(splits[22], (LAYERS, 6, D), jnp.float32) ** block_levels(splits[22], (LAYERS, 6, D), ((2, 16),), -0.2, 0.2)), 0.4096, 4.096),
    }


norm_eps = 1e-05
beta_one = 0.9
beta_two = 0.999
adam_eps = 1e-08
decay_rate = 0.1
rate_matrix = 0.01
rate_vector = 0.2
root_half = 0.7071067811865476
inv_root_two_pi = 0.3989422804014327

def widen(values):
    return lax.optimization_barrier(values).astype(jnp.float32)

def layer_norm(rows, gains, shifts):
    average = lax.optimization_barrier(jnp.mean(rows, axis=-1, keepdims=True))
    centred = rows - average
    inverse = lax.rsqrt(lax.optimization_barrier(jnp.mean(centred * centred, axis=-1, keepdims=True)) + norm_eps)
    normed = centred * inverse
    return (normed * gains + shifts, normed, inverse)

def norm_back(upstream, normed, inverse, gains):
    scaled = upstream * gains
    return inverse * (scaled - lax.optimization_barrier(jnp.mean(scaled, axis=-1, keepdims=True)) - normed * lax.optimization_barrier(jnp.mean(scaled * normed, axis=-1, keepdims=True)))

def gelu_value(before):
    return 0.5 * before * (1.0 + jax.scipy.special.erf(before * root_half))

def gelu_slope(before):
    return 0.5 * (1.0 + jax.scipy.special.erf(before * root_half)) + before * jnp.exp(-0.5 * before * before) * inv_root_two_pi

def attend(queries, key_rows, values):
    scale = HD ** (-0.5)
    query_heads = widen(queries).reshape(-1, H, HD)
    key_heads = widen(key_rows).reshape(-1, H, HD)
    value_heads = widen(values).reshape(-1, H, HD)
    scores = jnp.einsum('qhd,khd->hqk', query_heads, key_heads) * scale
    highest = lax.optimization_barrier(jnp.max(scores, axis=-1, keepdims=True))
    logsum = highest + jnp.log(lax.optimization_barrier(jnp.sum(jnp.exp(scores - highest), axis=-1, keepdims=True)))
    weights = widen(jnp.exp(scores - logsum).astype(jnp.bfloat16))
    context = jnp.einsum('hqk,khd->qhd', weights, value_heads).reshape(-1, D).astype(jnp.bfloat16)
    return (context, logsum)

def attend_back(queries, key_rows, values, logsum, grad_context):
    scale = HD ** (-0.5)
    query_heads = widen(queries).reshape(-1, H, HD)
    key_heads = widen(key_rows).reshape(-1, H, HD)
    value_heads = widen(values).reshape(-1, H, HD)
    grad_heads = widen(grad_context).reshape(-1, H, HD)
    scores = jnp.einsum('qhd,khd->hqk', query_heads, key_heads) * scale
    probs = jnp.exp(scores - logsum)
    weights = widen(probs.astype(jnp.bfloat16))
    grad_values = jnp.einsum('hqk,qhd->khd', weights, grad_heads)
    grad_probs = jnp.einsum('qhd,khd->hqk', grad_heads, value_heads)
    inner = lax.optimization_barrier(jnp.sum(probs * grad_probs, axis=-1, keepdims=True))
    grad_scores = widen((probs * (grad_probs - inner) * scale).astype(jnp.bfloat16))
    grad_query = jnp.einsum('hqk,khd->qhd', grad_scores, key_heads)
    grad_keys = jnp.einsum('hqk,qhd->khd', grad_scores, query_heads)
    return (grad_query.reshape(-1, D), grad_keys.reshape(-1, D), grad_values.reshape(-1, D))

def layer_params(masters, which_layer):
    w_qkv, w_out, w_up, w_down, b_qv, b_up, vectors = masters
    return (w_qkv[which_layer].astype(jnp.bfloat16), w_out[which_layer].astype(jnp.bfloat16), w_up[which_layer].astype(jnp.bfloat16), w_down[which_layer].astype(jnp.bfloat16), b_qv[which_layer].reshape(2, D).astype(jnp.bfloat16), b_up[which_layer].reshape(FF).astype(jnp.bfloat16), vectors[which_layer].astype(jnp.bfloat16))

def clip_forward(resid, params):
    wqkv, wout, wup, wdown, bqv, bup, vecs = params
    normed_one, hat_one, inv_one = layer_norm(resid, vecs[0], vecs[1])
    act_one = normed_one.astype(jnp.bfloat16)
    projected = jnp.dot(act_one, wqkv.reshape(D, 3 * D), preferred_element_type=jnp.float32).reshape(-1, 3, D)
    queries = (projected[:, 0] + bqv[0]).astype(jnp.bfloat16)
    key_rows = projected[:, 1].astype(jnp.bfloat16)
    values = (projected[:, 2] + bqv[1]).astype(jnp.bfloat16)
    context, logsum = attend(queries, key_rows, values)
    middle = resid + jnp.dot(context, wout, preferred_element_type=jnp.float32) + vecs[4]
    normed_two, hat_two, inv_two = layer_norm(middle, vecs[2], vecs[3])
    act_two = normed_two.astype(jnp.bfloat16)
    before = jnp.dot(act_two, wup, preferred_element_type=jnp.float32) + bup
    hidden = gelu_value(before).astype(jnp.bfloat16)
    result = middle + jnp.dot(hidden, wdown, preferred_element_type=jnp.float32) + vecs[5]
    saved = (act_one, hat_one, inv_one, queries, key_rows, values, context, logsum, act_two, hat_two, inv_two, before, hidden)
    return (result, saved)

def forward_only(resid, params):
    return clip_forward(resid, params)[0]

def clip_backward(resid, upstream, params):
    wqkv, wout, wup, wdown, bqv, bup, vecs = params
    saved = clip_forward(resid, params)[1]
    act_one, hat_one, inv_one, queries, key_rows, values, context, logsum, act_two, hat_two, inv_two, before, hidden = saved
    grad_shift_out = lax.optimization_barrier(jnp.sum(upstream, axis=0))
    upstream_low = upstream.astype(jnp.bfloat16)
    grad_down = jnp.dot(hidden.T, upstream_low, preferred_element_type=jnp.float32)
    grad_before = jnp.dot(upstream_low, wdown.T, preferred_element_type=jnp.float32) * gelu_slope(before)
    grad_bup = lax.optimization_barrier(jnp.sum(grad_before, axis=0))
    before_low = grad_before.astype(jnp.bfloat16)
    grad_up = jnp.dot(act_two.T, before_low, preferred_element_type=jnp.float32)
    grad_act_two = jnp.dot(before_low, wup.T, preferred_element_type=jnp.float32)
    grad_gain_two = lax.optimization_barrier(jnp.sum(grad_act_two * hat_two, axis=0))
    grad_shift_two = lax.optimization_barrier(jnp.sum(grad_act_two, axis=0))
    grad_middle = upstream + norm_back(grad_act_two, hat_two, inv_two, vecs[2])
    grad_bias_out = lax.optimization_barrier(jnp.sum(grad_middle, axis=0))
    middle_low = grad_middle.astype(jnp.bfloat16)
    grad_wout = jnp.dot(context.T, middle_low, preferred_element_type=jnp.float32)
    grad_context = jnp.dot(middle_low, wout.T, preferred_element_type=jnp.float32).astype(jnp.bfloat16)
    grad_query, grad_keys, grad_values = attend_back(queries, key_rows, values, logsum, grad_context)
    grad_bqv = jnp.stack([lax.optimization_barrier(jnp.sum(grad_query, axis=0)), lax.optimization_barrier(jnp.sum(grad_values, axis=0))])
    stacked = jnp.stack([grad_query, grad_keys, grad_values], axis=1).astype(jnp.bfloat16).reshape(-1, 3 * D)
    grad_qkv = jnp.dot(act_one.T, stacked, preferred_element_type=jnp.float32).reshape(D, 3, D)
    grad_act_one = jnp.dot(stacked, wqkv.reshape(D, 3 * D).T, preferred_element_type=jnp.float32)
    grad_gain_one = lax.optimization_barrier(jnp.sum(grad_act_one * hat_one, axis=0))
    grad_shift_one = lax.optimization_barrier(jnp.sum(grad_act_one, axis=0))
    grad_resid = grad_middle + norm_back(grad_act_one, hat_one, inv_one, vecs[0])
    grad_vectors = jnp.stack([grad_gain_one, grad_shift_one, grad_gain_two, grad_shift_two, grad_bias_out, grad_shift_out])
    return (grad_resid, (grad_qkv, grad_wout, grad_up, grad_down, grad_bqv, grad_bup, grad_vectors))

def adamw(weight, gradient, first, second, rate, decay):
    first_new = beta_one * first + (1.0 - beta_one) * gradient
    second_new = beta_two * second + (1.0 - beta_two) * gradient * gradient
    first_hat = first_new / (1.0 - beta_one ** STEP)
    second_hat = second_new / (1.0 - beta_two ** STEP)
    weight_new = weight - rate * (first_hat / (jnp.sqrt(second_hat) + adam_eps) + decay * weight)
    return (weight_new, first_new, second_new)

def reference(frames, cotangent, w_qkv, w_out, w_up, w_down, b_qv, b_up, vectors, first_qkv, first_out, first_up, first_down, first_bqv, first_bup, first_vec, second_qkv, second_out, second_up, second_down, second_bqv, second_bup, second_vec):
    masters = (w_qkv, w_out, w_up, w_down, b_qv, b_up, vectors)
    firsts = (first_qkv, first_out, first_up, first_down, first_bqv, first_bup, first_vec)
    seconds = (second_qkv, second_out, second_up, second_down, second_bqv, second_bup, second_vec)
    resid = frames.reshape(-1, SEQ, D).astype(jnp.float32)
    inputs = []
    for which_layer in range(LAYERS):
        params = layer_params(masters, which_layer)
        inputs.append(resid)
        resid = lax.map(partial(forward_only, params=params), resid)
    output = resid.reshape(-1, D).astype(jnp.bfloat16)
    upstream = cotangent.reshape(-1, SEQ, D).astype(jnp.float32)
    layer_grads = [None] * LAYERS
    for which_layer in reversed(range(LAYERS)):
        params = layer_params(masters, which_layer)
        zeros = tuple((jnp.zeros(master.shape[1:], jnp.float32) for master in masters))

        def accumulate(totals, item, params=params):
            grad_resid, pieces = clip_backward(item[0], item[1], params)
            return (tuple((total + piece.reshape(total.shape) for total, piece in zip(totals, pieces))), grad_resid)
        totals, upstream = lax.scan(accumulate, zeros, (inputs[which_layer], upstream))
        layer_grads[which_layer] = totals
    grads = tuple((jnp.stack([layer_grads[section][number] for section in range(LAYERS)]) for number in range(7)))
    rates = (rate_matrix,) * 4 + (rate_vector,) * 3
    decays = (decay_rate,) * 4 + (0.0,) * 3
    updated = [adamw(masters[number], grads[number], firsts[number], seconds[number], rates[number], decays[number]) for number in range(7)]
    grad_input = upstream.reshape(-1, D)
    return (output, grad_input, grads[0], grads[1], grads[2], grads[3], grads[4], grads[5], grads[6], updated[0][0], updated[1][0], updated[2][0], updated[3][0], updated[4][0], updated[5][0], updated[6][0], updated[0][1], updated[1][1], updated[2][1], updated[3][1], updated[4][1], updated[5][1], updated[6][1], updated[0][2], updated[1][2], updated[2][2], updated[3][2], updated[4][2], updated[5][2], updated[6][2])
```

```python
import functools
import jax
import jax.numpy as jnp
from jax import lax
from jax.experimental import pallas as pl
from jax.experimental.pallas import tpu as pltpu
from jax.sharding import PartitionSpec as P

HD = 64
SEQ = 256
STEP = 3

norm_eps = 1e-05
beta_one = 0.9
beta_two = 0.999
adam_eps = 1e-08
decay_rate = 0.1
rate_matrix = 0.01
rate_vector = 0.2
root_half = 0.7071067811865476
inv_root_two_pi = 0.3989422804014327

BF = jnp.bfloat16
F32 = jnp.float32
NN = (((1,), (0,)), ((), ()))
NT = (((1,), (1,)), ((), ()))
TN = (((0,), (0,)), ((), ()))
MESH = pl.DeviceIdType.MESH
LANES = 128
BIAS_ROWS = 16
VEC_ROWS = 8


def mm(left, right, dims):
    return lax.dot_general(left, right, dims, preferred_element_type=F32)


def factor_axes(count):
    chips = count // 2
    sizes = []
    while chips > 1:
        step = 4 if chips % 4 == 0 else 2 if chips % 2 == 0 else chips
        sizes.append(step)
        chips //= step
    return tuple(sizes) + (2,)


class Plan:
    def __init__(self, count, rows, width, half, hidden, layers):
        self.count = count
        self.axes = factor_axes(count)
        strides = []
        stride = count
        for size in self.axes:
            stride //= size
            strides.append(stride)
        self.strides = tuple(strides)
        self.rows = rows
        self.width = width
        self.own = width // count
        self.block = -(-self.own // 16) * 16
        self.padded = self.block * count
        self.half = half
        self.pairs = half // LANES
        self.layers = layers
        self.piece = 2 * half
        self.up_pieces = hidden // self.piece
        self.pieces = 2 + 2 * self.up_pieces
        self.quarter = HD // count
        self.heads = half // HD
        self.bias_cols = 2 * half + hidden
        self.slots = sum(size - 1 for size in self.axes)
        self.chunk = rows // 2


def train_kernel(
    plan,
    frames_ref,
    cot_ref,
    shard_ref,
    small_ref,
    out_ref,
    gin_ref,
    gout_ref,
    smallg_ref,
    W,
    SB,
    VEC,
    BIAS,
    XS,
    XR,
    MID,
    ACC,
    LAST,
    HAT,
    INV,
    ACT,
    Q,
    K,
    V,
    LSE,
    CTX,
    SLOPE,
    HIDDEN,
    DX,
    LOW,
    FL,
    DCTX,
    RQK,
    RV,
    VG,
    BG,
    TURN,
    SG,
    RBs,
    RSs,
    ag_send,
    ag_recv,
    rs_send,
    rs_recv,
    x_send,
    x_recv,
):
    axes = plan.axes
    depth = len(axes)
    rp = plan.block
    Dp = plan.padded
    L = plan.layers
    NP = plan.pieces
    UP = plan.up_pieces
    half = plan.half
    rows = plan.rows
    chunk = plan.chunk

    me = lax.axis_index("fsdp")
    side = lax.axis_index("tp")
    digit = [lax.rem(me // stride, size) for stride, size in zip(plan.strides, axes)]
    offsets = []
    total = 0
    for size in axes:
        offsets.append(total)
        total += size - 1

    def peer(k, j):
        value = lax.rem(digit[k] + j, axes[k])
        return value, (me + (value - digit[k]) * plan.strides[k], side)

    def source(k, j):
        return lax.rem(digit[k] - j + axes[k], axes[k])

    def place(k, value):
        return (slice(None),) * k + (value,) + tuple(digit[k + 1 :])

    other = (me, 1 - side)

    barrier = pltpu.get_barrier_semaphore()
    greeted = 1
    pl.semaphore_signal(barrier, inc=1, device_id=other, device_id_type=MESH)
    for k in range(depth):
        for j in range(1, axes[k]):
            pl.semaphore_signal(barrier, inc=1, device_id=peer(k, j)[1], device_id_type=MESH)
            greeted += 1
    pl.semaphore_wait(barrier, greeted)

    def remote(src, dst, send, recv, device):
        return pltpu.make_async_remote_copy(
            src_ref=src,
            dst_ref=dst,
            send_sem=send,
            recv_sem=recv,
            device_id=device,
            device_id_type=MESH,
        )

    small_index = L * NP

    def gather_copy(k, j, piece, small, sending):
        slot = offsets[k] + j - 1
        value, device = peer(k, j)
        spot = place(k, digit[k]) if sending else place(k, source(k, j))
        if small:
            dst = SB.at[spot]
            src = small_ref if (k == 0 and sending) else dst
        else:
            dst = W.at[(piece,) + spot]
            src = shard_ref.at[piece] if (k == 0 and sending) else dst
        return remote(src, dst, ag_send.at[piece, slot], ag_recv.at[piece, slot], device)

    def gather_start(k, piece, small=False):
        for j in range(1, axes[k]):
            gather_copy(k, j, piece, small, True).start()

    def gather_wait(k, piece, small=False):
        for j in range(1, axes[k]):
            gather_copy(k, j, piece, small, False).wait_recv()

    def gather_drain(piece, small=False):
        for k in range(depth):
            for j in range(1, axes[k]):
                gather_copy(k, j, piece, small, True).wait_send()

    def ready(piece):
        @pl.when(piece + 1 < L * NP)
        def _():
            gather_wait(0, piece + 1)
            gather_start(1, piece + 1)

        for k in range(1, depth):
            gather_wait(k, piece)
            if k + 1 < depth:
                gather_start(k + 1, piece)

    here = tuple(digit)
    SB[here] = small_ref[...]
    gather_start(0, small_index, True)
    for piece in range(L * NP):
        gather_start(0, piece)
    for piece in range(L * NP):
        W[(piece,) + here] = shard_ref[piece]

    gather_wait(0, small_index, True)
    for k in range(1, depth):
        gather_start(k, small_index, True)
        gather_wait(k, small_index, True)
    gather_wait(0, 0)
    gather_start(1, 0)

    vec_all = SB[(slice(None),) * depth + (slice(0, rp), slice(None))]
    vec_rows = vec_all.reshape(Dp, LANES).astype(F32).T
    for layer in range(L):
        VEC[layer] = vec_rows[layer * VEC_ROWS : (layer + 1) * VEC_ROWS]
    every = L * plan.bias_cols
    shift = HD.bit_length() - 1

    def static_place(owner):
        return tuple((owner // stride) % size for stride, size in zip(plan.strides, axes))

    def column_ids(lines):
        return lax.broadcasted_iota(jnp.int32, (lines, every), 1)

    def line_ids(lines):
        return lax.broadcasted_iota(jnp.int32, (lines, every), 0)

    def group_match():
        return lax.shift_right_logical(column_ids(LANES), shift) == line_ids(LANES)

    def feature_match(lines):
        return (column_ids(lines) & (HD - 1)) == line_ids(lines)

    for owner in range(plan.count):
        held = SB[static_place(owner) + (slice(rp, rp + BIAS_ROWS), slice(None))].astype(F32)
        low = owner * plan.quarter
        TURN[low : low + plan.quarter] = held[0 : plan.quarter]
    spread = mm(TURN[0:HD].astype(BF), group_match().astype(F32).astype(BF), NN)
    bias_row = jnp.sum(jnp.where(feature_match(HD), spread, 0.0), axis=0, keepdims=True)
    for layer in range(L):
        BIAS[layer] = bias_row[:, layer * plan.bias_cols : (layer + 1) * plan.bias_cols]

    if plan.block != plan.own:
        column = lax.broadcasted_iota(jnp.int32, (1, Dp), 1)
        valid = (lax.rem(column, rp) < plan.own).astype(F32)
    else:
        valid = None

    def average(values):
        return jnp.sum(values, axis=-1, keepdims=True) * (1.0 / plan.width)

    def masked(values):
        return values if valid is None else values * valid

    def piece_of(index, low=0, high=None):
        high = plan.piece if high is None else high
        tail = (slice(None), slice(low, high))
        return W[(index,) + (slice(None),) * depth + tail].reshape(Dp, high - low)

    def norm_forward(values, layer, which, region):
        centred = masked(values - average(values))
        inverse = lax.rsqrt(average(centred * centred) + norm_eps)
        hat = centred * inverse
        HAT[layer, which, region] = hat
        INV[layer, which, region] = inverse
        gain = VEC[layer, 2 * which : 2 * which + 1]
        shift = VEC[layer, 2 * which + 1 : 2 * which + 2]
        ACT[layer, which, region] = (hat * gain + shift).astype(BF)

    def exchange_copy(number, slot, part):
        region = pl.ds(part * chunk, chunk)
        return remote(
            XS.at[slot, region],
            XR.at[slot, region],
            x_send.at[number, part],
            x_recv.at[number, part],
            other,
        )

    def exchange_send(number, slot, part, values):
        XS[slot, pl.ds(part * chunk, chunk)] = values.astype(BF)
        exchange_copy(number, slot, part).start()

    def exchange_sum(number, slot, part):
        exchange_copy(number, slot, part).wait_recv()
        region = pl.ds(part * chunk, chunk)
        result = XS[slot, region].astype(F32) + XR[slot, region].astype(F32)
        return result

    def exchange_done(number, slot):
        for part in range(2):
            exchange_copy(number, slot, part).wait_send()

    lane = lax.broadcasted_iota(jnp.int32, (1, LANES), 1)
    head_mask = [((lane // HD) == h).astype(F32).astype(BF) for h in range(LANES // HD)]
    scale = HD ** (-0.5)
    clips = rows // SEQ

    def attend(layer):
        def one(item, _):
            pair = item // clips
            clip = lax.rem(item, clips)
            span = pl.ds(clip * SEQ, SEQ)
            query = Q[layer, pair, span]
            key = K[layer, pair, span]
            value = V[layer, pair, span]
            total = None
            for h, mask in enumerate(head_mask):
                scores = mm(query * mask, key, NT) * scale
                highest = jnp.max(scores, axis=1, keepdims=True)
                logsum = highest + jnp.log(jnp.sum(jnp.exp(scores - highest), axis=1, keepdims=True))
                LSE[layer, pair, h, span] = logsum
                weights = jnp.exp(scores - logsum).astype(BF)
                part = mm(weights, value * mask, NN)
                total = part if total is None else total + part
            CTX[layer, pair, span] = total.astype(BF)
            return 0

        lax.fori_loop(0, plan.pairs * clips, one, 0)

    def context_of(layer, region=slice(None)):
        return jnp.concatenate([CTX[layer, pair, region] for pair in range(plan.pairs)], axis=1)

    def forward_layer(layer, carry):
        first = layer * NP

        @pl.when(layer == 0)
        def _():
            value = frames_ref[...].astype(F32)
            DX[...] = value
            norm_forward(value, layer, 0, slice(None))

        @pl.when(layer > 0)
        def _():
            for part in range(2):
                region = pl.ds(part * chunk, chunk)
                value = MID[region] + exchange_sum(2 * layer - 1, 1, part) + VEC[layer - 1, 5:6]
                DX[region] = value
                norm_forward(value, layer, 0, region)
            exchange_done(2 * layer - 1, 1)

        ready(first)
        both = mm(ACT[layer, 0], piece_of(first), NN)
        for pair in range(plan.pairs):
            low = pair * LANES
            query = both[:, low : low + LANES] + BIAS[layer, :, low : low + LANES]
            Q[layer, pair] = query.astype(BF)
            K[layer, pair] = both[:, half + low : half + low + LANES].astype(BF)
        ready(first + 1)
        values = mm(ACT[layer, 0], piece_of(first + 1, 0, half), NN)
        for pair in range(plan.pairs):
            low = pair * LANES
            bias = BIAS[layer, :, half + low : half + low + LANES]
            V[layer, pair] = (values[:, low : low + LANES] + bias).astype(BF)
        attend(layer)
        for part in range(2):
            region = pl.ds(part * chunk, chunk)
            heads = context_of(layer, region)
            exchange_send(2 * layer, 0, part, mm(heads, piece_of(first + 1, half), NT))
        for number in range(UP):
            ready(first + 2 + number)
        for part in range(2):
            region = pl.ds(part * chunk, chunk)
            value = DX[region] + exchange_sum(2 * layer, 0, part) + VEC[layer, 4:5]
            MID[region] = value
            norm_forward(value, layer, 1, region)
        exchange_done(2 * layer, 0)
        for number in range(UP):
            before = mm(ACT[layer, 1], piece_of(first + 2 + number), NN)
            low = 2 * half + number * plan.piece
            before = before + BIAS[layer, :, low : low + plan.piece]
            bell = 0.5 * (1.0 + lax.erf(before * root_half))
            HIDDEN[layer, number] = (before * bell).astype(BF)
            slope = bell + before * jnp.exp(-0.5 * before * before) * inv_root_two_pi
            SLOPE[layer, number] = slope.astype(BF)
        for number in range(UP):
            ready(first + 2 + UP + number)
            term = mm(HIDDEN[layer, number], piece_of(first + 2 + UP + number), NT)
            if number + 1 < UP:
                ACC[...] = term if number == 0 else ACC[...] + term
            else:
                whole = term + ACC[...] if UP > 1 else term

                @pl.when(layer + 1 < L)
                def _():
                    for part in range(2):
                        exchange_send(2 * layer + 1, 1, part, whole[part * chunk : (part + 1) * chunk])

                @pl.when(layer + 1 == L)
                def _():
                    LAST[...] = whole.astype(BF)

        return carry

    lax.fori_loop(0, L, forward_layer, 0)

    def landing(k, piece):
        return lax.rem(piece, NP) if k == depth - 1 else piece

    def scatter_copy(k, j, piece, small):
        slot = offsets[k] + j - 1
        value, device = peer(k, j)
        spot = place(k, value)
        if small:
            src = SG.at[spot]
            dst = RSs[k].at[j - 1]
        else:
            src = W.at[(piece,) + spot]
            dst = RBs[k].at[landing(k, piece), j - 1]
        return remote(src, dst, rs_send.at[piece, slot], rs_recv.at[piece, slot], device)

    def scatter_start(k, piece, small=False):
        for j in range(1, axes[k]):
            scatter_copy(k, j, piece, small).start()

    def scatter_wait(k, piece, small=False):
        for j in range(1, axes[k]):
            scatter_copy(k, j, piece, small).wait_recv()

    def scatter_step(k, piece, small=False):
        scatter_wait(k, piece, small)
        spot = place(k, digit[k])
        if small:
            value = SG[spot]
            for j in range(1, axes[k]):
                value = value + RSs[k][j - 1]
            if k == 0:
                smallg_ref[...] = value
            else:
                SG[spot] = value
                scatter_start(k - 1, piece, True)
        else:
            value = W[(piece,) + spot].astype(F32)
            for j in range(1, axes[k]):
                value = value + RBs[k][landing(k, piece), j - 1].astype(F32)
            if k == 0:
                gout_ref[piece] = value
            else:
                W[(piece,) + spot] = value.astype(BF)
                scatter_start(k - 1, piece)

    def scatter_drain(piece, small=False):
        for k in range(depth):
            for j in range(1, axes[k]):
                scatter_copy(k, j, piece, small).wait_send()

    block_shape = axes + (rp,)

    def put_gradient(index, value, low=0, high=None):
        high = plan.piece if high is None else high
        tail = (slice(None), slice(low, high))
        W[(index,) + (slice(None),) * depth + tail] = value.astype(BF).reshape(block_shape + (high - low,))

    for piece in range(L * NP):
        gather_drain(piece)
    gather_drain(small_index, True)

    def attend_back(layer):
        def one(item, _):
            pair = item // clips
            clip = lax.rem(item, clips)
            span = pl.ds(clip * SEQ, SEQ)
            query = Q[layer, pair, span]
            key = K[layer, pair, span]
            value = V[layer, pair, span]
            upper = DCTX[pair, span]
            grad_q = grad_k = grad_v = None
            for h, mask in enumerate(head_mask):
                scores = mm(query * mask, key, NT) * scale
                probs = jnp.exp(scores - LSE[layer, pair, h, span])
                weights = probs.astype(BF)
                up_head = upper * mask
                part_v = mm(weights, up_head, TN)
                grad_p = mm(up_head, value, NT)
                inner = jnp.sum(probs * grad_p, axis=1, keepdims=True)
                grad_s = (probs * (grad_p - inner) * scale).astype(BF)
                part_q = mm(grad_s, key * mask, NN)
                part_k = mm(grad_s, query * mask, TN)
                grad_q = part_q if grad_q is None else grad_q + part_q
                grad_k = part_k if grad_k is None else grad_k + part_k
                grad_v = part_v if grad_v is None else grad_v + part_v
            low = pl.ds(pl.multiple_of(pair * LANES, LANES), LANES)
            next_low = pl.ds(pl.multiple_of(half + pair * LANES, LANES), LANES)
            RQK[span, low] = grad_q.astype(BF)
            RQK[span, next_low] = grad_k.astype(BF)
            RV[span, low] = grad_v.astype(BF)
            sum_q = jnp.sum(grad_q, axis=0, keepdims=True)
            sum_v = jnp.sum(grad_v, axis=0, keepdims=True)

            @pl.when(clip == 0)
            def _():
                BG[layer, :, low] = sum_q
                BG[layer, :, next_low] = sum_v

            @pl.when(clip > 0)
            def _():
                BG[layer, :, low] += sum_q
                BG[layer, :, next_low] += sum_v

            return 0

        lax.fori_loop(0, plan.pairs * clips, one, 0)

    def column_sum(values):
        return jnp.sum(values, axis=0, keepdims=True)

    def norm_backward(upper, layer, which, region):
        hat = HAT[layer, which, region]
        scaled = upper * VEC[layer, 2 * which : 2 * which + 1]
        return INV[layer, which, region] * (
            masked(scaled - average(scaled)) - hat * average(scaled * hat)
        )

    def keep_rows(layer, line, part, value):
        if part == 0:
            VG[layer, line : line + 1] = value
        else:
            VG[layer, line : line + 1] += value

    DX[...] = cot_ref[...].astype(F32)
    DMID = ACC

    def produced(m):
        step = m // NP
        turn = lax.rem(m, NP)
        name = jnp.where(
            turn < UP,
            2 + UP + turn,
            jnp.where(turn < 2 * UP, 2 + turn - UP, NP - 1 - turn),
        )
        return (L - 1 - step) * NP + name

    def pump(m, carry):
        for k in range(depth - 2, -1, -1):
            earlier = m - (depth - 2 - k)

            @pl.when((earlier >= 0) & (earlier < L * NP))
            def _():
                scatter_step(k, produced(earlier))

        return carry

    def pumped(step, place_in_layer):
        counts = PUMPS[place_in_layer]
        value = counts[0]
        for s in range(1, L):
            value = jnp.where(step == s, counts[min(s, len(counts) - 1)], value)
        return jnp.minimum(value, L * NP)

    def pump_to(step, place_in_layer):
        if place_in_layer == 0:
            low = jnp.where(step == 0, 0, pumped(step - 1, len(PUMPS) - 1))
        else:
            low = pumped(step, place_in_layer - 1)
        lax.fori_loop(low, pumped(step, place_in_layer), pump, 0)

    def backward_layer(step, carry):
        layer = L - 1 - step
        first = layer * NP
        up = first + 2
        down = first + 2 + UP
        number_up = 2 * L + 2 * step
        VG[layer] = jnp.zeros((VEC_ROWS, Dp), F32)
        upper = DX[...]
        VG[layer, 5:6] = column_sum(upper)
        LOW[...] = upper.astype(BF)
        for number in range(UP):
            grad = mm(LOW[...], piece_of(down + number), NN) * SLOPE[layer, number].astype(F32)
            low = 2 * half + number * plan.piece
            BG[layer, :, low : low + plan.piece] = column_sum(grad)
            FL[number] = grad.astype(BF)
            put_gradient(down + number, mm(LOW[...], HIDDEN[layer, number], TN))
            scatter_start(depth - 1, down + number)
        for part in range(2):
            region = pl.ds(part * chunk, chunk)
            whole = None
            for number in range(UP):
                term = mm(FL[number, region], piece_of(up + number), NT)
                whole = term if whole is None else whole + term
            exchange_send(number_up, 1, part, whole)
        for number in range(UP):
            scatter_step(depth - 1, down + number)
        for number in range(UP):
            put_gradient(up + number, mm(ACT[layer, 1], FL[number], TN))
            scatter_start(depth - 1, up + number)
        for number in range(UP):
            scatter_step(depth - 1, up + number)
        pump_to(step, 0)
        for part in range(2):
            region = pl.ds(part * chunk, chunk)
            grad = exchange_sum(number_up, 1, part)
            keep_rows(layer, 2, part, column_sum(grad * HAT[layer, 1, region]))
            keep_rows(layer, 3, part, column_sum(grad))
            grad_mid = DX[region] + norm_backward(grad, layer, 1, region)
            DMID[region] = grad_mid
            keep_rows(layer, 4, part, column_sum(grad_mid))
            LOW[region] = grad_mid.astype(BF)
        exchange_done(number_up, 1)
        heads = mm(LOW[...], piece_of(first + 1, half), NN)
        for pair in range(plan.pairs):
            DCTX[pair] = heads[:, pair * LANES : (pair + 1) * LANES].astype(BF)
        put_gradient(first + 1, mm(LOW[...], context_of(layer), TN), half)
        attend_back(layer)
        for part in range(2):
            region = pl.ds(part * chunk, chunk)
            whole = mm(RQK[region], piece_of(first), NT)
            whole = whole + mm(RV[region], piece_of(first + 1, 0, half), NT)
            exchange_send(number_up + 1, 0, part, whole)
        put_gradient(first + 1, mm(ACT[layer, 0], RV[...], TN), 0, half)
        scatter_start(depth - 1, first + 1)
        put_gradient(first, mm(ACT[layer, 0], RQK[...], TN))
        scatter_start(depth - 1, first)
        pump_to(step, 1)
        scatter_step(depth - 1, first + 1)
        scatter_step(depth - 1, first)
        pump_to(step, 2)

        @pl.when(step + 1 == L)
        def _():
            pack_biases()

        for part in range(2):
            region = pl.ds(part * chunk, chunk)
            grad = exchange_sum(number_up + 1, 0, part)
            keep_rows(layer, 0, part, column_sum(grad * HAT[layer, 0, region]))
            keep_rows(layer, 1, part, column_sum(grad))
            DX[region] = DMID[region] + norm_backward(grad, layer, 0, region)
        exchange_done(number_up + 1, 0)
        return carry

    def pack_biases():
        row = jnp.concatenate([BG[layer] for layer in range(L)], axis=1)
        wide = jnp.where(group_match(), row, 0.0)
        high = wide.astype(BF)
        low = (wide - high.astype(F32)).astype(BF)
        select = feature_match(LANES).astype(F32).astype(BF)
        table = (mm(high, select, NT) + mm(low, select, NT)).T
        for owner in range(plan.count):
            start = owner * plan.quarter
            spot = static_place(owner) + (slice(rp, rp + plan.quarter), slice(None))
            SG[spot] = table[start : start + plan.quarter]

    SG[...] = jnp.zeros(SG.shape, F32)
    lax.fori_loop(0, L, backward_layer, 0)

    lines = [VG[layer] for layer in range(L)]
    lines.append(jnp.zeros((LANES - L * VEC_ROWS, Dp), F32))
    turned = jnp.concatenate(lines, axis=0).T.reshape(axes + (rp, LANES))
    SG[(slice(None),) * depth + (slice(0, rp), slice(None))] = turned
    scatter_start(depth - 1, small_index, True)
    for part in range(2):
        exchange_send(2 * L - 1, 1, part, LAST[pl.ds(part * chunk, chunk)])
    gin_ref[...] = DX[...]
    scatter_step(depth - 1, small_index, True)
    for part in range(2):
        region = pl.ds(part * chunk, chunk)
        value = MID[region] + exchange_sum(2 * L - 1, 1, part) + VEC[L - 1, 5:6]
        out_ref[region] = value.astype(BF)
    exchange_done(2 * L - 1, 1)
    lax.fori_loop(pumped(L - 1, len(PUMPS) - 1), L * NP + depth - 2, pump, 0)
    for k in range(depth - 2, -1, -1):
        scatter_step(k, small_index, True)
    for piece in range(L * NP):
        scatter_drain(piece)
    scatter_drain(small_index, True)


PUMPS = ((1, 5), (2, 7), (3, 8))


def run_kernel(plan, frames, cotangent, shards, small):
    L, NP, Dp, rp, rows = plan.layers, plan.pieces, plan.padded, plan.block, plan.rows
    axes = plan.axes
    depth = len(axes)
    UP = plan.up_pieces
    piece = plan.piece
    landings = []
    small_landings = []
    for k, size in enumerate(axes):
        number = NP if k == depth - 1 else L * NP
        landings.append(pltpu.VMEM((number, size - 1) + axes[:k] + (rp, piece), BF))
        small_landings.append(pltpu.VMEM((size - 1,) + axes[:k] + (rp + BIAS_ROWS, LANES), F32))
    scratch = [
        pltpu.VMEM((L * NP,) + axes + (rp, piece), BF),
        pltpu.VMEM(axes + (rp + BIAS_ROWS, LANES), BF),
        pltpu.VMEM((L, VEC_ROWS, Dp), F32),
        pltpu.VMEM((L, 1, plan.bias_cols), F32),
        pltpu.VMEM((2, rows, Dp), BF),
        pltpu.VMEM((2, rows, Dp), BF),
        pltpu.VMEM((rows, Dp), F32),
        pltpu.VMEM((rows, Dp), F32),
        pltpu.VMEM((rows, Dp), BF),
        pltpu.VMEM((L, 2, rows, Dp), F32),
        pltpu.VMEM((L, 2, rows, 1), F32),
        pltpu.VMEM((L, 2, rows, Dp), BF),
        pltpu.VMEM((L, plan.pairs, rows, LANES), BF),
        pltpu.VMEM((L, plan.pairs, rows, LANES), BF),
        pltpu.VMEM((L, plan.pairs, rows, LANES), BF),
        pltpu.VMEM((L, plan.pairs, LANES // HD, rows, 1), F32),
        pltpu.VMEM((L, plan.pairs, rows, LANES), BF),
        pltpu.VMEM((L, UP, rows, piece), BF),
        pltpu.VMEM((L, UP, rows, piece), BF),
        pltpu.VMEM((rows, Dp), F32),
        pltpu.VMEM((rows, Dp), BF),
        pltpu.VMEM((UP, rows, piece), BF),
        pltpu.VMEM((plan.pairs, rows, LANES), BF),
        pltpu.VMEM((rows, piece), BF),
        pltpu.VMEM((rows, plan.half), BF),
        pltpu.VMEM((L, VEC_ROWS, Dp), F32),
        pltpu.VMEM((L, 1, plan.bias_cols), F32),
        pltpu.VMEM((HD, LANES), F32),
        pltpu.VMEM(axes + (rp + BIAS_ROWS, LANES), F32),
        landings,
        small_landings,
        pltpu.SemaphoreType.DMA((L * NP + 1, plan.slots)),
        pltpu.SemaphoreType.DMA((L * NP + 1, plan.slots)),
        pltpu.SemaphoreType.DMA((L * NP + 1, plan.slots)),
        pltpu.SemaphoreType.DMA((L * NP + 1, plan.slots)),
        pltpu.SemaphoreType.DMA((4 * L, 2)),
        pltpu.SemaphoreType.DMA((4 * L, 2)),
    ]
    return pl.pallas_call(
        functools.partial(train_kernel, plan),
        out_shape=(
            jax.ShapeDtypeStruct((rows, Dp), BF),
            jax.ShapeDtypeStruct((rows, Dp), F32),
            jax.ShapeDtypeStruct((L * NP, rp, piece), F32),
            jax.ShapeDtypeStruct((rp + BIAS_ROWS, LANES), F32),
        ),
        in_specs=[pl.BlockSpec(memory_space=pltpu.VMEM)] * 4,
        out_specs=tuple([pl.BlockSpec(memory_space=pltpu.VMEM)] * 4),
        scratch_shapes=scratch,
        compiler_params=pltpu.CompilerParams(
            collective_id=0, has_side_effects=True, vmem_limit_bytes=67043328
        ),
        name="train_step",
    )(frames, cotangent, shards, small)


def adamw(weight, gradient, first, second, rate, decay):
    first_new = beta_one * first + (1.0 - beta_one) * gradient
    second_new = beta_two * second + (1.0 - beta_two) * gradient * gradient
    first_hat = first_new / (1.0 - beta_one**STEP)
    second_hat = second_new / (1.0 - beta_two**STEP)
    weight_new = weight - rate * (first_hat / (jnp.sqrt(second_hat) + adam_eps) + decay * weight)
    return (weight_new, first_new, second_new)


def pad_axis(values, axis, size):
    widths = [(0, 0)] * values.ndim
    widths[axis] = (0, size - values.shape[axis])
    return jnp.pad(values, widths)


def on_device(count, frames, cotangent, *tensors):
    masters, firsts, seconds = tensors[:7], tensors[7:14], tensors[14:21]
    w_qkv, w_out, w_up, w_down, b_qv, b_up, vectors = masters
    L = w_qkv.shape[0]
    rows, width = frames.shape
    half = w_qkv.shape[3]
    hidden = w_up.shape[2]
    plan = Plan(count, rows, width, half, hidden, L)
    own, rp, piece, UP = plan.own, plan.block, plan.piece, plan.up_pieces

    def spread_features(values):
        if rp == own:
            return values
        return pad_axis(values.reshape(rows, count, own), 2, rp).reshape(rows, plan.padded)

    def gather_features(values):
        if rp == own:
            return values
        return values.reshape(rows, count, rp)[:, :, :own].reshape(rows, width)

    low_qkv = w_qkv.astype(BF).reshape(L, own, 3 * half)
    low_out = w_out.astype(BF).transpose(0, 2, 1)
    low_up = w_up.astype(BF)
    low_down = w_down.astype(BF).transpose(0, 2, 1)
    parts = [low_qkv[:, :, :piece], jnp.concatenate([low_qkv[:, :, piece:], low_out], axis=2)]
    parts += [low_up[:, :, n * piece : (n + 1) * piece] for n in range(UP)]
    parts += [low_down[:, :, n * piece : (n + 1) * piece] for n in range(UP)]
    shards = jnp.stack(parts, axis=1).reshape(L * plan.pieces, own, piece)
    shards = pad_axis(shards, 1, rp)

    quarter = plan.quarter
    vec_part = pad_axis(vectors.astype(BF).transpose(2, 0, 1), 2, VEC_ROWS).reshape(own, L * VEC_ROWS)
    bias_part = jnp.concatenate(
        [b_qv.astype(BF).reshape(L, -1, quarter), b_up.astype(BF).reshape(L, -1, quarter)], axis=1
    )
    groups = bias_part.shape[1]
    bias_part = bias_part.transpose(2, 0, 1).reshape(quarter, L * groups)
    small = jnp.concatenate(
        [
            pad_axis(pad_axis(vec_part, 1, LANES), 0, rp),
            pad_axis(pad_axis(bias_part, 1, LANES), 0, BIAS_ROWS),
        ],
        axis=0,
    )

    output, grad_input, wide, small_grad = run_kernel(
        plan, spread_features(frames), spread_features(cotangent), shards, small
    )

    wide = wide.reshape(L, plan.pieces, rp, piece)[:, :, :own]
    grad_qkv = jnp.concatenate([wide[:, 0], wide[:, 1, :, :half]], axis=2).reshape(w_qkv.shape)
    grad_out = wide[:, 1, :, half:].transpose(0, 2, 1)
    grad_up = jnp.concatenate([wide[:, 2 + n] for n in range(UP)], axis=2)
    grad_down = jnp.concatenate([wide[:, 2 + UP + n] for n in range(UP)], axis=2).transpose(0, 2, 1)
    vec_grad = small_grad[:own, : L * VEC_ROWS].reshape(own, L, VEC_ROWS)[:, :, : vectors.shape[1]]
    grad_vec = vec_grad.transpose(1, 2, 0)
    bias_grad = small_grad[rp : rp + quarter, : L * groups].reshape(quarter, L, groups)
    bias_grad = bias_grad.transpose(1, 2, 0)
    split = b_qv.shape[1] * b_qv.shape[2]
    grad_bqv = bias_grad[:, :split].reshape(b_qv.shape)
    grad_bup = bias_grad[:, split:]
    grads = (grad_qkv, grad_out, grad_up, grad_down, grad_bqv, grad_bup, grad_vec)
    rates = (rate_matrix,) * 4 + (rate_vector,) * 3
    decays = (decay_rate,) * 4 + (0.0,) * 3
    updated = [
        adamw(masters[n], grads[n], firsts[n], seconds[n], rates[n], decays[n]) for n in range(7)
    ]
    return (
        (gather_features(output), gather_features(grad_input))
        + grads
        + tuple(updated[n][0] for n in range(7))
        + tuple(updated[n][1] for n in range(7))
        + tuple(updated[n][2] for n in range(7))
    )


def solution(mesh):
    tensors = (
        P(None, "fsdp", None, "tp"),
        P(None, "tp", "fsdp"),
        P(None, "fsdp", "tp"),
        P(None, "tp", "fsdp"),
        P(None, None, "tp", "fsdp"),
        P(None, "tp", "fsdp"),
        P(None, None, "fsdp"),
    )
    rows = (P("fsdp", None), P("fsdp", None))
    return jax.shard_map(
        functools.partial(on_device, mesh.shape["fsdp"]),
        mesh=mesh,
        in_specs=rows + tensors * 3,
        out_specs=rows + tensors * 4,
        check_vma=False,
    )
```

```python
import functools
import jax
import jax.numpy as jnp
from jax import lax
from jax.experimental import pallas as pl
from jax.experimental.pallas import tpu as pltpu
from jax.sharding import PartitionSpec as P

HD = 64
SEQ = 256
STEP = 3

norm_eps = 1e-05
beta_one = 0.9
beta_two = 0.999
adam_eps = 1e-08
decay_rate = 0.1
rate_matrix = 0.01
rate_vector = 0.2
root_half = 0.7071067811865476
inv_root_two_pi = 0.3989422804014327

BF = jnp.bfloat16
F32 = jnp.float32
NN = (((1,), (0,)), ((), ()))
NT = (((1,), (1,)), ((), ()))
TN = (((0,), (0,)), ((), ()))
MESH = pl.DeviceIdType.MESH
LANES = 128
BIAS_ROWS = 16
VEC_ROWS = 8


def mm(left, right, dims):
    return lax.dot_general(left, right, dims, preferred_element_type=F32)


def factor_axes(count):
    chips = count // 2
    sizes = []
    while chips > 1:
        step = 4 if chips % 4 == 0 else 2 if chips % 2 == 0 else chips
        sizes.append(step)
        chips //= step
    return tuple(sizes) + (2,)


class Plan:
    def __init__(self, count, rows, width, half, hidden, layers):
        self.count = count
        self.axes = factor_axes(count)
        strides = []
        stride = count
        for size in self.axes:
            stride //= size
            strides.append(stride)
        self.strides = tuple(strides)
        self.rows = rows
        self.width = width
        self.own = width // count
        self.block = -(-self.own // 16) * 16
        self.padded = self.block * count
        self.half = half
        self.pairs = half // LANES
        self.layers = layers
        self.ups = hidden // half
        self.units = 4 + 2 * self.ups
        self.quarter = HD // count
        self.bias_cols = 2 * half + hidden
        self.hops = tuple(1 if size == 2 else 3 for size in self.axes)
        self.slots = sum(self.hops)
        self.chunk = rows // 2


def train_kernel(
    plan,
    frames_ref,
    cot_ref,
    shard_ref,
    small_ref,
    out_ref,
    gin_ref,
    gout_ref,
    smallg_ref,
    W,
    SB,
    VEC,
    BIAS,
    XS,
    XR,
    MID,
    ACC,
    LAST,
    HAT,
    INV,
    ACT,
    Q,
    K,
    V,
    LSE,
    CTX,
    SLOPE,
    HIDDEN,
    DX,
    LOW,
    FL,
    VG,
    BG,
    TURN,
    SG,
    RBs,
    RSs,
    ag_send,
    ag_recv,
    rs_send,
    rs_recv,
    x_send,
    x_recv,
):
    axes = plan.axes
    depth = len(axes)
    rp = plan.block
    Dp = plan.padded
    L = plan.layers
    NP = plan.units
    UP = plan.ups
    half = plan.half
    rows = plan.rows
    chunk = plan.chunk

    me = lax.axis_index("fsdp")
    side = lax.axis_index("tp")
    digit = [lax.rem(me // stride, size) for stride, size in zip(plan.strides, axes)]
    slot_of = [sum(plan.hops[:k]) for k in range(depth)]
    other = (me, 1 - side)

    def device(k, value):
        return (me + (value - digit[k]) * plan.strides[k], side)

    half_side = [d // 2 for d in digit]
    outer = [(d == 0) | (d == 3) for d in digit]
    inner = [jnp.logical_not(flag) for flag in outer]
    mine_in = [1 + s for s in half_side]
    mine_out = [3 * s for s in half_side]
    far_in = [2 - s for s in half_side]
    near = [pl.ds(2 * s, 2) for s in half_side]
    far = [pl.ds(2 * (1 - s), 2) for s in half_side]
    three = [pl.ds(1 - s, 3) for s in half_side]

    barrier = pltpu.get_barrier_semaphore()

    def greet(target):
        pl.semaphore_signal(barrier, inc=1, device_id=target, device_id_type=MESH)

    greet(other)
    greeted = 1
    for k in range(depth):
        if axes[k] == 2:
            greet(device(k, 1 - digit[k]))
        else:
            greet(device(k, jnp.where(outer[k], mine_in[k], mine_out[k])))
        greeted += 1
    for k in range(depth):
        if axes[k] == 4:

            @pl.when(inner[k])
            def _():
                greet(device(k, far_in[k]))

            greeted = greeted + jnp.where(inner[k], 1, 0)
    pl.semaphore_wait(barrier, greeted)

    def remote(src, dst, send, recv, target):
        return pltpu.make_async_remote_copy(
            src_ref=src,
            dst_ref=dst,
            send_sem=send,
            recv_sem=recv,
            device_id=target,
            device_id_type=MESH,
        )

    small_index = L * NP
    straight = tuple(range(depth))

    def gather_copy(k, hop, unit, order, small, sending):
        done = order[: order.index(k)]

        def spot(value):
            return tuple(
                slice(None) if a in done else value if a == k else digit[a] for a in range(depth)
            )

        if axes[k] == 2:
            value = digit[k] if sending else 1 - digit[k]
            target = 1 - digit[k]
        elif hop == 0:
            value = digit[k] if sending else mine_out[k]
            target = mine_in[k]
        elif hop == 1:
            value = near[k] if sending else far[k]
            target = far_in[k]
        else:
            value = three[k]
            target = mine_out[k]
        dst = SB.at[spot(value)] if small else W.at[(unit,) + spot(value)]
        src = dst
        if sending and not done and hop == 0:
            src = small_ref if small else shard_ref.at[unit]
        slot = slot_of[k] + hop
        return remote(src, dst, ag_send.at[unit, slot], ag_recv.at[unit, slot], device(k, target))

    def gather_begin(k, unit, order, small):
        if axes[k] == 2:
            gather_copy(k, 0, unit, order, small, True).start()
        else:

            @pl.when(outer[k])
            def _():
                gather_copy(k, 0, unit, order, small, True).start()

    def gather_next(k, unit, order, small):
        position = order.index(k) + 1
        if position < depth:
            gather_begin(order[position], unit, order, small)

    def gather_hop(index, unit, order, small):
        for k in order:
            if index < plan.hops[k]:
                break
            index -= plan.hops[k]
        if axes[k] == 2:
            gather_copy(k, 0, unit, order, small, False).wait_recv()
            gather_next(k, unit, order, small)
            return

        @pl.when(outer[k] if index == 2 else inner[k])
        def _():
            gather_copy(k, index, unit, order, small, False).wait_recv()
            if index < 2:
                gather_copy(k, index + 1, unit, order, small, True).start()
            if index > 0:
                gather_next(k, unit, order, small)

    def gather_drain(unit, small=False):
        for k in range(depth):
            for hop in range(plan.hops[k]):
                if axes[k] == 2:
                    gather_copy(k, hop, unit, straight, small, True).wait_send()
                else:

                    @pl.when(outer[k] if hop == 0 else inner[k])
                    def _():
                        gather_copy(k, hop, unit, straight, small, True).wait_send()

    hops = plan.slots

    def gather_ahead(n, low, high):
        for index in range(low, high):
            unit = n + (hops - 1 - index if index < hops - 2 else 0)

            @pl.when((unit >= 0) & (unit < L * NP))
            def _():
                gather_hop(index, unit, straight, False)

    def gather_tick(n, carry=0):
        gather_ahead(n, 0, hops)
        return carry

    def ready(low, high):
        lax.fori_loop(low, high, gather_tick, 0)

    gather_begin(0, small_index, straight, True)
    for unit in range(L * NP):
        gather_begin(0, unit, straight, False)
    here = tuple(digit)
    SB[here] = small_ref[...]
    for unit in range(L * NP):
        W[(unit,) + here] = shard_ref[unit]
    for index in range(hops):
        gather_hop(index, small_index, straight, True)
        if index < hops - 1:
            gather_ahead(index - (hops - 1), 0, hops)

    vec_all = SB[(slice(None),) * depth + (slice(0, rp), slice(None))]
    vec_rows = vec_all.reshape(Dp, LANES).astype(F32).T
    for layer in range(L):
        VEC[layer] = vec_rows[layer * VEC_ROWS : (layer + 1) * VEC_ROWS]
    every = L * plan.bias_cols
    shift = HD.bit_length() - 1

    def static_place(owner):
        return tuple((owner // stride) % size for stride, size in zip(plan.strides, axes))

    def column_ids(lines):
        return lax.broadcasted_iota(jnp.int32, (lines, every), 1)

    def line_ids(lines):
        return lax.broadcasted_iota(jnp.int32, (lines, every), 0)

    def group_match():
        return lax.shift_right_logical(column_ids(LANES), shift) == line_ids(LANES)

    def feature_match(lines):
        return (column_ids(lines) & (HD - 1)) == line_ids(lines)

    for owner in range(plan.count):
        held = SB[static_place(owner) + (slice(rp, rp + BIAS_ROWS), slice(None))].astype(F32)
        low = owner * plan.quarter
        TURN[low : low + plan.quarter] = held[0 : plan.quarter]
    spread = mm(TURN[0:HD].astype(BF), group_match().astype(F32).astype(BF), NN)
    bias_row = jnp.sum(jnp.where(feature_match(HD), spread, 0.0), axis=0, keepdims=True)
    for layer in range(L):
        BIAS[layer] = bias_row[:, layer * plan.bias_cols : (layer + 1) * plan.bias_cols]

    if plan.block != plan.own:
        column = lax.broadcasted_iota(jnp.int32, (1, Dp), 1)
        valid = (lax.rem(column, rp) < plan.own).astype(F32)
    else:
        valid = None

    def average(values):
        return jnp.sum(values, axis=-1, keepdims=True) * (1.0 / plan.width)

    def masked(values):
        return values if valid is None else values * valid

    def unit_of(index):
        return W[index].reshape(Dp, half)

    def pair_of(index):
        return jnp.concatenate([unit_of(index), unit_of(index + 1)], axis=1)

    def norm_forward(values, layer, which, region):
        centred = masked(values - average(values))
        inverse = lax.rsqrt(average(centred * centred) + norm_eps)
        hat = centred * inverse
        HAT[layer, which, region] = hat
        INV[layer, which, region] = inverse
        gain = VEC[layer, 2 * which : 2 * which + 1]
        shift = VEC[layer, 2 * which + 1 : 2 * which + 2]
        ACT[layer, which, region] = (hat * gain + shift).astype(BF)

    def exchange_copy(number, slot, part):
        region = pl.ds(part * chunk, chunk)
        return remote(
            XS.at[slot, region],
            XR.at[slot, region],
            x_send.at[number, part],
            x_recv.at[number, part],
            other,
        )

    def exchange_send(number, slot, part, values):
        XS[slot, pl.ds(part * chunk, chunk)] = values.astype(BF)
        exchange_copy(number, slot, part).start()

    def exchange_sum(number, slot, part):
        exchange_copy(number, slot, part).wait_recv()
        region = pl.ds(part * chunk, chunk)
        result = XS[slot, region].astype(F32) + XR[slot, region].astype(F32)
        return result

    def exchange_done(number, slot):
        for part in range(2):
            exchange_copy(number, slot, part).wait_send()

    lane = lax.broadcasted_iota(jnp.int32, (1, LANES), 1)
    head_mask = [((lane // HD) == h).astype(F32).astype(BF) for h in range(LANES // HD)]
    scale = HD ** (-0.5)
    clips = rows // SEQ

    def attend(layer):
        def one(item, _):
            pair = item // clips
            clip = lax.rem(item, clips)
            span = pl.ds(clip * SEQ, SEQ)
            query = Q[layer, pair, span]
            key = K[layer, pair, span]
            value = V[layer, pair, span]
            total = None
            for h, mask in enumerate(head_mask):
                scores = mm(query * mask, key, NT) * scale
                highest = jnp.max(scores, axis=1, keepdims=True)
                logsum = highest + jnp.log(jnp.sum(jnp.exp(scores - highest), axis=1, keepdims=True))
                kept = logsum if h == 0 else jnp.where(lane < h * HD, kept, logsum)
                weights = jnp.exp(scores - logsum).astype(BF)
                part = mm(weights, value * mask, NN)
                total = part if total is None else total + part
            LSE[layer, pair, span] = jnp.broadcast_to(kept, (SEQ, LANES))
            CTX[layer, pair, span] = total.astype(BF)
            return 0

        lax.fori_loop(0, plan.pairs * clips, one, 0)

    def context_of(layer, region=slice(None)):
        return jnp.concatenate([CTX[layer, pair, region] for pair in range(plan.pairs)], axis=1)

    def forward_layer(layer, carry):
        first = layer * NP
        up = first + 4
        down = up + UP

        @pl.when(layer == 0)
        def _():
            value = frames_ref[...].astype(F32)
            DX[...] = value
            norm_forward(value, layer, 0, slice(None))

        ready(first, first + 2)

        @pl.when(layer > 0)
        def _():
            for part in range(2):
                region = pl.ds(part * chunk, chunk)
                value = MID[region] + exchange_sum(2 * layer - 1, 1, part) + VEC[layer - 1, 5:6]
                DX[region] = value
                norm_forward(value, layer, 0, region)
            exchange_done(2 * layer - 1, 1)

        both = mm(ACT[layer, 0], pair_of(first), NN)
        for pair in range(plan.pairs):
            low = pair * LANES
            query = both[:, low : low + LANES] + BIAS[layer, :, low : low + LANES]
            Q[layer, pair] = query.astype(BF)
            K[layer, pair] = both[:, half + low : half + low + LANES].astype(BF)
        ready(first + 2, first + 3)
        values = mm(ACT[layer, 0], unit_of(first + 2), NN)
        for pair in range(plan.pairs):
            low = pair * LANES
            bias = BIAS[layer, :, half + low : half + low + LANES]
            V[layer, pair] = (values[:, low : low + LANES] + bias).astype(BF)
        attend(layer)
        ready(first + 3, first + 4)
        for part in range(2):
            region = pl.ds(part * chunk, chunk)
            heads = context_of(layer, region)
            exchange_send(2 * layer, 0, part, mm(heads, unit_of(first + 3), NT))
        ready(up, up + UP)
        for part in range(2):
            region = pl.ds(part * chunk, chunk)
            value = DX[region] + exchange_sum(2 * layer, 0, part) + VEC[layer, 4:5]
            MID[region] = value
            norm_forward(value, layer, 1, region)
        exchange_done(2 * layer, 0)
        for number in range(0, UP, 2):
            before = mm(ACT[layer, 1], pair_of(up + number), NN)
            low = (2 + number) * half
            before = before + BIAS[layer, :, low : low + 2 * half]
            bell = 0.5 * (1.0 + lax.erf(before * root_half))
            HIDDEN[layer, number // 2] = (before * bell).astype(BF)
            slope = bell + before * jnp.exp(-0.5 * before * before) * inv_root_two_pi
            SLOPE[layer, number // 2] = slope.astype(BF)
        for number in range(0, UP, 2):
            ready(down + number, down + number + 2)
            term = mm(HIDDEN[layer, number // 2], pair_of(down + number), NT)
            if number + 2 < UP:
                ACC[...] = term if number == 0 else ACC[...] + term
            else:
                whole = term + ACC[...] if UP > 2 else term

                @pl.when(layer + 1 < L)
                def _():
                    for part in range(2):
                        exchange_send(2 * layer + 1, 1, part, whole[part * chunk : (part + 1) * chunk])

                @pl.when(layer + 1 == L)
                def _():
                    LAST[...] = whole.astype(BF)

        return carry

    lax.fori_loop(0, L, forward_layer, 0)

    def landing(k, unit):
        return lax.rem(unit, NP) if k == depth - 1 else unit

    def land(k, slots):
        return (slice(None),) * k + (slots,)

    def scatter_spot(k, order, value):
        done = order[order.index(k) + 1 :]
        return tuple(
            digit[a] if a in done else value if a == k else slice(None) for a in range(depth)
        )

    def scatter_copy(k, hop, unit, order, small):
        if axes[k] == 2:
            value, target, slots = 1 - digit[k], 1 - digit[k], 0
        elif hop == 0:
            value, target, slots = three[k], mine_in[k], pl.ds(0, 3)
        elif hop == 1:
            value, target, slots = far[k], far_in[k], pl.ds(3, 2)
        else:
            value, target, slots = mine_out[k], mine_out[k], 0
        spot = scatter_spot(k, order, value)
        if small:
            src, dst = SG.at[spot], RSs[k].at[land(k, slots)]
        else:
            src, dst = W.at[(unit,) + spot], RBs[k].at[(landing(k, unit),) + land(k, slots)]
        slot = slot_of[k] + hop
        return remote(src, dst, rs_send.at[unit, slot], rs_recv.at[unit, slot], device(k, target))

    def scatter_begin(k, unit, order, small=False):
        if axes[k] == 2:
            scatter_copy(k, 0, unit, order, small).start()
        else:

            @pl.when(outer[k])
            def _():
                scatter_copy(k, 0, unit, order, small).start()

    def held(small, unit, spot):
        return SG[spot] if small else W[(unit,) + spot].astype(F32)

    def arrived(k, small, unit, slots):
        if small:
            return RSs[k][land(k, slots)]
        return RBs[k][(landing(k, unit),) + land(k, slots)].astype(F32)

    def keep(small, unit, spot, value):
        if small:
            SG[spot] = value
        else:
            W[(unit,) + spot] = value.astype(BF)

    def finish(k, unit, order, small, slots):
        spot = scatter_spot(k, order, digit[k])
        value = held(small, unit, spot) + arrived(k, small, unit, slots)
        position = order.index(k)
        if position > 0:
            keep(small, unit, spot, value)
            scatter_begin(order[position - 1], unit, order, small)
        elif small:
            smallg_ref[...] = value
        else:
            gout_ref[unit] = value

    def add_in(k, unit, order, small, value, slots):
        spot = scatter_spot(k, order, value)
        keep(small, unit, spot, held(small, unit, spot) + arrived(k, small, unit, slots))

    def scatter_hop(index, unit, order, small=False):
        for k in reversed(order):
            if index < plan.hops[k]:
                break
            index -= plan.hops[k]
        if axes[k] == 2:
            scatter_copy(k, 0, unit, order, small).wait_recv()
            finish(k, unit, order, small, 0)
            return

        @pl.when(outer[k] if index == 2 else inner[k])
        def _():
            scatter_copy(k, index, unit, order, small).wait_recv()
            if index == 0:
                add_in(k, unit, order, small, three[k], pl.ds(0, 3))
                scatter_copy(k, 1, unit, order, small).start()
            elif index == 1:
                add_in(k, unit, order, small, mine_out[k], 3 + mine_out[k] - 2 * half_side[k])
                scatter_copy(k, 2, unit, order, small).start()
                finish(k, unit, order, small, 3 + digit[k] - 2 * half_side[k])
            else:
                finish(k, unit, order, small, 0)

    def scatter_drain(unit, small=False):
        for k in range(depth):
            for hop in range(plan.hops[k]):
                if axes[k] == 2:
                    scatter_copy(k, hop, unit, straight, small).wait_send()
                else:

                    @pl.when(outer[k] if hop == 0 else inner[k])
                    def _():
                        scatter_copy(k, hop, unit, straight, small).wait_send()

    block_shape = axes + (rp,)

    def put_gradient(index, value):
        W[index] = value.astype(BF).reshape(block_shape + (half,))
        scatter_begin(depth - 1, index, straight)

    def put_pair(index, value):
        put_gradient(index, value[:, :half])
        put_gradient(index + 1, value[:, half:])

    for unit in range(L * NP):
        gather_drain(unit)
    gather_drain(small_index, True)

    def attend_back(layer):
        def one(item, _):
            pair = item // clips
            clip = lax.rem(item, clips)
            span = pl.ds(clip * SEQ, SEQ)
            query = Q[layer, pair, span]
            key = K[layer, pair, span]
            value = V[layer, pair, span]
            upper = FL[1, span, pl.ds(pl.multiple_of(half + pair * LANES, LANES), LANES)]
            logsums = LSE[layer, pair, span]
            grad_q = grad_k = grad_v = None
            for h, mask in enumerate(head_mask):
                scores = mm(query * mask, key, NT) * scale
                probs = jnp.exp(scores - logsums[:, h * HD : h * HD + 1])
                weights = probs.astype(BF)
                up_head = upper * mask
                part_v = mm(weights, up_head, TN)
                grad_p = mm(up_head, value, NT)
                inner = jnp.sum(probs * grad_p, axis=1, keepdims=True)
                grad_s = (probs * (grad_p - inner) * scale).astype(BF)
                part_q = mm(grad_s, key * mask, NN)
                part_k = mm(grad_s, query * mask, TN)
                grad_q = part_q if grad_q is None else grad_q + part_q
                grad_k = part_k if grad_k is None else grad_k + part_k
                grad_v = part_v if grad_v is None else grad_v + part_v
            low = pl.ds(pl.multiple_of(pair * LANES, LANES), LANES)
            next_low = pl.ds(pl.multiple_of(half + pair * LANES, LANES), LANES)
            FL[0, span, low] = grad_q.astype(BF)
            FL[0, span, next_low] = grad_k.astype(BF)
            FL[1, span, low] = grad_v.astype(BF)
            sum_q = jnp.sum(grad_q, axis=0, keepdims=True)
            sum_v = jnp.sum(grad_v, axis=0, keepdims=True)

            @pl.when(clip == 0)
            def _():
                BG[layer, :, low] = sum_q
                BG[layer, :, next_low] = sum_v

            @pl.when(clip > 0)
            def _():
                BG[layer, :, low] += sum_q
                BG[layer, :, next_low] += sum_v

            return 0

        lax.fori_loop(0, plan.pairs * clips, one, 0)

    def column_sum(values):
        return jnp.sum(values, axis=0, keepdims=True)

    def norm_backward(upper, layer, which, region):
        hat = HAT[layer, which, region]
        scaled = upper * VEC[layer, 2 * which : 2 * which + 1]
        return INV[layer, which, region] * (
            masked(scaled - average(scaled)) - hat * average(scaled * hat)
        )

    def keep_rows(layer, line, part, value):
        if part == 0:
            VG[layer, line : line + 1] = value
        else:
            VG[layer, line : line + 1] += value

    DX[...] = cot_ref[...].astype(F32)
    DMID = ACC

    def produced(m):
        turn = lax.rem(m, NP)
        name = jnp.where(
            turn < UP,
            4 + UP + turn,
            jnp.where(turn < 2 * UP, 4 + turn - UP, NP - 1 - turn),
        )
        return (L - 1 - m // NP) * NP + name

    def pumped(step, place, index):
        counts = [row[min(index - 1, len(row) - 1)] - max(0, index - len(row)) for row in PUMPS[place]]
        value = counts[0]
        for s in range(1, L):
            value = jnp.where(step == s, counts[min(s, len(counts) - 1)], value)
        return jnp.clip(value, 0, L * NP)

    def pump_range(index, low, high):
        def one(m, carry):
            scatter_hop(index, produced(m), straight)
            return carry

        lax.fori_loop(low, high, one, 0)

    def pump_to(step, place):
        for index in range(1, hops):
            if place == 0:
                low = jnp.where(step == 0, 0, pumped(step - 1, len(PUMPS) - 1, index))
            else:
                low = pumped(step, place - 1, index)
            pump_range(index, low, pumped(step, place, index))

    def pump_rest():
        last = len(PUMPS) - 1
        start = PUMPS[last][-1][0]
        delays = [0 if index == 1 else index for index in range(1, hops)]
        for index in range(1, hops):
            pump_range(index, pumped(L - 1, last, index), max(0, min(start - delays[index - 1], L * NP)))

        def one(m, carry):
            for index in range(1, hops):
                earlier = m - delays[index - 1]

                @pl.when((earlier >= 0) & (earlier < L * NP))
                def _():
                    scatter_hop(index, produced(earlier), straight)

                @pl.when(earlier == L * NP)
                def _():
                    scatter_hop(index, small_index, straight, True)

            return carry

        lax.fori_loop(start, L * NP + 1 + max(delays), one, 0)

    def backward_layer(step, carry):
        layer = L - 1 - step
        first = layer * NP
        up = first + 4
        down = up + UP
        number_up = 2 * L + 2 * step

        def from_core(low, high):
            for n in range(low, high):
                scatter_hop(0, first + n, straight)

        VG[layer] = jnp.zeros((VEC_ROWS, Dp), F32)
        upper = DX[...]
        VG[layer, 5:6] = column_sum(upper)
        LOW[...] = upper.astype(BF)
        for number in range(0, UP, 2):
            grad = mm(LOW[...], pair_of(down + number), NN) * SLOPE[layer, number // 2].astype(F32)
            low = (2 + number) * half
            BG[layer, :, low : low + 2 * half] = column_sum(grad)
            FL[number // 2] = grad.astype(BF)
            put_pair(down + number, mm(LOW[...], HIDDEN[layer, number // 2], TN))
        for part in range(2):
            region = pl.ds(part * chunk, chunk)
            whole = None
            for number in range(0, UP, 2):
                term = mm(FL[number // 2, region], pair_of(up + number), NT)
                whole = term if whole is None else whole + term
            exchange_send(number_up, 1, part, whole)
        from_core(4 + UP, 4 + 2 * UP)
        pump_to(step, 0)
        for number in range(0, UP, 2):
            put_pair(up + number, mm(ACT[layer, 1], FL[number // 2], TN))
        from_core(4, 4 + UP)
        pump_to(step, 1)
        for part in range(2):
            region = pl.ds(part * chunk, chunk)
            grad = exchange_sum(number_up, 1, part)
            keep_rows(layer, 2, part, column_sum(grad * HAT[layer, 1, region]))
            keep_rows(layer, 3, part, column_sum(grad))
            grad_mid = DX[region] + norm_backward(grad, layer, 1, region)
            DMID[region] = grad_mid
            keep_rows(layer, 4, part, column_sum(grad_mid))
            LOW[region] = grad_mid.astype(BF)
        exchange_done(number_up, 1)
        heads = mm(LOW[...], unit_of(first + 3), NN)
        FL[1, :, half : 2 * half] = heads.astype(BF)
        put_gradient(first + 3, mm(LOW[...], context_of(layer), TN))
        pump_to(step, 2)
        attend_back(layer)
        for part in range(2):
            region = pl.ds(part * chunk, chunk)
            whole = mm(FL[0, region], pair_of(first), NT)
            whole = whole + mm(FL[1, region, 0:half], unit_of(first + 2), NT)
            exchange_send(number_up + 1, 0, part, whole)
        from_core(3, 4)
        pump_to(step, 3)
        put_gradient(first + 2, mm(ACT[layer, 0], FL[1, :, 0:half], TN))
        grad_qk = mm(ACT[layer, 0], FL[0], TN)
        put_gradient(first + 1, grad_qk[:, half:])
        put_gradient(first, grad_qk[:, :half])
        for n in (2, 1, 0):
            from_core(n, n + 1)
        pump_to(step, 4)

        @pl.when(step + 1 == L)
        def _():
            pack_biases()

        for part in range(2):
            region = pl.ds(part * chunk, chunk)
            grad = exchange_sum(number_up + 1, 0, part)
            keep_rows(layer, 0, part, column_sum(grad * HAT[layer, 0, region]))
            keep_rows(layer, 1, part, column_sum(grad))
            DX[region] = DMID[region] + norm_backward(grad, layer, 0, region)
        exchange_done(number_up + 1, 0)
        return carry

    def pack_biases():
        row = jnp.concatenate([BG[layer] for layer in range(L)], axis=1)
        wide = jnp.where(group_match(), row, 0.0)
        high = wide.astype(BF)
        low = (wide - high.astype(F32)).astype(BF)
        select = feature_match(LANES).astype(F32).astype(BF)
        table = (mm(high, select, NT) + mm(low, select, NT)).T
        for owner in range(plan.count):
            start = owner * plan.quarter
            spot = static_place(owner) + (slice(rp, rp + plan.quarter), slice(None))
            SG[spot] = table[start : start + plan.quarter]

    SG[...] = jnp.zeros(SG.shape, F32)
    lax.fori_loop(0, L, backward_layer, 0)

    lines = [VG[layer] for layer in range(L)]
    lines.append(jnp.zeros((LANES - L * VEC_ROWS, Dp), F32))
    turned = jnp.concatenate(lines, axis=0).T.reshape(axes + (rp, LANES))
    SG[(slice(None),) * depth + (slice(0, rp), slice(None))] = turned
    scatter_begin(depth - 1, small_index, straight, True)
    for part in range(2):
        exchange_send(2 * L - 1, 1, part, LAST[pl.ds(part * chunk, chunk)])
    gin_ref[...] = DX[...]
    scatter_hop(0, small_index, straight, True)
    pump_rest()
    for part in range(2):
        region = pl.ds(part * chunk, chunk)
        value = MID[region] + exchange_sum(2 * L - 1, 1, part) + VEC[L - 1, 5:6]
        out_ref[region] = value.astype(BF)
    exchange_done(2 * L - 1, 1)
    for unit in range(L * NP):
        scatter_drain(unit)
    scatter_drain(small_index, True)


PUMPS = (
    ((0, 0, 0, 0), (9, 7, 5, 3)),
    ((2, 1, 0, 0), (12, 9, 7, 5)),
    ((3, 2, 1, 0), (13, 11, 9, 7)),
    ((5, 2, 1, 0), (15, 13, 11, 9)),
    ((7, 5, 3, 2), (18, 15, 13, 11)),
)


def run_kernel(plan, frames, cotangent, shards, small):
    L, NP, Dp, rp, rows = plan.layers, plan.units, plan.padded, plan.block, plan.rows
    axes = plan.axes
    depth = len(axes)
    half = plan.half
    UP = plan.ups // 2
    piece = 2 * half
    landings = []
    small_landings = []
    for k, size in enumerate(axes):
        number = NP if k == depth - 1 else L * NP
        slots = 1 if size == 2 else 5
        landings.append(pltpu.VMEM((number,) + axes[:k] + (slots, rp, half), BF))
        small_landings.append(pltpu.VMEM(axes[:k] + (slots, rp + BIAS_ROWS, LANES), F32))
    scratch = [
        pltpu.VMEM((L * NP,) + axes + (rp, half), BF),
        pltpu.VMEM(axes + (rp + BIAS_ROWS, LANES), BF),
        pltpu.VMEM((L, VEC_ROWS, Dp), F32),
        pltpu.VMEM((L, 1, plan.bias_cols), F32),
        pltpu.VMEM((2, rows, Dp), BF),
        pltpu.VMEM((2, rows, Dp), BF),
        pltpu.VMEM((rows, Dp), F32),
        pltpu.VMEM((rows, Dp), F32),
        pltpu.VMEM((rows, Dp), BF),
        pltpu.VMEM((L, 2, rows, Dp), F32),
        pltpu.VMEM((L, 2, rows, 1), F32),
        pltpu.VMEM((L, 2, rows, Dp), BF),
        pltpu.VMEM((L, plan.pairs, rows, LANES), BF),
        pltpu.VMEM((L, plan.pairs, rows, LANES), BF),
        pltpu.VMEM((L, plan.pairs, rows, LANES), BF),
        pltpu.VMEM((L, plan.pairs, rows, LANES), F32),
        pltpu.VMEM((L, plan.pairs, rows, LANES), BF),
        pltpu.VMEM((L, UP, rows, piece), BF),
        pltpu.VMEM((L, UP, rows, piece), BF),
        pltpu.VMEM((rows, Dp), F32),
        pltpu.VMEM((rows, Dp), BF),
        pltpu.VMEM((UP, rows, piece), BF),
        pltpu.VMEM((L, VEC_ROWS, Dp), F32),
        pltpu.VMEM((L, 1, plan.bias_cols), F32),
        pltpu.VMEM((HD, LANES), F32),
        pltpu.VMEM(axes + (rp + BIAS_ROWS, LANES), F32),
        landings,
        small_landings,
        pltpu.SemaphoreType.DMA((L * NP + 1, plan.slots)),
        pltpu.SemaphoreType.DMA((L * NP + 1, plan.slots)),
        pltpu.SemaphoreType.DMA((L * NP + 1, plan.slots)),
        pltpu.SemaphoreType.DMA((L * NP + 1, plan.slots)),
        pltpu.SemaphoreType.DMA((4 * L, 2)),
        pltpu.SemaphoreType.DMA((4 * L, 2)),
    ]
    return pl.pallas_call(
        functools.partial(train_kernel, plan),
        out_shape=(
            jax.ShapeDtypeStruct((rows, Dp), BF),
            jax.ShapeDtypeStruct((rows, Dp), F32),
            jax.ShapeDtypeStruct((L * NP, rp, half), F32),
            jax.ShapeDtypeStruct((rp + BIAS_ROWS, LANES), F32),
        ),
        in_specs=[pl.BlockSpec(memory_space=pltpu.VMEM)] * 4,
        out_specs=tuple([pl.BlockSpec(memory_space=pltpu.VMEM)] * 4),
        scratch_shapes=scratch,
        compiler_params=pltpu.CompilerParams(
            collective_id=0, has_side_effects=True, vmem_limit_bytes=67043328
        ),
        name="train_step",
    )(frames, cotangent, shards, small)


def adamw(weight, gradient, first, second, rate, decay):
    first_new = beta_one * first + (1.0 - beta_one) * gradient
    second_new = beta_two * second + (1.0 - beta_two) * gradient * gradient
    first_hat = first_new / (1.0 - beta_one**STEP)
    second_hat = second_new / (1.0 - beta_two**STEP)
    weight_new = weight - rate * (first_hat / (jnp.sqrt(second_hat) + adam_eps) + decay * weight)
    return (weight_new, first_new, second_new)


def pad_axis(values, axis, size):
    widths = [(0, 0)] * values.ndim
    widths[axis] = (0, size - values.shape[axis])
    return jnp.pad(values, widths)


def on_device(count, frames, cotangent, *tensors):
    masters, firsts, seconds = tensors[:7], tensors[7:14], tensors[14:21]
    w_qkv, w_out, w_up, w_down, b_qv, b_up, vectors = masters
    L = w_qkv.shape[0]
    rows, width = frames.shape
    half = w_qkv.shape[3]
    hidden = w_up.shape[2]
    plan = Plan(count, rows, width, half, hidden, L)
    own, rp, UP = plan.own, plan.block, plan.ups

    def spread_features(values):
        if rp == own:
            return values
        return pad_axis(values.reshape(rows, count, own), 2, rp).reshape(rows, plan.padded)

    def gather_features(values):
        if rp == own:
            return values
        return values.reshape(rows, count, rp)[:, :, :own].reshape(rows, width)

    low_qkv = w_qkv.astype(BF).reshape(L, own, 3 * half)
    low_out = w_out.astype(BF).transpose(0, 2, 1)
    low_up = w_up.astype(BF)
    low_down = w_down.astype(BF).transpose(0, 2, 1)
    parts = [low_qkv[:, :, n * half : (n + 1) * half] for n in range(3)] + [low_out]
    parts += [low_up[:, :, n * half : (n + 1) * half] for n in range(UP)]
    parts += [low_down[:, :, n * half : (n + 1) * half] for n in range(UP)]
    shards = jnp.stack(parts, axis=1).reshape(L * plan.units, own, half)
    shards = pad_axis(shards, 1, rp)

    quarter = plan.quarter
    vec_part = pad_axis(vectors.astype(BF).transpose(2, 0, 1), 2, VEC_ROWS).reshape(own, L * VEC_ROWS)
    bias_part = jnp.concatenate(
        [b_qv.astype(BF).reshape(L, -1, quarter), b_up.astype(BF).reshape(L, -1, quarter)], axis=1
    )
    groups = bias_part.shape[1]
    bias_part = bias_part.transpose(2, 0, 1).reshape(quarter, L * groups)
    small = jnp.concatenate(
        [
            pad_axis(pad_axis(vec_part, 1, LANES), 0, rp),
            pad_axis(pad_axis(bias_part, 1, LANES), 0, BIAS_ROWS),
        ],
        axis=0,
    )

    output, grad_input, wide, small_grad = run_kernel(
        plan, spread_features(frames), spread_features(cotangent), shards, small
    )

    wide = wide.reshape(L, plan.units, rp, half)[:, :, :own]
    grad_qkv = jnp.stack([wide[:, n] for n in range(3)], axis=2)
    grad_out = wide[:, 3].transpose(0, 2, 1)
    grad_up = jnp.concatenate([wide[:, 4 + n] for n in range(UP)], axis=2)
    grad_down = jnp.concatenate([wide[:, 4 + UP + n] for n in range(UP)], axis=2).transpose(0, 2, 1)
    vec_grad = small_grad[:own, : L * VEC_ROWS].reshape(own, L, VEC_ROWS)[:, :, : vectors.shape[1]]
    grad_vec = vec_grad.transpose(1, 2, 0)
    bias_grad = small_grad[rp : rp + quarter, : L * groups].reshape(quarter, L, groups)
    bias_grad = bias_grad.transpose(1, 2, 0)
    split = b_qv.shape[1] * b_qv.shape[2]
    grad_bqv = bias_grad[:, :split].reshape(b_qv.shape)
    grad_bup = bias_grad[:, split:]
    grads = (grad_qkv, grad_out, grad_up, grad_down, grad_bqv, grad_bup, grad_vec)
    rates = (rate_matrix,) * 4 + (rate_vector,) * 3
    decays = (decay_rate,) * 4 + (0.0,) * 3
    updated = [
        adamw(masters[n], grads[n], firsts[n], seconds[n], rates[n], decays[n]) for n in range(7)
    ]
    return (
        (gather_features(output), gather_features(grad_input))
        + grads
        + tuple(updated[n][0] for n in range(7))
        + tuple(updated[n][1] for n in range(7))
        + tuple(updated[n][2] for n in range(7))
    )


def solution(mesh):
    tensors = (
        P(None, "fsdp", None, "tp"),
        P(None, "tp", "fsdp"),
        P(None, "fsdp", "tp"),
        P(None, "tp", "fsdp"),
        P(None, None, "tp", "fsdp"),
        P(None, "tp", "fsdp"),
        P(None, None, "fsdp"),
    )
    rows = (P("fsdp", None), P("fsdp", None))
    return jax.shard_map(
        functools.partial(on_device, mesh.shape["fsdp"]),
        mesh=mesh,
        in_specs=rows + tensors * 3,
        out_specs=rows + tensors * 4,
        check_vma=False,
    )
```

```python
import functools
import jax
import jax.numpy as jnp
from jax import lax
from jax.experimental import pallas as pl
from jax.experimental.pallas import tpu as pltpu
from jax.sharding import PartitionSpec as P

HD = 64
SEQ = 256
STEP = 3

norm_eps = 1e-05
beta_one = 0.9
beta_two = 0.999
adam_eps = 1e-08
decay_rate = 0.1
rate_matrix = 0.01
rate_vector = 0.2
root_half = 0.7071067811865476
inv_root_two_pi = 0.3989422804014327

BF = jnp.bfloat16
F32 = jnp.float32
NN = (((1,), (0,)), ((), ()))
NT = (((1,), (1,)), ((), ()))
TN = (((0,), (0,)), ((), ()))
MESH = pl.DeviceIdType.MESH
LANES = 128
BIAS_ROWS = 16
TURN_EVERY = 6
VEC_ROWS = 8


def mm(left, right, dims):
    return lax.dot_general(left, right, dims, preferred_element_type=F32)


def factor_axes(count):
    chips = count // 2
    sizes = []
    while chips > 1:
        step = 4 if chips % 4 == 0 else 2 if chips % 2 == 0 else chips
        sizes.append(step)
        chips //= step
    return tuple(sizes) + (2,)


LEADS = (6, 5, 3, 1, 0)
TURNED_LEADS = (8, 7, 5, 1, 0)


def spread_leads(leads, hops):
    extra = hops - len(leads)
    return [leads[0] + extra - n for n in range(extra)] + list(leads)


class Plan:
    def __init__(self, count, rows, width, half, hidden, layers):
        self.count = count
        self.axes = factor_axes(count)
        strides = []
        stride = count
        for size in self.axes:
            stride //= size
            strides.append(stride)
        self.strides = tuple(strides)
        self.rows = rows
        self.width = width
        self.own = width // count
        self.block = -(-self.own // 16) * 16
        self.padded = self.block * count
        self.half = half
        self.pairs = half // LANES
        self.layers = layers
        self.ups = hidden // half
        self.units = 4 + 2 * self.ups
        self.quarter = HD // count
        self.bias_cols = 2 * half + hidden
        self.hops = tuple(1 if size == 2 else 3 for size in self.axes)
        self.slots = sum(self.hops)
        self.chunk = rows // 2
        self.early = TURN_EVERY - 1 if self.axes[:2] == (4, 2) else 0


def train_kernel(
    plan,
    frames_ref,
    cot_ref,
    shard_ref,
    small_ref,
    out_ref,
    gin_ref,
    gout_ref,
    smallg_ref,
    W,
    SB,
    VEC,
    BIAS,
    XS,
    XR,
    MID,
    ACC,
    LAST,
    HAT,
    INV,
    ACT,
    Q,
    K,
    V,
    LSE,
    CTX,
    SLOPE,
    HIDDEN,
    DX,
    LOW,
    FL,
    VG,
    BG,
    TURN,
    SG,
    RBs,
    RBt,
    RSs,
    ag_send,
    ag_recv,
    rs_send,
    rs_recv,
    x_send,
    x_recv,
):
    axes = plan.axes
    depth = len(axes)
    rp = plan.block
    Dp = plan.padded
    L = plan.layers
    NP = plan.units
    UP = plan.ups
    half = plan.half
    rows = plan.rows
    chunk = plan.chunk

    me = lax.axis_index("fsdp")
    side = lax.axis_index("tp")
    digit = [lax.rem(me // stride, size) for stride, size in zip(plan.strides, axes)]
    slot_of = [sum(plan.hops[:k]) for k in range(depth)]
    other = (me, 1 - side)

    def device(k, value):
        return (me + (value - digit[k]) * plan.strides[k], side)

    half_side = [d // 2 for d in digit]
    outer = [(d == 0) | (d == 3) for d in digit]
    inner = [jnp.logical_not(flag) for flag in outer]
    mine_in = [1 + s for s in half_side]
    mine_out = [3 * s for s in half_side]
    far_in = [2 - s for s in half_side]
    near = [pl.ds(2 * s, 2) for s in half_side]
    far = [pl.ds(2 * (1 - s), 2) for s in half_side]
    three = [pl.ds(1 - s, 3) for s in half_side]

    barrier = pltpu.get_barrier_semaphore()

    def greet(target):
        pl.semaphore_signal(barrier, inc=1, device_id=target, device_id_type=MESH)

    greet(other)
    greeted = 1
    for k in range(depth):
        if axes[k] == 2:
            greet(device(k, 1 - digit[k]))
        else:
            greet(device(k, jnp.where(outer[k], mine_in[k], mine_out[k])))
        greeted += 1
    for k in range(depth):
        if axes[k] == 4:

            @pl.when(inner[k])
            def _():
                greet(device(k, far_in[k]))

            greeted = greeted + jnp.where(inner[k], 1, 0)
    pl.semaphore_wait(barrier, greeted)

    def remote(src, dst, send, recv, target):
        return pltpu.make_async_remote_copy(
            src_ref=src,
            dst_ref=dst,
            send_sem=send,
            recv_sem=recv,
            device_id=target,
            device_id_type=MESH,
        )

    small_index = L * NP
    straight = tuple(range(depth))
    turned = (1, 0) + straight[2:]
    early = plan.early

    def gather_turned(unit):
        return lax.rem(unit, TURN_EVERY) == TURN_EVERY - 1

    def gather_order(unit):
        return turned if unit % TURN_EVERY == TURN_EVERY - 1 else straight

    def gather_copy(k, hop, unit, order, small, sending):
        done = order[: order.index(k)]

        def spot(value):
            return tuple(
                slice(None) if a in done else value if a == k else digit[a] for a in range(depth)
            )

        if axes[k] == 2:
            value = digit[k] if sending else 1 - digit[k]
            target = 1 - digit[k]
        elif hop == 0:
            value = digit[k] if sending else mine_out[k]
            target = mine_in[k]
        elif hop == 1:
            value = near[k] if sending else far[k]
            target = far_in[k]
        else:
            value = three[k]
            target = mine_out[k]
        dst = SB.at[spot(value)] if small else W.at[(unit,) + spot(value)]
        src = dst
        if sending and not done and hop == 0:
            src = small_ref if small else shard_ref.at[unit]
        slot = slot_of[k] + hop
        return remote(src, dst, ag_send.at[unit, slot], ag_recv.at[unit, slot], device(k, target))

    def early_copy(value, slot, unit, sending):
        own = value is digit[0]
        spot = (value, digit[1] if sending else 1 - digit[1]) + tuple(digit[2:])
        dst = W.at[(unit,) + spot]
        src = shard_ref.at[unit] if own and sending else dst
        target = device(1, 1 - digit[1])
        return remote(src, dst, ag_send.at[unit, slot], ag_recv.at[unit, slot], target)

    def early_own(unit, sending):
        return early_copy(digit[0], plan.slots, unit, sending)

    def early_rest(unit, sending, act):
        @pl.when(outer[0])
        def _():
            act(early_copy(three[0], slot_of[1], unit, sending))

        @pl.when(inner[0])
        def _():
            act(early_copy(mine_out[0], slot_of[1], unit, sending))
            act(early_copy(far[0], plan.slots + 1, unit, sending))

    def is_early(k, order, small):
        return bool(early) and k == 1 and order == straight and not small

    def gather_begin(k, unit, order, small):
        if is_early(k, order, small):

            @pl.when(unit < early)
            def _():
                early_rest(unit, True, lambda copy: copy.start())

            @pl.when(unit >= early)
            def _():
                gather_copy(k, 0, unit, order, small, True).start()

        elif axes[k] == 2:
            gather_copy(k, 0, unit, order, small, True).start()
        else:

            @pl.when(outer[k])
            def _():
                gather_copy(k, 0, unit, order, small, True).start()

    def gather_next(k, unit, order, small):
        position = order.index(k) + 1
        if position < depth:
            gather_begin(order[position], unit, order, small)

    def gather_hop(index, unit, order, small):
        for k in order:
            if index < plan.hops[k]:
                break
            index -= plan.hops[k]
        if axes[k] == 2:
            if is_early(k, order, small):

                @pl.when(unit < early)
                def _():
                    early_own(unit, False).wait_recv()
                    early_rest(unit, False, lambda copy: copy.wait_recv())

                @pl.when(unit >= early)
                def _():
                    gather_copy(k, 0, unit, order, small, False).wait_recv()

            else:
                gather_copy(k, 0, unit, order, small, False).wait_recv()
            gather_next(k, unit, order, small)
            return

        @pl.when(outer[k] if index == 2 else inner[k])
        def _():
            gather_copy(k, index, unit, order, small, False).wait_recv()
            if index < 2:
                gather_copy(k, index + 1, unit, order, small, True).start()
            if index > 0:
                gather_next(k, unit, order, small)

    def gather_drain(unit, order, small=False):
        for k in range(depth):
            for hop in range(plan.hops[k]):
                if is_early(k, order, small):

                    @pl.when(unit < early)
                    def _():
                        early_own(unit, True).wait_send()
                        early_rest(unit, True, lambda copy: copy.wait_send())

                    @pl.when(unit >= early)
                    def _():
                        gather_copy(k, hop, unit, order, small, True).wait_send()

                elif axes[k] == 2:
                    gather_copy(k, hop, unit, order, small, True).wait_send()
                else:

                    @pl.when(outer[k] if hop == 0 else inner[k])
                    def _():
                        gather_copy(k, hop, unit, order, small, True).wait_send()

    hops = plan.slots
    leads = spread_leads(LEADS, hops)
    turned_leads = spread_leads(TURNED_LEADS, hops)

    def gather_tick(n, carry=0):
        for index in range(hops):
            ahead = n + leads[index]
            inside = (ahead >= 0) & (ahead < L * NP)

            @pl.when(inside & jnp.logical_not(gather_turned(ahead)))
            def _():
                gather_hop(index, ahead, straight, False)

            further = n + turned_leads[index]
            inside = (further >= 0) & (further < L * NP)

            @pl.when(inside & gather_turned(further))
            def _():
                gather_hop(index, further, turned, False)

        return carry

    def ready(low, high):
        lax.fori_loop(low, high, gather_tick, 0)

    gather_begin(0, small_index, straight, True)
    for unit in range(L * NP):
        order = gather_order(unit)
        gather_begin(order[0], unit, order, False)
        if unit < early:
            early_own(unit, True).start()
    here = tuple(digit)
    SB[here] = small_ref[...]
    for unit in range(L * NP):
        W[(unit,) + here] = shard_ref[unit]
    before = max(max(leads), hops)
    for n in range(-before, 0):
        gather_tick(n)
        index = n + before
        if index < hops:
            gather_hop(index, small_index, straight, True)

    vec_all = SB[(slice(None),) * depth + (slice(0, rp), slice(None))]
    vec_rows = vec_all.reshape(Dp, LANES).astype(F32).T
    for layer in range(L):
        VEC[layer] = vec_rows[layer * VEC_ROWS : (layer + 1) * VEC_ROWS]
    every = L * plan.bias_cols
    shift = HD.bit_length() - 1

    def static_place(owner):
        return tuple((owner // stride) % size for stride, size in zip(plan.strides, axes))

    def column_ids(lines):
        return lax.broadcasted_iota(jnp.int32, (lines, every), 1)

    def line_ids(lines):
        return lax.broadcasted_iota(jnp.int32, (lines, every), 0)

    def group_match():
        return lax.shift_right_logical(column_ids(LANES), shift) == line_ids(LANES)

    def feature_match(lines):
        return (column_ids(lines) & (HD - 1)) == line_ids(lines)

    for owner in range(plan.count):
        held = SB[static_place(owner) + (slice(rp, rp + BIAS_ROWS), slice(None))].astype(F32)
        low = owner * plan.quarter
        TURN[low : low + plan.quarter] = held[0 : plan.quarter]
    spread = mm(TURN[0:HD].astype(BF), group_match().astype(F32).astype(BF), NN)
    bias_row = jnp.sum(jnp.where(feature_match(HD), spread, 0.0), axis=0, keepdims=True)
    for layer in range(L):
        BIAS[layer] = bias_row[:, layer * plan.bias_cols : (layer + 1) * plan.bias_cols]

    if plan.block != plan.own:
        column = lax.broadcasted_iota(jnp.int32, (1, Dp), 1)
        valid = (lax.rem(column, rp) < plan.own).astype(F32)
    else:
        valid = None

    def average(values):
        return jnp.sum(values, axis=-1, keepdims=True) * (1.0 / plan.width)

    def masked(values):
        return values if valid is None else values * valid

    def unit_of(index):
        return W[index].reshape(Dp, half)

    def pair_of(index):
        return jnp.concatenate([unit_of(index), unit_of(index + 1)], axis=1)

    def norm_forward(values, layer, which, region):
        centred = masked(values - average(values))
        inverse = lax.rsqrt(average(centred * centred) + norm_eps)
        hat = centred * inverse
        HAT[layer, which, region] = hat
        INV[layer, which, region] = inverse
        gain = VEC[layer, 2 * which : 2 * which + 1]
        shift = VEC[layer, 2 * which + 1 : 2 * which + 2]
        ACT[layer, which, region] = (hat * gain + shift).astype(BF)

    def exchange_copy(number, slot, part):
        region = pl.ds(part * chunk, chunk)
        return remote(
            XS.at[slot, region],
            XR.at[slot, region],
            x_send.at[number, part],
            x_recv.at[number, part],
            other,
        )

    def exchange_send(number, slot, part, values):
        XS[slot, pl.ds(part * chunk, chunk)] = values.astype(BF)
        exchange_copy(number, slot, part).start()

    def exchange_sum(number, slot, part):
        exchange_copy(number, slot, part).wait_recv()
        region = pl.ds(part * chunk, chunk)
        result = XS[slot, region].astype(F32) + XR[slot, region].astype(F32)
        return result

    def exchange_done(number, slot):
        for part in range(2):
            exchange_copy(number, slot, part).wait_send()

    lane = lax.broadcasted_iota(jnp.int32, (1, LANES), 1)
    head_mask = [((lane // HD) == h).astype(F32).astype(BF) for h in range(LANES // HD)]
    scale = HD ** (-0.5)
    clips = rows // SEQ

    def landing(k, order, unit):
        if k == depth - 1:
            return lax.rem(unit, NP)
        if k > 1:
            return unit
        m = production(unit)
        return m // TURN_EVERY if order == turned else m - m // TURN_EVERY - 1

    def production(unit):
        name = lax.rem(unit, NP)
        turn = jnp.where(
            name >= 4 + UP,
            name - 4 - UP,
            jnp.where(name >= 4, name - 4 + UP, NP - 1 - name),
        )
        return (L - 1 - unit // NP) * NP + turn

    def land(k, order, slots):
        done = order[order.index(k) + 1 :]
        return tuple(slots if a == k else slice(None) for a in range(depth) if a not in done)

    def landing_ref(k, order):
        return RBt[k] if order == turned and k < 2 else RBs[k]

    def scatter_spot(k, order, value):
        done = order[order.index(k) + 1 :]
        return tuple(
            digit[a] if a in done else value if a == k else slice(None) for a in range(depth)
        )

    def scatter_copy(k, hop, unit, order, small):
        if axes[k] == 2:
            value, target, slots = 1 - digit[k], 1 - digit[k], 0
        elif hop == 0:
            value, target, slots = three[k], mine_in[k], pl.ds(0, 3)
        elif hop == 1:
            value, target, slots = far[k], far_in[k], pl.ds(3, 2)
        else:
            value, target, slots = mine_out[k], mine_out[k], 0
        spot = scatter_spot(k, order, value)
        if small:
            src, dst = SG.at[spot], RSs[k].at[land(k, order, slots)]
        else:
            src, dst = W.at[(unit,) + spot], landing_ref(k, order).at[(landing(k, order, unit),) + land(k, order, slots)]
        slot = slot_of[k] + hop
        return remote(src, dst, rs_send.at[unit, slot], rs_recv.at[unit, slot], device(k, target))

    def scatter_begin(k, unit, order, small=False):
        if axes[k] == 2:
            scatter_copy(k, 0, unit, order, small).start()
        else:

            @pl.when(outer[k])
            def _():
                scatter_copy(k, 0, unit, order, small).start()

    def held(small, unit, spot):
        return SG[spot] if small else W[(unit,) + spot].astype(F32)

    def arrived(k, order, small, unit, slots):
        if small:
            return RSs[k][land(k, order, slots)]
        spot = (landing(k, order, unit),) + land(k, order, slots)
        return landing_ref(k, order)[spot].astype(F32)

    def keep(small, unit, spot, value):
        if small:
            SG[spot] = value
        else:
            W[(unit,) + spot] = value.astype(BF)

    def finish(k, unit, order, small, slots):
        spot = scatter_spot(k, order, digit[k])
        value = held(small, unit, spot) + arrived(k, order, small, unit, slots)
        position = order.index(k)
        if position > 0:
            keep(small, unit, spot, value)
            scatter_begin(order[position - 1], unit, order, small)
        elif small:
            smallg_ref[...] = value
        else:
            gout_ref[unit] = value

    def add_in(k, unit, order, small, value, slots):
        spot = scatter_spot(k, order, value)
        keep(small, unit, spot, held(small, unit, spot) + arrived(k, order, small, unit, slots))

    def scatter_hop(index, unit, order, small=False):
        for k in reversed(order):
            if index < plan.hops[k]:
                break
            index -= plan.hops[k]
        if axes[k] == 2:
            scatter_copy(k, 0, unit, order, small).wait_recv()
            finish(k, unit, order, small, 0)
            return

        @pl.when(outer[k] if index == 2 else inner[k])
        def _():
            scatter_copy(k, index, unit, order, small).wait_recv()
            if index == 0:
                add_in(k, unit, order, small, three[k], pl.ds(0, 3))
                scatter_copy(k, 1, unit, order, small).start()
            elif index == 1:
                add_in(k, unit, order, small, mine_out[k], 3 + mine_out[k] - 2 * half_side[k])
                scatter_copy(k, 2, unit, order, small).start()
                finish(k, unit, order, small, 3 + digit[k] - 2 * half_side[k])
            else:
                finish(k, unit, order, small, 0)

    def scatter_drain(unit, order, small=False):
        for k in range(depth):
            for hop in range(plan.hops[k]):
                if axes[k] == 2:
                    scatter_copy(k, hop, unit, order, small).wait_send()
                else:

                    @pl.when(outer[k] if hop == 0 else inner[k])
                    def _():
                        scatter_copy(k, hop, unit, order, small).wait_send()

    block_shape = axes + (rp,)

    def put_gradient(index, value):
        W[index] = value.astype(BF).reshape(block_shape + (half,))
        scatter_begin(depth - 1, index, straight)

    def put_pair(index, value):
        put_gradient(index, value[:, :half])
        put_gradient(index + 1, value[:, half:])

    def column_sum(values):
        return jnp.sum(values, axis=0, keepdims=True)

    def drain_down(unit):
        for order in (straight, turned):

            @pl.when(gather_turned(unit) == (order == turned))
            def _():
                gather_drain(unit, order)

    def down_gradient(layer, number):
        down = layer * NP + 4 + UP
        grad = mm(LOW[...], pair_of(down + number), NN) * SLOPE[layer, number // 2].astype(F32)
        low = (2 + number) * half
        BG[layer, :, low : low + 2 * half] = column_sum(grad)
        FL[number // 2] = grad.astype(BF)
        put_pair(down + number, mm(LOW[...], HIDDEN[layer, number // 2], TN))

    LOW[...] = cot_ref[...]
    VG[...] = jnp.zeros(VG.shape, F32)
    SG[...] = jnp.zeros(SG.shape, F32)

    def attend(layer):
        def one(item, _):
            pair = item // clips
            clip = lax.rem(item, clips)
            span = pl.ds(clip * SEQ, SEQ)
            query = Q[layer, pair, span]
            key = K[layer, pair, span]
            value = V[layer, pair, span]
            total = None
            for h, mask in enumerate(head_mask):
                scores = mm(query * mask, key, NT) * scale
                highest = jnp.max(scores, axis=1, keepdims=True)
                logsum = highest + jnp.log(jnp.sum(jnp.exp(scores - highest), axis=1, keepdims=True))
                kept = logsum if h == 0 else jnp.where(lane < h * HD, kept, logsum)
                weights = jnp.exp(scores - logsum).astype(BF)
                part = mm(weights, value * mask, NN)
                total = part if total is None else total + part
            LSE[layer, pair, span] = jnp.broadcast_to(kept, (SEQ, LANES))
            CTX[layer, pair, span] = total.astype(BF)
            return 0

        lax.fori_loop(0, plan.pairs * clips, one, 0)

    def context_of(layer, region=slice(None)):
        return jnp.concatenate([CTX[layer, pair, region] for pair in range(plan.pairs)], axis=1)

    def forward_layer(layer, carry):
        first = layer * NP
        up = first + 4
        down = up + UP

        @pl.when(layer == 0)
        def _():
            value = frames_ref[...].astype(F32)
            DX[...] = value
            norm_forward(value, layer, 0, slice(None))

        ready(first, first + 2)

        @pl.when(layer > 0)
        def _():
            for part in range(2):
                region = pl.ds(part * chunk, chunk)
                value = MID[region] + exchange_sum(2 * layer - 1, 1, part) + VEC[layer - 1, 5:6]
                DX[region] = value
                norm_forward(value, layer, 0, region)
            exchange_done(2 * layer - 1, 1)

        both = mm(ACT[layer, 0], pair_of(first), NN)
        for pair in range(plan.pairs):
            low = pair * LANES
            query = both[:, low : low + LANES] + BIAS[layer, :, low : low + LANES]
            Q[layer, pair] = query.astype(BF)
            K[layer, pair] = both[:, half + low : half + low + LANES].astype(BF)
        ready(first + 2, first + 3)
        values = mm(ACT[layer, 0], unit_of(first + 2), NN)
        for pair in range(plan.pairs):
            low = pair * LANES
            bias = BIAS[layer, :, half + low : half + low + LANES]
            V[layer, pair] = (values[:, low : low + LANES] + bias).astype(BF)
        attend(layer)
        ready(first + 3, first + 4)
        for part in range(2):
            region = pl.ds(part * chunk, chunk)
            heads = context_of(layer, region)
            exchange_send(2 * layer, 0, part, mm(heads, unit_of(first + 3), NT))
        ready(up, up + UP)
        for part in range(2):
            region = pl.ds(part * chunk, chunk)
            value = DX[region] + exchange_sum(2 * layer, 0, part) + VEC[layer, 4:5]
            MID[region] = value
            norm_forward(value, layer, 1, region)
        exchange_done(2 * layer, 0)
        for number in range(0, UP, 2):
            before = mm(ACT[layer, 1], pair_of(up + number), NN)
            low = (2 + number) * half
            before = before + BIAS[layer, :, low : low + 2 * half]
            bell = 0.5 * (1.0 + lax.erf(before * root_half))
            HIDDEN[layer, number // 2] = (before * bell).astype(BF)
            slope = bell + before * jnp.exp(-0.5 * before * before) * inv_root_two_pi
            SLOPE[layer, number // 2] = slope.astype(BF)
        for number in range(0, UP, 2):
            ready(down + number, down + number + 2)
            term = mm(HIDDEN[layer, number // 2], pair_of(down + number), NT)
            if number + 2 < UP:
                ACC[...] = term if number == 0 else ACC[...] + term
            else:
                whole = term + ACC[...] if UP > 2 else term

                @pl.when(layer + 1 < L)
                def _():
                    for part in range(2):
                        exchange_send(2 * layer + 1, 1, part, whole[part * chunk : (part + 1) * chunk])

                @pl.when(layer + 1 == L)
                def _():
                    LAST[...] = whole.astype(BF)

            @pl.when(layer + 1 == L)
            def _():
                for unit in (down + number, down + number + 1):
                    drain_down(unit)
                down_gradient(layer, number)

        return carry

    lax.fori_loop(0, L, forward_layer, 0)

    def attend_back(layer):
        def one(item, _):
            pair = item // clips
            clip = lax.rem(item, clips)
            span = pl.ds(clip * SEQ, SEQ)
            query = Q[layer, pair, span]
            key = K[layer, pair, span]
            value = V[layer, pair, span]
            upper = FL[1, span, pl.ds(pl.multiple_of(half + pair * LANES, LANES), LANES)]
            logsums = LSE[layer, pair, span]
            grad_q = grad_k = grad_v = None
            for h, mask in enumerate(head_mask):
                scores = mm(query * mask, key, NT) * scale
                probs = jnp.exp(scores - logsums[:, h * HD : h * HD + 1])
                weights = probs.astype(BF)
                up_head = upper * mask
                part_v = mm(weights, up_head, TN)
                grad_p = mm(up_head, value, NT)
                inner = jnp.sum(probs * grad_p, axis=1, keepdims=True)
                grad_s = (probs * (grad_p - inner) * scale).astype(BF)
                part_q = mm(grad_s, key * mask, NN)
                part_k = mm(grad_s, query * mask, TN)
                grad_q = part_q if grad_q is None else grad_q + part_q
                grad_k = part_k if grad_k is None else grad_k + part_k
                grad_v = part_v if grad_v is None else grad_v + part_v
            low = pl.ds(pl.multiple_of(pair * LANES, LANES), LANES)
            next_low = pl.ds(pl.multiple_of(half + pair * LANES, LANES), LANES)
            FL[0, span, low] = grad_q.astype(BF)
            FL[0, span, next_low] = grad_k.astype(BF)
            FL[1, span, low] = grad_v.astype(BF)
            sum_q = jnp.sum(grad_q, axis=0, keepdims=True)
            sum_v = jnp.sum(grad_v, axis=0, keepdims=True)

            @pl.when(clip == 0)
            def _():
                BG[layer, :, low] = sum_q
                BG[layer, :, next_low] = sum_v

            @pl.when(clip > 0)
            def _():
                BG[layer, :, low] += sum_q
                BG[layer, :, next_low] += sum_v

            return 0

        lax.fori_loop(0, plan.pairs * clips, one, 0)

    def norm_backward(upper, layer, which, region):
        hat = HAT[layer, which, region]
        scaled = upper * VEC[layer, 2 * which : 2 * which + 1]
        return INV[layer, which, region] * (
            masked(scaled - average(scaled)) - hat * average(scaled * hat)
        )

    def keep_rows(layer, line, part, value):
        if part == 0:
            VG[layer, line : line + 1] = value
        else:
            VG[layer, line : line + 1] += value

    DX[...] = cot_ref[...].astype(F32)
    VG[L - 1, 5:6] = column_sum(DX[...])
    DMID = ACC
    for unit in range((L - 1) * NP + 4 + UP):
        gather_drain(unit, gather_order(unit))
    gather_drain(small_index, straight, True)

    def produced(m):
        turn = lax.rem(m, NP)
        name = jnp.where(
            turn < UP,
            4 + UP + turn,
            jnp.where(turn < 2 * UP, 4 + turn - UP, NP - 1 - turn),
        )
        return (L - 1 - m // NP) * NP + name

    def pumped(step, place, index):
        counts = [row[min(index - 1, len(row) - 1)] - max(0, index - len(row)) for row in PUMPS[place]]
        value = counts[0]
        for s in range(1, L):
            value = jnp.where(step == s, counts[min(s, len(counts) - 1)], value)
        return jnp.clip(value, 0, L * NP)

    def scatter_either(index, m):
        unit = produced(m)

        @pl.when(lax.rem(m, TURN_EVERY) != 0)
        def _():
            scatter_hop(index, unit, straight)

        @pl.when(lax.rem(m, TURN_EVERY) == 0)
        def _():
            scatter_hop(index, unit, turned)

    def pump_between(lows, highs):
        length = functools.reduce(jnp.maximum, [high - low for low, high in zip(lows, highs)])

        def one(t, carry):
            for index in range(1, hops):
                m = lows[index - 1] + t

                @pl.when(m < highs[index - 1])
                def _():
                    scatter_either(index, m)

            return carry

        lax.fori_loop(0, length, one, 0)

    def pump_to(step, place):
        if place == 0:
            before = [
                jnp.where(step == 0, 0, pumped(step - 1, len(PUMPS) - 1, index)) for index in range(1, hops)
            ]
        else:
            before = [pumped(step, place - 1, index) for index in range(1, hops)]
        pump_between(before, [pumped(step, place, index) for index in range(1, hops)])

    def rest_order():
        last = [row[-1] for row in PUMPS][-1]
        done = [min(last[min(index, 4) - 1], L * NP) for index in range(1, 5)]
        done += [0] * (hops - 5)
        if hops == 5 and sum(done) + len(REST) == 4 * L * NP:
            given = list(REST)
        else:
            done = [max(0, min(done[min(index, 4) - 1] - max(0, index - 4), L * NP)) for index in range(1, hops)]
            left = [(m + 2 * index, index) for index in range(1, hops) for m in range(done[index - 1], L * NP)]
            given = [index for _, index in sorted(left)]
        events = []
        for index in given:
            events.append((index, done[index - 1]))
            done[index - 1] += 1
        return events

    def pump_rest():
        for index, m in rest_order():
            name = m % NP
            name = 4 + UP + name if name < UP else 4 + name - UP if name < 2 * UP else NP - 1 - name
            unit = (L - 1 - m // NP) * NP + name
            scatter_hop(index, unit, turned if m % TURN_EVERY == 0 else straight)
            if m == L * NP - 1:
                scatter_hop(index, small_index, straight, True)

    def backward_layer(step, carry):
        layer = L - 1 - step
        first = layer * NP
        up = first + 4
        down = up + UP
        number_up = 2 * L + 2 * step

        def from_core(low, high):
            for n in range(low, high):
                turn = n - 4 - UP if n >= 4 + UP else n - 4 + UP if n >= 4 else NP - 1 - n
                scatter_hop(0, first + n, turned if turn % TURN_EVERY == 0 else straight)

        for part in range(2):
            from_core(4 + UP + part * UP // 2, 4 + UP + (part + 1) * UP // 2)
            region = pl.ds(part * chunk, chunk)
            whole = None
            for number in range(0, UP, 2):
                term = mm(FL[number // 2, region], pair_of(up + number), NT)
                whole = term if whole is None else whole + term
            exchange_send(number_up, 1, part, whole)
        pump_to(step, 0)
        for number in range(0, UP, 2):
            put_pair(up + number, mm(ACT[layer, 1], FL[number // 2], TN))
        from_core(4, 4 + UP)
        pump_to(step, 1)
        for part in range(2):
            region = pl.ds(part * chunk, chunk)
            grad = exchange_sum(number_up, 1, part)
            keep_rows(layer, 2, part, column_sum(grad * HAT[layer, 1, region]))
            keep_rows(layer, 3, part, column_sum(grad))
            grad_mid = DX[region] + norm_backward(grad, layer, 1, region)
            DMID[region] = grad_mid
            keep_rows(layer, 4, part, column_sum(grad_mid))
            LOW[region] = grad_mid.astype(BF)
        exchange_done(number_up, 1)
        heads = mm(LOW[...], unit_of(first + 3), NN)
        FL[1, :, half : 2 * half] = heads.astype(BF)
        put_gradient(first + 3, mm(LOW[...], context_of(layer), TN))
        pump_to(step, 2)
        attend_back(layer)
        for part in range(2):
            region = pl.ds(part * chunk, chunk)
            whole = mm(FL[0, region], pair_of(first), NT)
            whole = whole + mm(FL[1, region, 0:half], unit_of(first + 2), NT)
            exchange_send(number_up + 1, 0, part, whole)
        from_core(3, 4)
        pump_to(step, 3)
        put_gradient(first + 2, mm(ACT[layer, 0], FL[1, :, 0:half], TN))
        grad_qk = mm(ACT[layer, 0], FL[0], TN)
        put_gradient(first + 1, grad_qk[:, half:])
        put_gradient(first, grad_qk[:, :half])
        for n in (2, 1, 0):
            from_core(n, n + 1)
        pump_to(step, 4)

        @pl.when(step + 1 == L)
        def _():
            pack_biases()

        for part in range(2):
            region = pl.ds(part * chunk, chunk)
            grad = exchange_sum(number_up + 1, 0, part)
            keep_rows(layer, 0, part, column_sum(grad * HAT[layer, 0, region]))
            keep_rows(layer, 1, part, column_sum(grad))
            upper = DMID[region] + norm_backward(grad, layer, 0, region)
            DX[region] = upper
            LOW[region] = upper.astype(BF)
        exchange_done(number_up + 1, 0)

        @pl.when(step + 1 < L)
        def _():
            VG[layer - 1, 5:6] = column_sum(DX[...])
            for number in range(0, UP, 2):
                down_gradient(layer - 1, number)

        return carry

    def pack_biases():
        row = jnp.concatenate([BG[layer] for layer in range(L)], axis=1)
        wide = jnp.where(group_match(), row, 0.0)
        high = wide.astype(BF)
        low = (wide - high.astype(F32)).astype(BF)
        select = feature_match(LANES).astype(F32).astype(BF)
        table = (mm(high, select, NT) + mm(low, select, NT)).T
        for owner in range(plan.count):
            start = owner * plan.quarter
            spot = static_place(owner) + (slice(rp, rp + plan.quarter), slice(None))
            SG[spot] = table[start : start + plan.quarter]

    lax.fori_loop(0, L, backward_layer, 0)

    lines = [VG[layer] for layer in range(L)]
    lines.append(jnp.zeros((LANES - L * VEC_ROWS, Dp), F32))
    columns = jnp.concatenate(lines, axis=0).T.reshape(axes + (rp, LANES))
    SG[(slice(None),) * depth + (slice(0, rp), slice(None))] = columns
    scatter_begin(depth - 1, small_index, straight, True)
    for part in range(2):
        exchange_send(2 * L - 1, 1, part, LAST[pl.ds(part * chunk, chunk)])
    gin_ref[...] = DX[...]
    scatter_hop(0, small_index, straight, True)
    pump_rest()
    for part in range(2):
        region = pl.ds(part * chunk, chunk)
        value = MID[region] + exchange_sum(2 * L - 1, 1, part) + VEC[L - 1, 5:6]
        out_ref[region] = value.astype(BF)
    exchange_done(2 * L - 1, 1)
    for unit in range(L * NP):
        name = unit % NP
        turn = name - 4 - UP if name >= 4 + UP else name - 4 + UP if name >= 4 else NP - 1 - name
        scatter_drain(unit, turned if turn % TURN_EVERY == 0 else straight)
    scatter_drain(small_index, straight, True)


PUMPS = (
    ((0, 0, 0, 0), (12, 8, 5, 1)),
    ((2, 0, 0, 0), (14, 9, 8, 1)),
    ((4, 1, 0, 0), (16, 11, 8, 6)),
    ((7, 3, 1, 0), (18, 13, 11, 6)),
    ((8, 5, 1, 0), (20, 14, 13, 9)),
)
REST = (
    1, 1, 2, 2, 2, 3, 4, 4, 4, 1, 2, 2, 2, 3, 3, 2, 3, 2, 3, 2, 1, 4, 4, 3,
    3, 3, 2, 3, 4, 3, 4, 4, 4, 4, 3, 4, 4, 4, 4, 4,
)


def run_kernel(plan, frames, cotangent, shards, small):
    L, NP, Dp, rp, rows = plan.layers, plan.units, plan.padded, plan.block, plan.rows
    axes = plan.axes
    depth = len(axes)
    half = plan.half
    UP = plan.ups // 2
    piece = 2 * half
    landings = []
    small_landings = []
    for k, size in enumerate(axes):
        turned_number = -(-L * NP // TURN_EVERY)
        number = NP if k == depth - 1 else L * NP - turned_number if k < 2 else L * NP
        slots = 1 if size == 2 else 5
        landings.append(pltpu.VMEM((number,) + axes[:k] + (slots, rp, half), BF))
        small_landings.append(pltpu.VMEM(axes[:k] + (slots, rp + BIAS_ROWS, LANES), F32))
    turned_landings = [
        pltpu.VMEM((-(-L * NP // TURN_EVERY), 1 if axes[0] == 2 else 5, axes[1], rp, half), BF),
        pltpu.VMEM((-(-L * NP // TURN_EVERY), 1 if axes[1] == 2 else 5, rp, half), BF),
    ]
    scratch = [
        pltpu.VMEM((L * NP,) + axes + (rp, half), BF),
        pltpu.VMEM(axes + (rp + BIAS_ROWS, LANES), BF),
        pltpu.VMEM((L, VEC_ROWS, Dp), F32),
        pltpu.VMEM((L, 1, plan.bias_cols), F32),
        pltpu.VMEM((2, rows, Dp), BF),
        pltpu.VMEM((2, rows, Dp), BF),
        pltpu.VMEM((rows, Dp), F32),
        pltpu.VMEM((rows, Dp), F32),
        pltpu.VMEM((rows, Dp), BF),
        pltpu.VMEM((L, 2, rows, Dp), F32),
        pltpu.VMEM((L, 2, rows, 1), F32),
        pltpu.VMEM((L, 2, rows, Dp), BF),
        pltpu.VMEM((L, plan.pairs, rows, LANES), BF),
        pltpu.VMEM((L, plan.pairs, rows, LANES), BF),
        pltpu.VMEM((L, plan.pairs, rows, LANES), BF),
        pltpu.VMEM((L, plan.pairs, rows, LANES), F32),
        pltpu.VMEM((L, plan.pairs, rows, LANES), BF),
        pltpu.VMEM((L, UP, rows, piece), BF),
        pltpu.VMEM((L, UP, rows, piece), BF),
        pltpu.VMEM((rows, Dp), F32),
        pltpu.VMEM((rows, Dp), BF),
        pltpu.VMEM((UP, rows, piece), BF),
        pltpu.VMEM((L, VEC_ROWS, Dp), F32),
        pltpu.VMEM((L, 1, plan.bias_cols), F32),
        pltpu.VMEM((HD, LANES), F32),
        pltpu.VMEM(axes + (rp + BIAS_ROWS, LANES), F32),
        landings,
        turned_landings,
        small_landings,
        pltpu.SemaphoreType.DMA((L * NP + 1, plan.slots + (2 if plan.early else 0))),
        pltpu.SemaphoreType.DMA((L * NP + 1, plan.slots + (2 if plan.early else 0))),
        pltpu.SemaphoreType.DMA((L * NP + 1, plan.slots)),
        pltpu.SemaphoreType.DMA((L * NP + 1, plan.slots)),
        pltpu.SemaphoreType.DMA((4 * L, 2)),
        pltpu.SemaphoreType.DMA((4 * L, 2)),
    ]
    return pl.pallas_call(
        functools.partial(train_kernel, plan),
        out_shape=(
            jax.ShapeDtypeStruct((rows, Dp), BF),
            jax.ShapeDtypeStruct((rows, Dp), F32),
            jax.ShapeDtypeStruct((L * NP, rp, half), F32),
            jax.ShapeDtypeStruct((rp + BIAS_ROWS, LANES), F32),
        ),
        in_specs=[pl.BlockSpec(memory_space=pltpu.VMEM)] * 4,
        out_specs=tuple([pl.BlockSpec(memory_space=pltpu.VMEM)] * 4),
        scratch_shapes=scratch,
        compiler_params=pltpu.CompilerParams(
            collective_id=0, has_side_effects=True, vmem_limit_bytes=67043328
        ),
        name="train_step",
    )(frames, cotangent, shards, small)


def adamw(weight, gradient, first, second, rate, decay):
    first_new = beta_one * first + (1.0 - beta_one) * gradient
    second_new = beta_two * second + (1.0 - beta_two) * gradient * gradient
    first_hat = first_new / (1.0 - beta_one**STEP)
    second_hat = second_new / (1.0 - beta_two**STEP)
    weight_new = weight - rate * (first_hat / (jnp.sqrt(second_hat) + adam_eps) + decay * weight)
    return (weight_new, first_new, second_new)


def pad_axis(values, axis, size):
    widths = [(0, 0)] * values.ndim
    widths[axis] = (0, size - values.shape[axis])
    return jnp.pad(values, widths)


def on_device(count, frames, cotangent, *tensors):
    masters, firsts, seconds = tensors[:7], tensors[7:14], tensors[14:21]
    w_qkv, w_out, w_up, w_down, b_qv, b_up, vectors = masters
    L = w_qkv.shape[0]
    rows, width = frames.shape
    half = w_qkv.shape[3]
    hidden = w_up.shape[2]
    plan = Plan(count, rows, width, half, hidden, L)
    own, rp, UP = plan.own, plan.block, plan.ups

    def spread_features(values):
        if rp == own:
            return values
        return pad_axis(values.reshape(rows, count, own), 2, rp).reshape(rows, plan.padded)

    def gather_features(values):
        if rp == own:
            return values
        return values.reshape(rows, count, rp)[:, :, :own].reshape(rows, width)

    low_qkv = w_qkv.astype(BF).reshape(L, own, 3 * half)
    low_out = w_out.astype(BF).transpose(0, 2, 1)
    low_up = w_up.astype(BF)
    low_down = w_down.astype(BF).transpose(0, 2, 1)
    parts = [low_qkv[:, :, n * half : (n + 1) * half] for n in range(3)] + [low_out]
    parts += [low_up[:, :, n * half : (n + 1) * half] for n in range(UP)]
    parts += [low_down[:, :, n * half : (n + 1) * half] for n in range(UP)]
    shards = jnp.stack(parts, axis=1).reshape(L * plan.units, own, half)
    shards = pad_axis(shards, 1, rp)

    quarter = plan.quarter
    vec_part = pad_axis(vectors.astype(BF).transpose(2, 0, 1), 2, VEC_ROWS).reshape(own, L * VEC_ROWS)
    bias_part = jnp.concatenate(
        [b_qv.astype(BF).reshape(L, -1, quarter), b_up.astype(BF).reshape(L, -1, quarter)], axis=1
    )
    groups = bias_part.shape[1]
    bias_part = bias_part.transpose(2, 0, 1).reshape(quarter, L * groups)
    small = jnp.concatenate(
        [
            pad_axis(pad_axis(vec_part, 1, LANES), 0, rp),
            pad_axis(pad_axis(bias_part, 1, LANES), 0, BIAS_ROWS),
        ],
        axis=0,
    )

    output, grad_input, wide, small_grad = run_kernel(
        plan, spread_features(frames), spread_features(cotangent), shards, small
    )

    wide = wide.reshape(L, plan.units, rp, half)[:, :, :own]
    grad_qkv = jnp.stack([wide[:, n] for n in range(3)], axis=2)
    grad_out = wide[:, 3].transpose(0, 2, 1)
    grad_up = jnp.concatenate([wide[:, 4 + n] for n in range(UP)], axis=2)
    grad_down = jnp.concatenate([wide[:, 4 + UP + n] for n in range(UP)], axis=2).transpose(0, 2, 1)
    vec_grad = small_grad[:own, : L * VEC_ROWS].reshape(own, L, VEC_ROWS)[:, :, : vectors.shape[1]]
    grad_vec = vec_grad.transpose(1, 2, 0)
    bias_grad = small_grad[rp : rp + quarter, : L * groups].reshape(quarter, L, groups)
    bias_grad = bias_grad.transpose(1, 2, 0)
    split = b_qv.shape[1] * b_qv.shape[2]
    grad_bqv = bias_grad[:, :split].reshape(b_qv.shape)
    grad_bup = bias_grad[:, split:]
    grads = (grad_qkv, grad_out, grad_up, grad_down, grad_bqv, grad_bup, grad_vec)
    rates = (rate_matrix,) * 4 + (rate_vector,) * 3
    decays = (decay_rate,) * 4 + (0.0,) * 3
    updated = [
        adamw(masters[n], grads[n], firsts[n], seconds[n], rates[n], decays[n]) for n in range(7)
    ]
    return (
        (gather_features(output), gather_features(grad_input))
        + grads
        + tuple(updated[n][0] for n in range(7))
        + tuple(updated[n][1] for n in range(7))
        + tuple(updated[n][2] for n in range(7))
    )


def solution(mesh):
    tensors = (
        P(None, "fsdp", None, "tp"),
        P(None, "tp", "fsdp"),
        P(None, "fsdp", "tp"),
        P(None, "tp", "fsdp"),
        P(None, None, "tp", "fsdp"),
        P(None, "tp", "fsdp"),
        P(None, None, "fsdp"),
    )
    rows = (P("fsdp", None), P("fsdp", None))
    return jax.shard_map(
        functools.partial(on_device, mesh.shape["fsdp"]),
        mesh=mesh,
        in_specs=rows + tensors * 3,
        out_specs=rows + tensors * 4,
        check_vma=False,
    )
```

```python
import functools
import jax
import jax.numpy as jnp
from jax import lax
from jax.experimental import pallas as pl
from jax.experimental.pallas import tpu as pltpu
from jax.sharding import PartitionSpec as P

HD = 64
SEQ = 256
STEP = 3

norm_eps = 1e-05
beta_one = 0.9
beta_two = 0.999
adam_eps = 1e-08
decay_rate = 0.1
rate_matrix = 0.01
rate_vector = 0.2
root_half = 0.7071067811865476
inv_root_two_pi = 0.3989422804014327

BF = jnp.bfloat16
F32 = jnp.float32
NN = (((1,), (0,)), ((), ()))
NT = (((1,), (1,)), ((), ()))
TN = (((0,), (0,)), ((), ()))
MESH = pl.DeviceIdType.MESH
LANES = 128
BIAS_ROWS = 16
TURN_EVERY = 6
VEC_ROWS = 8


def mm(left, right, dims):
    return lax.dot_general(left, right, dims, preferred_element_type=F32)


def factor_axes(count):
    chips = count // 2
    sizes = []
    while chips > 1:
        step = 4 if chips % 4 == 0 else 2 if chips % 2 == 0 else chips
        sizes.append(step)
        chips //= step
    return tuple(sizes) + (2,)


LEADS = (7, 5, 4, 2, 0)
EARLY = 12


def spread_leads(leads, hops):
    extra = hops - len(leads)
    return [leads[0] + extra - n for n in range(extra)] + list(leads)


class Plan:
    def __init__(self, count, rows, width, half, hidden, layers):
        self.count = count
        self.axes = factor_axes(count)
        strides = []
        stride = count
        for size in self.axes:
            stride //= size
            strides.append(stride)
        self.strides = tuple(strides)
        self.rows = rows
        self.width = width
        self.own = width // count
        self.block = -(-self.own // 16) * 16
        self.padded = self.block * count
        self.half = half
        self.pairs = half // LANES
        self.layers = layers
        self.ups = hidden // half
        self.units = 4 + 2 * self.ups
        self.quarter = HD // count
        self.bias_cols = 2 * half + hidden
        self.hops = tuple(1 if size == 2 else 3 for size in self.axes)
        self.slots = sum(self.hops)
        self.chunk = rows // 2
        self.early = EARLY if self.axes[:2] == (4, 2) else 0


def train_kernel(
    plan,
    frames_ref,
    cot_ref,
    shard_ref,
    small_ref,
    out_ref,
    gin_ref,
    gout_ref,
    smallg_ref,
    W,
    SB,
    VEC,
    BIAS,
    XS,
    XR,
    MID,
    ACC,
    LAST,
    HAT,
    INV,
    ACT,
    Q,
    K,
    V,
    LSE,
    CTX,
    SLOPE,
    HIDDEN,
    DX,
    LOW,
    FL,
    VG,
    BG,
    TURN,
    SG,
    RBs,
    RBt,
    RSs,
    ag_send,
    ag_recv,
    rs_send,
    rs_recv,
    x_send,
    x_recv,
    GO,
    OUT,
    go_sem,
):
    axes = plan.axes
    depth = len(axes)
    rp = plan.block
    Dp = plan.padded
    L = plan.layers
    NP = plan.units
    UP = plan.ups
    half = plan.half
    rows = plan.rows
    chunk = plan.chunk

    me = lax.axis_index("fsdp")
    side = lax.axis_index("tp")
    digit = [lax.rem(me // stride, size) for stride, size in zip(plan.strides, axes)]
    slot_of = [sum(plan.hops[:k]) for k in range(depth)]
    other = (me, 1 - side)

    def device(k, value):
        return (me + (value - digit[k]) * plan.strides[k], side)

    half_side = [d // 2 for d in digit]
    outer = [(d == 0) | (d == 3) for d in digit]
    inner = [jnp.logical_not(flag) for flag in outer]
    mine_in = [1 + s for s in half_side]
    mine_out = [3 * s for s in half_side]
    far_in = [2 - s for s in half_side]
    near = [pl.ds(2 * s, 2) for s in half_side]
    far = [pl.ds(2 * (1 - s), 2) for s in half_side]
    three = [pl.ds(1 - s, 3) for s in half_side]

    barrier = pltpu.get_barrier_semaphore()

    def greet(target):
        pl.semaphore_signal(barrier, inc=1, device_id=target, device_id_type=MESH)

    greet(other)
    greeted = 1
    for k in range(depth):
        if axes[k] == 2:
            greet(device(k, 1 - digit[k]))
        else:
            greet(device(k, jnp.where(outer[k], mine_in[k], mine_out[k])))
        greeted += 1
    for k in range(depth):
        if axes[k] == 4:

            @pl.when(inner[k])
            def _():
                greet(device(k, far_in[k]))

            greeted = greeted + jnp.where(inner[k], 1, 0)
    pl.semaphore_wait(barrier, greeted)

    def remote(src, dst, send, recv, target):
        return pltpu.make_async_remote_copy(
            src_ref=src,
            dst_ref=dst,
            send_sem=send,
            recv_sem=recv,
            device_id=target,
            device_id_type=MESH,
        )

    small_index = L * NP
    straight = tuple(range(depth))
    turned = (1, 0) + straight[2:]
    early = plan.early

    def gather_copy(k, hop, unit, order, small, sending):
        done = order[: order.index(k)]

        def spot(value):
            return tuple(
                slice(None) if a in done else value if a == k else digit[a] for a in range(depth)
            )

        if axes[k] == 2:
            value = digit[k] if sending else 1 - digit[k]
            target = 1 - digit[k]
        elif hop == 0:
            value = digit[k] if sending else mine_out[k]
            target = mine_in[k]
        elif hop == 1:
            value = near[k] if sending else far[k]
            target = far_in[k]
        else:
            value = three[k]
            target = mine_out[k]
        dst = SB.at[spot(value)] if small else W.at[(unit,) + spot(value)]
        src = dst
        if sending and not done and hop == 0:
            src = small_ref if small else shard_ref.at[unit]
        slot = slot_of[k] + hop
        return remote(src, dst, ag_send.at[unit, slot], ag_recv.at[unit, slot], device(k, target))

    def early_copy(value, slot, unit, sending):
        own = value is digit[0]
        spot = (value, digit[1] if sending else 1 - digit[1]) + tuple(digit[2:])
        dst = W.at[(unit,) + spot]
        src = shard_ref.at[unit] if own and sending else dst
        target = device(1, 1 - digit[1])
        return remote(src, dst, ag_send.at[unit, slot], ag_recv.at[unit, slot], target)

    def early_own(unit, sending):
        return early_copy(digit[0], plan.slots, unit, sending)

    def early_rest(unit, sending, act):
        @pl.when(outer[0])
        def _():
            act(early_copy(three[0], slot_of[1], unit, sending))

        @pl.when(inner[0])
        def _():
            act(early_copy(mine_out[0], slot_of[1], unit, sending))
            act(early_copy(far[0], plan.slots + 1, unit, sending))

    def is_early(k, order, small):
        return bool(early) and k == 1 and order == straight and not small

    def gather_begin(k, unit, order, small):
        if is_early(k, order, small):

            @pl.when(unit < early)
            def _():
                early_rest(unit, True, lambda copy: copy.start())

            @pl.when(unit >= early)
            def _():
                gather_copy(k, 0, unit, order, small, True).start()

        elif axes[k] == 2:
            gather_copy(k, 0, unit, order, small, True).start()
        else:

            @pl.when(outer[k])
            def _():
                gather_copy(k, 0, unit, order, small, True).start()

    def gather_next(k, unit, order, small):
        position = order.index(k) + 1
        if position < depth:
            gather_begin(order[position], unit, order, small)

    def gather_hop(index, unit, order, small):
        for k in order:
            if index < plan.hops[k]:
                break
            index -= plan.hops[k]
        if axes[k] == 2:
            if is_early(k, order, small):

                @pl.when(unit < early)
                def _():
                    early_own(unit, False).wait_recv()
                    early_rest(unit, False, lambda copy: copy.wait_recv())

                @pl.when(unit >= early)
                def _():
                    gather_copy(k, 0, unit, order, small, False).wait_recv()

            else:
                gather_copy(k, 0, unit, order, small, False).wait_recv()
            gather_next(k, unit, order, small)
            return

        @pl.when(outer[k] if index == 2 else inner[k])
        def _():
            gather_copy(k, index, unit, order, small, False).wait_recv()
            if index < 2:
                gather_copy(k, index + 1, unit, order, small, True).start()
            if index > 0:
                gather_next(k, unit, order, small)

    def gather_drain(unit, order, small=False):
        for k in range(depth):
            for hop in range(plan.hops[k]):
                if is_early(k, order, small):

                    @pl.when(unit < early)
                    def _():
                        early_own(unit, True).wait_send()
                        early_rest(unit, True, lambda copy: copy.wait_send())

                    @pl.when(unit >= early)
                    def _():
                        gather_copy(k, hop, unit, order, small, True).wait_send()

                elif axes[k] == 2:
                    gather_copy(k, hop, unit, order, small, True).wait_send()
                else:

                    @pl.when(outer[k] if hop == 0 else inner[k])
                    def _():
                        gather_copy(k, hop, unit, order, small, True).wait_send()

    hops = plan.slots
    leads = spread_leads(LEADS, hops)

    def gather_tick(n, carry=0):
        for index in range(hops):
            ahead = n + leads[index]

            @pl.when((ahead >= 0) & (ahead < L * NP))
            def _():
                gather_hop(index, ahead, straight, False)

        return carry

    def ready(low, high):
        lax.fori_loop(low, high, gather_tick, 0)

    gather_begin(0, small_index, straight, True)
    for unit in range(L * NP):
        gather_begin(0, unit, straight, False)
        if unit < early:
            early_own(unit, True).start()
    here = tuple(digit)
    SB[here] = small_ref[...]
    for unit in range(L * NP):
        W[(unit,) + here] = shard_ref[unit]
    before = max(max(leads), hops)
    for n in range(-before, 0):
        gather_tick(n)
        index = n + before
        if index < hops:
            gather_hop(index, small_index, straight, True)

    vec_all = SB[(slice(None),) * depth + (slice(0, rp), slice(None))]
    vec_rows = vec_all.reshape(Dp, LANES).astype(F32).T
    for layer in range(L):
        VEC[layer] = vec_rows[layer * VEC_ROWS : (layer + 1) * VEC_ROWS]
    every = L * plan.bias_cols
    shift = HD.bit_length() - 1

    def static_place(owner):
        return tuple((owner // stride) % size for stride, size in zip(plan.strides, axes))

    def column_ids(lines):
        return lax.broadcasted_iota(jnp.int32, (lines, every), 1)

    def line_ids(lines):
        return lax.broadcasted_iota(jnp.int32, (lines, every), 0)

    def group_match():
        return lax.shift_right_logical(column_ids(LANES), shift) == line_ids(LANES)

    def feature_match(lines):
        return (column_ids(lines) & (HD - 1)) == line_ids(lines)

    for owner in range(plan.count):
        held = SB[static_place(owner) + (slice(rp, rp + BIAS_ROWS), slice(None))].astype(F32)
        low = owner * plan.quarter
        TURN[low : low + plan.quarter] = held[0 : plan.quarter]
    spread = mm(TURN[0:HD].astype(BF), group_match().astype(F32).astype(BF), NN)
    bias_row = jnp.sum(jnp.where(feature_match(HD), spread, 0.0), axis=0, keepdims=True)
    for layer in range(L):
        BIAS[layer] = bias_row[:, layer * plan.bias_cols : (layer + 1) * plan.bias_cols]

    if plan.block != plan.own:
        column = lax.broadcasted_iota(jnp.int32, (1, Dp), 1)
        valid = (lax.rem(column, rp) < plan.own).astype(F32)
    else:
        valid = None

    def average(values):
        return jnp.sum(values, axis=-1, keepdims=True) * (1.0 / plan.width)

    def masked(values):
        return values if valid is None else values * valid

    def unit_of(index):
        return W[index].reshape(Dp, half)

    def pair_of(index):
        return jnp.concatenate([unit_of(index), unit_of(index + 1)], axis=1)

    def norm_forward(values, layer, which, region):
        centred = masked(values - average(values))
        inverse = lax.rsqrt(average(centred * centred) + norm_eps)
        hat = centred * inverse
        HAT[layer, which, region] = hat
        INV[layer, which, region] = inverse
        gain = VEC[layer, 2 * which : 2 * which + 1]
        shift = VEC[layer, 2 * which + 1 : 2 * which + 2]
        ACT[layer, which, region] = (hat * gain + shift).astype(BF)

    def exchange_copy(number, slot, part):
        region = pl.ds(part * chunk, chunk)
        return remote(
            XS.at[slot, region],
            XR.at[slot, region],
            x_send.at[number, part],
            x_recv.at[number, part],
            other,
        )

    def exchange_send(number, slot, part, values):
        XS[slot, pl.ds(part * chunk, chunk)] = values.astype(BF)
        exchange_copy(number, slot, part).start()

    def exchange_sum(number, slot, part):
        exchange_copy(number, slot, part).wait_recv()
        region = pl.ds(part * chunk, chunk)
        result = XS[slot, region].astype(F32) + XR[slot, region].astype(F32)
        return result

    def exchange_done(number, slot):
        for part in range(2):
            exchange_copy(number, slot, part).wait_send()

    lane = lax.broadcasted_iota(jnp.int32, (1, LANES), 1)
    head_mask = [((lane // HD) == h).astype(F32).astype(BF) for h in range(LANES // HD)]
    scale = HD ** (-0.5)
    clips = rows // SEQ

    def landing(k, order, unit):
        if k == depth - 1:
            return lax.rem(unit, NP)
        if k > 1:
            return unit
        m = production(unit)
        return m // TURN_EVERY if order == turned else m - m // TURN_EVERY - 1

    def production(unit):
        name = lax.rem(unit, NP)
        turn = jnp.where(
            name >= 4 + UP,
            name - 4 - UP,
            jnp.where(name >= 4, name - 4 + UP, NP - 1 - name),
        )
        return (L - 1 - unit // NP) * NP + turn

    def land(k, order, slots):
        done = order[order.index(k) + 1 :]
        return tuple(slots if a == k else slice(None) for a in range(depth) if a not in done)

    def landing_ref(k, order):
        return RBt[k] if order == turned and k < 2 else RBs[k]

    def scatter_spot(k, order, value):
        done = order[order.index(k) + 1 :]
        return tuple(
            digit[a] if a in done else value if a == k else slice(None) for a in range(depth)
        )

    def scatter_copy(k, hop, unit, order, small):
        if axes[k] == 2:
            value, target, slots = 1 - digit[k], 1 - digit[k], 0
        elif hop == 0:
            value, target, slots = three[k], mine_in[k], pl.ds(0, 3)
        elif hop == 1:
            value, target, slots = far[k], far_in[k], pl.ds(3, 2)
        else:
            value, target, slots = mine_out[k], mine_out[k], 0
        spot = scatter_spot(k, order, value)
        if small:
            src, dst = SG.at[spot], RSs[k].at[land(k, order, slots)]
        else:
            src, dst = W.at[(unit,) + spot], landing_ref(k, order).at[(landing(k, order, unit),) + land(k, order, slots)]
        slot = slot_of[k] + hop
        return remote(src, dst, rs_send.at[unit, slot], rs_recv.at[unit, slot], device(k, target))

    def scatter_begin(k, unit, order, small=False):
        if axes[k] == 2:
            scatter_copy(k, 0, unit, order, small).start()
        else:

            @pl.when(outer[k])
            def _():
                scatter_copy(k, 0, unit, order, small).start()

    def held(small, unit, spot):
        return SG[spot] if small else W[(unit,) + spot].astype(F32)

    def arrived(k, order, small, unit, slots):
        if small:
            return RSs[k][land(k, order, slots)]
        spot = (landing(k, order, unit),) + land(k, order, slots)
        return landing_ref(k, order)[spot].astype(F32)

    def keep(small, unit, spot, value):
        if small:
            SG[spot] = value
        else:
            W[(unit,) + spot] = value.astype(BF)

    def keep_copy(unit):
        return pltpu.make_async_copy(GO.at[unit], gout_ref.at[unit], go_sem.at[unit])

    def finish(k, unit, order, small, slots):
        spot = scatter_spot(k, order, digit[k])
        value = held(small, unit, spot) + arrived(k, order, small, unit, slots)
        position = order.index(k)
        if position > 0:
            keep(small, unit, spot, value)
            scatter_begin(order[position - 1], unit, order, small)
        elif small:
            smallg_ref[...] = value
        else:
            GO[unit] = value
            keep_copy(unit).start()

    def add_in(k, unit, order, small, value, slots):
        spot = scatter_spot(k, order, value)
        keep(small, unit, spot, held(small, unit, spot) + arrived(k, order, small, unit, slots))

    def scatter_hop(index, unit, order, small=False):
        for k in reversed(order):
            if index < plan.hops[k]:
                break
            index -= plan.hops[k]
        if axes[k] == 2:
            scatter_copy(k, 0, unit, order, small).wait_recv()
            finish(k, unit, order, small, 0)
            return

        @pl.when(outer[k] if index == 2 else inner[k])
        def _():
            scatter_copy(k, index, unit, order, small).wait_recv()
            if index == 0:
                add_in(k, unit, order, small, three[k], pl.ds(0, 3))
                scatter_copy(k, 1, unit, order, small).start()
            elif index == 1:
                add_in(k, unit, order, small, mine_out[k], 3 + mine_out[k] - 2 * half_side[k])
                scatter_copy(k, 2, unit, order, small).start()
                finish(k, unit, order, small, 3 + digit[k] - 2 * half_side[k])
            else:
                finish(k, unit, order, small, 0)

    def scatter_drain(unit, order, small=False):
        for k in range(depth):
            for hop in range(plan.hops[k]):
                if axes[k] == 2:
                    scatter_copy(k, hop, unit, order, small).wait_send()
                else:

                    @pl.when(outer[k] if hop == 0 else inner[k])
                    def _():
                        scatter_copy(k, hop, unit, order, small).wait_send()

    block_shape = axes + (rp,)

    def put_gradient(index, value):
        W[index] = value.astype(BF).reshape(block_shape + (half,))
        scatter_begin(depth - 1, index, straight)

    def put_pair(index, value):
        put_gradient(index, value[:, :half])
        put_gradient(index + 1, value[:, half:])

    def column_sum(values):
        return jnp.sum(values, axis=0, keepdims=True)

    def down_gradient(layer, number):
        down = layer * NP + 4 + UP
        grad = mm(LOW[...], pair_of(down + number), NN) * SLOPE[layer, number // 2].astype(F32)
        low = (2 + number) * half
        BG[layer, :, low : low + 2 * half] = column_sum(grad)
        FL[number // 2] = grad.astype(BF)
        put_pair(down + number, mm(LOW[...], HIDDEN[layer, number // 2], TN))

    LOW[...] = cot_ref[...]
    VG[...] = jnp.zeros(VG.shape, F32)
    SG[...] = jnp.zeros(SG.shape, F32)

    def attend(layer):
        def one(item, _):
            pair = item // clips
            clip = lax.rem(item, clips)
            span = pl.ds(clip * SEQ, SEQ)
            query = Q[layer, pair, span]
            key = K[layer, pair, span]
            value = V[layer, pair, span]
            total = None
            for h, mask in enumerate(head_mask):
                scores = mm(query * mask, key, NT) * scale
                highest = jnp.max(scores, axis=1, keepdims=True)
                logsum = highest + jnp.log(jnp.sum(jnp.exp(scores - highest), axis=1, keepdims=True))
                kept = logsum if h == 0 else jnp.where(lane < h * HD, kept, logsum)
                weights = jnp.exp(scores - logsum).astype(BF)
                part = mm(weights, value * mask, NN)
                total = part if total is None else total + part
            LSE[layer, pair, span] = jnp.broadcast_to(kept, (SEQ, LANES))
            CTX[layer, pair, span] = total.astype(BF)
            return 0

        lax.fori_loop(0, plan.pairs * clips, one, 0)

    def context_of(layer, region=slice(None)):
        return jnp.concatenate([CTX[layer, pair, region] for pair in range(plan.pairs)], axis=1)

    def forward_layer(layer, carry):
        first = layer * NP
        up = first + 4
        down = up + UP

        @pl.when(layer == 0)
        def _():
            value = frames_ref[...].astype(F32)
            DX[...] = value
            norm_forward(value, layer, 0, slice(None))

        ready(first, first + 2)

        @pl.when(layer > 0)
        def _():
            for part in range(2):
                region = pl.ds(part * chunk, chunk)
                value = MID[region] + exchange_sum(2 * layer - 1, 1, part) + VEC[layer - 1, 5:6]
                DX[region] = value
                norm_forward(value, layer, 0, region)
            exchange_done(2 * layer - 1, 1)

        both = mm(ACT[layer, 0], pair_of(first), NN)
        for pair in range(plan.pairs):
            low = pair * LANES
            query = both[:, low : low + LANES] + BIAS[layer, :, low : low + LANES]
            Q[layer, pair] = query.astype(BF)
            K[layer, pair] = both[:, half + low : half + low + LANES].astype(BF)
        ready(first + 2, first + 3)
        values = mm(ACT[layer, 0], unit_of(first + 2), NN)
        for pair in range(plan.pairs):
            low = pair * LANES
            bias = BIAS[layer, :, half + low : half + low + LANES]
            V[layer, pair] = (values[:, low : low + LANES] + bias).astype(BF)
        attend(layer)
        ready(first + 3, first + 4)
        for part in range(2):
            region = pl.ds(part * chunk, chunk)
            heads = context_of(layer, region)
            exchange_send(2 * layer, 0, part, mm(heads, unit_of(first + 3), NT))
        ready(up, up + UP)
        for part in range(2):
            region = pl.ds(part * chunk, chunk)
            value = DX[region] + exchange_sum(2 * layer, 0, part) + VEC[layer, 4:5]
            MID[region] = value
            norm_forward(value, layer, 1, region)
        exchange_done(2 * layer, 0)
        for number in range(0, UP, 2):
            before = mm(ACT[layer, 1], pair_of(up + number), NN)
            low = (2 + number) * half
            before = before + BIAS[layer, :, low : low + 2 * half]
            bell = 0.5 * (1.0 + lax.erf(before * root_half))
            HIDDEN[layer, number // 2] = (before * bell).astype(BF)
            slope = bell + before * jnp.exp(-0.5 * before * before) * inv_root_two_pi
            SLOPE[layer, number // 2] = slope.astype(BF)
        for number in range(0, UP, 2):
            ready(down + number, down + number + 2)
            term = mm(HIDDEN[layer, number // 2], pair_of(down + number), NT)
            if number + 2 < UP:
                ACC[...] = term if number == 0 else ACC[...] + term
            else:
                whole = term + ACC[...] if UP > 2 else term

                @pl.when(layer + 1 < L)
                def _():
                    for part in range(2):
                        exchange_send(2 * layer + 1, 1, part, whole[part * chunk : (part + 1) * chunk])

                @pl.when(layer + 1 == L)
                def _():
                    LAST[...] = whole.astype(BF)

            @pl.when(layer + 1 == L)
            def _():
                for unit in (down + number, down + number + 1):
                    gather_drain(unit, straight)
                down_gradient(layer, number)

        return carry

    lax.fori_loop(0, L, forward_layer, 0)

    def attend_back(layer):
        def one(item, _):
            pair = item // clips
            clip = lax.rem(item, clips)
            span = pl.ds(clip * SEQ, SEQ)
            query = Q[layer, pair, span]
            key = K[layer, pair, span]
            value = V[layer, pair, span]
            upper = FL[1, span, pl.ds(pl.multiple_of(half + pair * LANES, LANES), LANES)]
            logsums = LSE[layer, pair, span]
            grad_q = grad_k = grad_v = None
            for h, mask in enumerate(head_mask):
                scores = mm(query * mask, key, NT) * scale
                probs = jnp.exp(scores - logsums[:, h * HD : h * HD + 1])
                weights = probs.astype(BF)
                up_head = upper * mask
                part_v = mm(weights, up_head, TN)
                grad_p = mm(up_head, value, NT)
                inner = jnp.sum(probs * grad_p, axis=1, keepdims=True)
                grad_s = (probs * (grad_p - inner) * scale).astype(BF)
                part_q = mm(grad_s, key * mask, NN)
                part_k = mm(grad_s, query * mask, TN)
                grad_q = part_q if grad_q is None else grad_q + part_q
                grad_k = part_k if grad_k is None else grad_k + part_k
                grad_v = part_v if grad_v is None else grad_v + part_v
            low = pl.ds(pl.multiple_of(pair * LANES, LANES), LANES)
            next_low = pl.ds(pl.multiple_of(half + pair * LANES, LANES), LANES)
            FL[0, span, low] = grad_q.astype(BF)
            FL[0, span, next_low] = grad_k.astype(BF)
            FL[1, span, low] = grad_v.astype(BF)
            sum_q = jnp.sum(grad_q, axis=0, keepdims=True)
            sum_v = jnp.sum(grad_v, axis=0, keepdims=True)

            @pl.when(clip == 0)
            def _():
                BG[layer, :, low] = sum_q
                BG[layer, :, next_low] = sum_v

            @pl.when(clip > 0)
            def _():
                BG[layer, :, low] += sum_q
                BG[layer, :, next_low] += sum_v

            return 0

        lax.fori_loop(0, plan.pairs * clips, one, 0)

    def norm_backward(upper, layer, which, region):
        hat = HAT[layer, which, region]
        scaled = upper * VEC[layer, 2 * which : 2 * which + 1]
        return INV[layer, which, region] * (
            masked(scaled - average(scaled)) - hat * average(scaled * hat)
        )

    def keep_rows(layer, line, part, value):
        if part == 0:
            VG[layer, line : line + 1] = value
        else:
            VG[layer, line : line + 1] += value

    DX[...] = cot_ref[...].astype(F32)
    VG[L - 1, 5:6] = column_sum(DX[...])
    DMID = ACC
    for unit in range((L - 1) * NP + 4 + UP):
        gather_drain(unit, straight)
    gather_drain(small_index, straight, True)

    def produced(m):
        turn = lax.rem(m, NP)
        name = jnp.where(
            turn < UP,
            4 + UP + turn,
            jnp.where(turn < 2 * UP, 4 + turn - UP, NP - 1 - turn),
        )
        return (L - 1 - m // NP) * NP + name

    def pumped(step, place, index):
        counts = [row[min(index - 1, len(row) - 1)] - max(0, index - len(row)) for row in PUMPS[place]]
        value = counts[0]
        for s in range(1, L):
            value = jnp.where(step == s, counts[min(s, len(counts) - 1)], value)
        return jnp.clip(value, 0, L * NP)

    def scatter_either(index, m):
        unit = produced(m)

        @pl.when(lax.rem(m, TURN_EVERY) != 0)
        def _():
            scatter_hop(index, unit, straight)

        @pl.when(lax.rem(m, TURN_EVERY) == 0)
        def _():
            scatter_hop(index, unit, turned)

    def pump_between(lows, highs):
        length = functools.reduce(jnp.maximum, [high - low for low, high in zip(lows, highs)])

        def one(t, carry):
            for index in range(1, hops):
                m = lows[index - 1] + t

                @pl.when(m < highs[index - 1])
                def _():
                    scatter_either(index, m)

            return carry

        lax.fori_loop(0, length, one, 0)

    def pump_to(step, place):
        if place == 0:
            before = [
                jnp.where(step == 0, 0, pumped(step - 1, len(PUMPS) - 1, index)) for index in range(1, hops)
            ]
        else:
            before = [pumped(step, place - 1, index) for index in range(1, hops)]
        pump_between(before, [pumped(step, place, index) for index in range(1, hops)])

    def rest_order():
        last = [row[-1] for row in PUMPS][-1]
        done = [min(last[min(index, 4) - 1], L * NP) for index in range(1, 5)]
        done += [0] * (hops - 5)
        if hops == 5 and sum(done) + len(REST) == 4 * L * NP:
            given = list(REST)
        else:
            done = [max(0, min(done[min(index, 4) - 1] - max(0, index - 4), L * NP)) for index in range(1, hops)]
            left = [(m + 2 * index, index) for index in range(1, hops) for m in range(done[index - 1], L * NP)]
            given = [index for _, index in sorted(left)]
        events = []
        for index in given:
            events.append((index, done[index - 1]))
            done[index - 1] += 1
        return events

    def named(m):
        name = m % NP
        name = 4 + UP + name if name < UP else 4 + name - UP if name < 2 * UP else NP - 1 - name
        return (L - 1 - m // NP) * NP + name, turned if m % TURN_EVERY == 0 else straight

    def pump_rest(aside):
        events = rest_order()
        for number, (index, m) in enumerate(events):
            unit, order = named(m)
            scatter_hop(index, unit, order)
            if m == L * NP - 1:
                scatter_hop(index, small_index, straight, True)
            if len(events) - 1 - number in aside:
                aside[len(events) - 1 - number]()

    def backward_layer(step, carry):
        layer = L - 1 - step
        first = layer * NP
        up = first + 4
        down = up + UP
        number_up = 2 * L + 2 * step

        def from_core(low, high):
            for n in range(low, high):
                turn = n - 4 - UP if n >= 4 + UP else n - 4 + UP if n >= 4 else NP - 1 - n
                scatter_hop(0, first + n, turned if turn % TURN_EVERY == 0 else straight)

        for part in range(2):
            from_core(4 + UP + part * UP // 2, 4 + UP + (part + 1) * UP // 2)
            region = pl.ds(part * chunk, chunk)
            whole = None
            for number in range(0, UP, 2):
                term = mm(FL[number // 2, region], pair_of(up + number), NT)
                whole = term if whole is None else whole + term
            exchange_send(number_up, 1, part, whole)
        pump_to(step, 0)
        for number in range(0, UP, 2):
            put_pair(up + number, mm(ACT[layer, 1], FL[number // 2], TN))
        from_core(4, 4 + UP)
        pump_to(step, 1)
        for part in range(2):
            region = pl.ds(part * chunk, chunk)
            grad = exchange_sum(number_up, 1, part)
            keep_rows(layer, 2, part, column_sum(grad * HAT[layer, 1, region]))
            keep_rows(layer, 3, part, column_sum(grad))
            grad_mid = DX[region] + norm_backward(grad, layer, 1, region)
            DMID[region] = grad_mid
            keep_rows(layer, 4, part, column_sum(grad_mid))
            LOW[region] = grad_mid.astype(BF)
        exchange_done(number_up, 1)
        heads = mm(LOW[...], unit_of(first + 3), NN)
        FL[1, :, half : 2 * half] = heads.astype(BF)
        put_gradient(first + 3, mm(LOW[...], context_of(layer), TN))
        pump_to(step, 2)
        attend_back(layer)
        for part in range(2):
            region = pl.ds(part * chunk, chunk)
            whole = mm(FL[0, region], pair_of(first), NT)
            whole = whole + mm(FL[1, region, 0:half], unit_of(first + 2), NT)
            exchange_send(number_up + 1, 0, part, whole)
        from_core(3, 4)
        pump_to(step, 3)
        put_gradient(first + 2, mm(ACT[layer, 0], FL[1, :, 0:half], TN))
        grad_qk = mm(ACT[layer, 0], FL[0], TN)
        put_gradient(first + 1, grad_qk[:, half:])
        put_gradient(first, grad_qk[:, :half])
        for n in (2, 1, 0):
            from_core(n, n + 1)
        pump_to(step, 4)

        @pl.when(step + 1 == L)
        def _():
            pack_biases()

        for part in range(2):
            region = pl.ds(part * chunk, chunk)
            grad = exchange_sum(number_up + 1, 0, part)
            keep_rows(layer, 0, part, column_sum(grad * HAT[layer, 0, region]))
            keep_rows(layer, 1, part, column_sum(grad))
            upper = DMID[region] + norm_backward(grad, layer, 0, region)
            DX[region] = upper
            LOW[region] = upper.astype(BF)
        exchange_done(number_up + 1, 0)

        @pl.when(step + 1 < L)
        def _():
            VG[layer - 1, 5:6] = column_sum(DX[...])
            for number in range(0, UP, 2):
                down_gradient(layer - 1, number)

        return carry

    def pack_biases():
        row = jnp.concatenate([BG[layer] for layer in range(L)], axis=1)
        wide = jnp.where(group_match(), row, 0.0)
        high = wide.astype(BF)
        low = (wide - high.astype(F32)).astype(BF)
        select = feature_match(LANES).astype(F32).astype(BF)
        table = (mm(high, select, NT) + mm(low, select, NT)).T
        for owner in range(plan.count):
            start = owner * plan.quarter
            spot = static_place(owner) + (slice(rp, rp + plan.quarter), slice(None))
            SG[spot] = table[start : start + plan.quarter]

    lax.fori_loop(0, L, backward_layer, 0)

    lines = [VG[layer] for layer in range(L)]
    lines.append(jnp.zeros((LANES - L * VEC_ROWS, Dp), F32))
    columns = jnp.concatenate(lines, axis=0).T.reshape(axes + (rp, LANES))
    SG[(slice(None),) * depth + (slice(0, rp), slice(None))] = columns
    scatter_begin(depth - 1, small_index, straight, True)
    for part in range(2):
        exchange_send(2 * L - 1, 1, part, LAST[pl.ds(part * chunk, chunk)])
    gin_copy = pltpu.make_async_copy(DX, gin_ref, go_sem.at[L * NP])
    out_copy = pltpu.make_async_copy(OUT, out_ref, go_sem.at[L * NP + 1])
    gin_copy.start()
    scatter_hop(0, small_index, straight, True)

    def output():
        for part in range(2):
            region = pl.ds(part * chunk, chunk)
            value = MID[region] + exchange_sum(2 * L - 1, 1, part) + VEC[L - 1, 5:6]
            OUT[region] = value.astype(BF)
        out_copy.start()
        exchange_done(2 * L - 1, 1)
        gin_copy.wait()

    first_left = L * NP - NP // 2

    def drain_first():
        for m in range(first_left):
            scatter_drain(*named(m))

    pump_rest({14: output, 4: drain_first})
    for m in range(first_left, L * NP):
        scatter_drain(*named(m))
    scatter_drain(small_index, straight, True)
    out_copy.wait()
    for unit in range(L * NP):
        keep_copy(unit).wait()


PUMPS = (
    ((0, 0, 0, 0), (12, 8, 5, 1)),
    ((2, 0, 0, 0), (14, 9, 8, 1)),
    ((4, 1, 0, 0), (16, 11, 8, 6)),
    ((7, 3, 1, 0), (18, 13, 11, 6)),
    ((8, 5, 1, 0), (20, 14, 13, 9)),
)
REST = (
    1, 1, 2, 2, 2, 3, 4, 4, 4, 1, 2, 2, 2, 3, 3, 2, 3, 2, 3, 2, 1, 4, 4, 3,
    3, 3, 2, 3, 4, 3, 4, 4, 4, 4, 3, 4, 4, 4, 4, 4,
)


def run_kernel(plan, frames, cotangent, shards, small):
    L, NP, Dp, rp, rows = plan.layers, plan.units, plan.padded, plan.block, plan.rows
    axes = plan.axes
    depth = len(axes)
    half = plan.half
    UP = plan.ups // 2
    piece = 2 * half
    landings = []
    small_landings = []
    for k, size in enumerate(axes):
        turned_number = -(-L * NP // TURN_EVERY)
        number = NP if k == depth - 1 else L * NP - turned_number if k < 2 else L * NP
        slots = 1 if size == 2 else 5
        landings.append(pltpu.VMEM((number,) + axes[:k] + (slots, rp, half), BF))
        small_landings.append(pltpu.VMEM(axes[:k] + (slots, rp + BIAS_ROWS, LANES), F32))
    turned_landings = [
        pltpu.VMEM((-(-L * NP // TURN_EVERY), 1 if axes[0] == 2 else 5, axes[1], rp, half), BF),
        pltpu.VMEM((-(-L * NP // TURN_EVERY), 1 if axes[1] == 2 else 5, rp, half), BF),
    ]
    scratch = [
        pltpu.VMEM((L * NP,) + axes + (rp, half), BF),
        pltpu.VMEM(axes + (rp + BIAS_ROWS, LANES), BF),
        pltpu.VMEM((L, VEC_ROWS, Dp), F32),
        pltpu.VMEM((L, 1, plan.bias_cols), F32),
        pltpu.VMEM((2, rows, Dp), BF),
        pltpu.VMEM((2, rows, Dp), BF),
        pltpu.VMEM((rows, Dp), F32),
        pltpu.VMEM((rows, Dp), F32),
        pltpu.VMEM((rows, Dp), BF),
        pltpu.VMEM((L, 2, rows, Dp), F32),
        pltpu.VMEM((L, 2, rows, 1), F32),
        pltpu.VMEM((L, 2, rows, Dp), BF),
        pltpu.VMEM((L, plan.pairs, rows, LANES), BF),
        pltpu.VMEM((L, plan.pairs, rows, LANES), BF),
        pltpu.VMEM((L, plan.pairs, rows, LANES), BF),
        pltpu.VMEM((L, plan.pairs, rows, LANES), F32),
        pltpu.VMEM((L, plan.pairs, rows, LANES), BF),
        pltpu.VMEM((L, UP, rows, piece), BF),
        pltpu.VMEM((L, UP, rows, piece), BF),
        pltpu.VMEM((rows, Dp), F32),
        pltpu.VMEM((rows, Dp), BF),
        pltpu.VMEM((UP, rows, piece), BF),
        pltpu.VMEM((L, VEC_ROWS, Dp), F32),
        pltpu.VMEM((L, 1, plan.bias_cols), F32),
        pltpu.VMEM((HD, LANES), F32),
        pltpu.VMEM(axes + (rp + BIAS_ROWS, LANES), F32),
        landings,
        turned_landings,
        small_landings,
        pltpu.SemaphoreType.DMA((L * NP + 1, plan.slots + (2 if plan.early else 0))),
        pltpu.SemaphoreType.DMA((L * NP + 1, plan.slots + (2 if plan.early else 0))),
        pltpu.SemaphoreType.DMA((L * NP + 1, plan.slots)),
        pltpu.SemaphoreType.DMA((L * NP + 1, plan.slots)),
        pltpu.SemaphoreType.DMA((4 * L, 2)),
        pltpu.SemaphoreType.DMA((4 * L, 2)),
        pltpu.VMEM((L * NP, rp, half), F32),
        pltpu.VMEM((rows, Dp), BF),
        pltpu.SemaphoreType.DMA((L * NP + 2,)),
    ]
    return pl.pallas_call(
        functools.partial(train_kernel, plan),
        out_shape=(
            jax.ShapeDtypeStruct((rows, Dp), BF),
            jax.ShapeDtypeStruct((rows, Dp), F32),
            jax.ShapeDtypeStruct((L * NP, rp, half), F32),
            jax.ShapeDtypeStruct((rp + BIAS_ROWS, LANES), F32),
        ),
        in_specs=[pl.BlockSpec(memory_space=pltpu.VMEM)] * 4,
        out_specs=tuple([pl.BlockSpec(memory_space=pl.ANY)] * 3 + [pl.BlockSpec(memory_space=pltpu.VMEM)]),
        scratch_shapes=scratch,
        compiler_params=pltpu.CompilerParams(
            collective_id=0, has_side_effects=True, vmem_limit_bytes=67043328
        ),
        name="train_step",
    )(frames, cotangent, shards, small)


def adamw(weight, gradient, first, second, rate, decay):
    first_new = beta_one * first + (1.0 - beta_one) * gradient
    second_new = beta_two * second + (1.0 - beta_two) * gradient * gradient
    first_hat = first_new / (1.0 - beta_one**STEP)
    second_hat = second_new / (1.0 - beta_two**STEP)
    weight_new = weight - rate * (first_hat / (jnp.sqrt(second_hat) + adam_eps) + decay * weight)
    return (weight_new, first_new, second_new)


def pad_axis(values, axis, size):
    widths = [(0, 0)] * values.ndim
    widths[axis] = (0, size - values.shape[axis])
    return jnp.pad(values, widths)


def on_device(count, frames, cotangent, *tensors):
    masters, firsts, seconds = tensors[:7], tensors[7:14], tensors[14:21]
    w_qkv, w_out, w_up, w_down, b_qv, b_up, vectors = masters
    L = w_qkv.shape[0]
    rows, width = frames.shape
    half = w_qkv.shape[3]
    hidden = w_up.shape[2]
    plan = Plan(count, rows, width, half, hidden, L)
    own, rp, UP = plan.own, plan.block, plan.ups

    def spread_features(values):
        if rp == own:
            return values
        return pad_axis(values.reshape(rows, count, own), 2, rp).reshape(rows, plan.padded)

    def gather_features(values):
        if rp == own:
            return values
        return values.reshape(rows, count, rp)[:, :, :own].reshape(rows, width)

    low_qkv = w_qkv.astype(BF).reshape(L, own, 3 * half)
    low_out = w_out.astype(BF).transpose(0, 2, 1)
    low_up = w_up.astype(BF)
    low_down = w_down.astype(BF).transpose(0, 2, 1)
    parts = [low_qkv[:, :, n * half : (n + 1) * half] for n in range(3)] + [low_out]
    parts += [low_up[:, :, n * half : (n + 1) * half] for n in range(UP)]
    parts += [low_down[:, :, n * half : (n + 1) * half] for n in range(UP)]
    shards = jnp.stack(parts, axis=1).reshape(L * plan.units, own, half)
    shards = pad_axis(shards, 1, rp)

    quarter = plan.quarter
    vec_part = pad_axis(vectors.astype(BF).transpose(2, 0, 1), 2, VEC_ROWS).reshape(own, L * VEC_ROWS)
    bias_part = jnp.concatenate(
        [b_qv.astype(BF).reshape(L, -1, quarter), b_up.astype(BF).reshape(L, -1, quarter)], axis=1
    )
    groups = bias_part.shape[1]
    bias_part = bias_part.transpose(2, 0, 1).reshape(quarter, L * groups)
    small = jnp.concatenate(
        [
            pad_axis(pad_axis(vec_part, 1, LANES), 0, rp),
            pad_axis(pad_axis(bias_part, 1, LANES), 0, BIAS_ROWS),
        ],
        axis=0,
    )

    output, grad_input, wide, small_grad = run_kernel(
        plan, spread_features(frames), spread_features(cotangent), shards, small
    )

    wide = wide.reshape(L, plan.units, rp, half)[:, :, :own]
    grad_qkv = jnp.stack([wide[:, n] for n in range(3)], axis=2)
    grad_out = wide[:, 3].transpose(0, 2, 1)
    grad_up = jnp.concatenate([wide[:, 4 + n] for n in range(UP)], axis=2)
    grad_down = jnp.concatenate([wide[:, 4 + UP + n] for n in range(UP)], axis=2).transpose(0, 2, 1)
    vec_grad = small_grad[:own, : L * VEC_ROWS].reshape(own, L, VEC_ROWS)[:, :, : vectors.shape[1]]
    grad_vec = vec_grad.transpose(1, 2, 0)
    bias_grad = small_grad[rp : rp + quarter, : L * groups].reshape(quarter, L, groups)
    bias_grad = bias_grad.transpose(1, 2, 0)
    split = b_qv.shape[1] * b_qv.shape[2]
    grad_bqv = bias_grad[:, :split].reshape(b_qv.shape)
    grad_bup = bias_grad[:, split:]
    grads = (grad_qkv, grad_out, grad_up, grad_down, grad_bqv, grad_bup, grad_vec)
    rates = (rate_matrix,) * 4 + (rate_vector,) * 3
    decays = (decay_rate,) * 4 + (0.0,) * 3
    updated = [
        adamw(masters[n], grads[n], firsts[n], seconds[n], rates[n], decays[n]) for n in range(7)
    ]
    return (
        (gather_features(output), gather_features(grad_input))
        + grads
        + tuple(updated[n][0] for n in range(7))
        + tuple(updated[n][1] for n in range(7))
        + tuple(updated[n][2] for n in range(7))
    )


def solution(mesh):
    tensors = (
        P(None, "fsdp", None, "tp"),
        P(None, "tp", "fsdp"),
        P(None, "fsdp", "tp"),
        P(None, "tp", "fsdp"),
        P(None, None, "tp", "fsdp"),
        P(None, "tp", "fsdp"),
        P(None, None, "fsdp"),
    )
    rows = (P("fsdp", None), P("fsdp", None))
    return jax.shard_map(
        functools.partial(on_device, mesh.shape["fsdp"]),
        mesh=mesh,
        in_specs=rows + tensors * 3,
        out_specs=rows + tensors * 4,
        check_vma=False,
    )
```

```python
import functools
import jax
import jax.numpy as jnp
from jax import lax
from jax.experimental import pallas as pl
from jax.experimental.pallas import tpu as pltpu
from jax.sharding import PartitionSpec as P

HD = 64
SEQ = 256
STEP = 3

norm_eps = 1e-05
beta_one = 0.9
beta_two = 0.999
adam_eps = 1e-08
decay_rate = 0.1
rate_matrix = 0.01
rate_vector = 0.2
root_half = 0.7071067811865476
inv_root_two_pi = 0.3989422804014327

BF = jnp.bfloat16
F32 = jnp.float32
NN = (((1,), (0,)), ((), ()))
NT = (((1,), (1,)), ((), ()))
TN = (((0,), (0,)), ((), ()))
MESH = pl.DeviceIdType.MESH
LANES = 128
BIAS_ROWS = 16
TURN_EVERY = 6
VEC_ROWS = 8


def mm(left, right, dims):
    return lax.dot_general(left, right, dims, preferred_element_type=F32)


def factor_axes(count):
    chips = count // 2
    sizes = []
    while chips > 1:
        step = 4 if chips % 4 == 0 else 2 if chips % 2 == 0 else chips
        sizes.append(step)
        chips //= step
    return tuple(sizes) + (2,)


LEADS = (7, 5, 4, 2, 0)
EARLY = 12


def spread_leads(leads, hops):
    extra = hops - len(leads)
    return [leads[0] + extra - n for n in range(extra)] + list(leads)


class Plan:
    def __init__(self, count, rows, width, half, hidden, layers):
        self.count = count
        self.axes = factor_axes(count)
        strides = []
        stride = count
        for size in self.axes:
            stride //= size
            strides.append(stride)
        self.strides = tuple(strides)
        self.rows = rows
        self.width = width
        self.own = width // count
        self.block = -(-self.own // 16) * 16
        self.padded = self.block * count
        self.half = half
        self.pairs = half // LANES
        self.layers = layers
        self.ups = hidden // half
        self.units = 4 + 2 * self.ups
        self.quarter = HD // count
        self.bias_cols = 2 * half + hidden
        self.hops = tuple(1 if size == 2 else 3 for size in self.axes)
        self.slots = sum(self.hops)
        self.signals = sum(1 if size == 2 else 2 for size in self.axes)
        self.chunk = rows // 2
        self.early = EARLY if self.axes[:2] == (4, 2) else 0


def train_kernel(
    plan,
    frames_ref,
    cot_ref,
    shard_ref,
    small_ref,
    out_ref,
    gin_ref,
    gout_ref,
    smallg_ref,
    W,
    SB,
    VEC,
    BIAS,
    XS,
    XR,
    MID,
    ACC,
    LAST,
    HAT,
    INV,
    ACT,
    Q,
    K,
    V,
    LSE,
    CTX,
    SLOPE,
    HIDDEN,
    DX,
    LOW,
    FL,
    VG,
    BG,
    TURN,
    SG,
    RBs,
    RBt,
    RSs,
    ag_send,
    ag_recv,
    early_recv,
    rs_send,
    rs_recv,
    x_send,
    x_recv,
    GO,
    OUT,
    go_sem,
):
    axes = plan.axes
    depth = len(axes)
    rp = plan.block
    Dp = plan.padded
    L = plan.layers
    NP = plan.units
    UP = plan.ups
    half = plan.half
    rows = plan.rows
    chunk = plan.chunk

    me = lax.axis_index("fsdp")
    side = lax.axis_index("tp")
    digit = [lax.rem(me // stride, size) for stride, size in zip(plan.strides, axes)]
    slot_of = [sum(1 if size == 2 else 2 for size in axes[:k]) for k in range(depth)]
    other = (me, 1 - side)

    def device(k, value):
        return (me + (value - digit[k]) * plan.strides[k], side)

    half_side = [d // 2 for d in digit]
    outer = [(d == 0) | (d == 3) for d in digit]
    inner = [jnp.logical_not(flag) for flag in outer]
    mine_in = [1 + s for s in half_side]
    mine_out = [3 * s for s in half_side]
    far_in = [2 - s for s in half_side]
    near = [pl.ds(2 * s, 2) for s in half_side]
    far = [pl.ds(2 * (1 - s), 2) for s in half_side]
    three = [pl.ds(1 - s, 3) for s in half_side]

    barrier = pltpu.get_barrier_semaphore()

    def greet(target):
        pl.semaphore_signal(barrier, inc=1, device_id=target, device_id_type=MESH)

    greet(other)
    greeted = 1
    for k in range(depth):
        if axes[k] == 2:
            greet(device(k, 1 - digit[k]))
        else:
            greet(device(k, jnp.where(outer[k], mine_in[k], mine_out[k])))
        greeted += 1
    for k in range(depth):
        if axes[k] == 4:

            @pl.when(inner[k])
            def _():
                greet(device(k, far_in[k]))

            greeted = greeted + jnp.where(inner[k], 1, 0)
    pl.semaphore_wait(barrier, greeted)

    def remote(src, dst, send, recv, target):
        return pltpu.make_async_remote_copy(
            src_ref=src,
            dst_ref=dst,
            send_sem=send,
            recv_sem=recv,
            device_id=target,
            device_id_type=MESH,
        )

    small_index = L * NP
    straight = tuple(range(depth))
    turned = (1, 0) + straight[2:]
    early = plan.early

    late = L * NP - UP

    def group_of(unit, small=False):
        if small:
            return 1 + UP // 2
        return jnp.where(unit < late, 0, 1 + (unit - late) // 2)

    def gather_copy(k, hop, unit, order, small, sending):
        done = order[: order.index(k)]

        def spot(value):
            return tuple(
                slice(None) if a in done else value if a == k else digit[a] for a in range(depth)
            )

        if axes[k] == 2:
            value = digit[k] if sending else 1 - digit[k]
            target = 1 - digit[k]
        elif hop == 0:
            value = digit[k] if sending else mine_out[k]
            target = mine_in[k]
        elif hop == 1:
            value = near[k] if sending else far[k]
            target = far_in[k]
        else:
            value = three[k]
            target = mine_out[k]
        dst = SB.at[spot(value)] if small else W.at[(unit,) + spot(value)]
        src = dst
        if sending and not done and hop == 0:
            src = small_ref if small else shard_ref.at[unit]
        slot = slot_of[k] + hop % 2
        return remote(src, dst, ag_send.at[group_of(unit, small), slot], ag_recv.at[unit, slot], device(k, target))

    def early_copy(value, number, unit, sending):
        own = value is digit[0]
        spot = (value, digit[1] if sending else 1 - digit[1]) + tuple(digit[2:])
        dst = W.at[(unit,) + spot]
        src = shard_ref.at[unit] if own and sending else dst
        target = device(1, 1 - digit[1])
        arrival = ag_recv.at[unit, slot_of[1]] if number == 1 else early_recv.at[unit, number // 2]
        return remote(src, dst, ag_send.at[0, plan.signals + number], arrival, target)

    def early_own(unit, sending):
        return early_copy(digit[0], 0, unit, sending)

    def early_rest(unit, sending, act):
        @pl.when(outer[0])
        def _():
            act(early_copy(three[0], 1, unit, sending))

        @pl.when(inner[0])
        def _():
            act(early_copy(mine_out[0], 1, unit, sending))
            act(early_copy(far[0], 2, unit, sending))

    def is_early(k, order, small):
        return bool(early) and k == 1 and order == straight and not small

    def gather_begin(k, unit, order, small):
        if is_early(k, order, small):

            @pl.when(unit < early)
            def _():
                early_rest(unit, True, lambda copy: copy.start())

            @pl.when(unit >= early)
            def _():
                gather_copy(k, 0, unit, order, small, True).start()

        elif axes[k] == 2:
            gather_copy(k, 0, unit, order, small, True).start()
        else:

            @pl.when(outer[k])
            def _():
                gather_copy(k, 0, unit, order, small, True).start()

    def gather_next(k, unit, order, small):
        position = order.index(k) + 1
        if position < depth:
            gather_begin(order[position], unit, order, small)

    def gather_hop(index, unit, order, small):
        for k in order:
            if index < plan.hops[k]:
                break
            index -= plan.hops[k]
        if axes[k] == 2:
            if is_early(k, order, small):

                @pl.when(unit < early)
                def _():
                    early_own(unit, False).wait_recv()
                    early_rest(unit, False, lambda copy: copy.wait_recv())

                @pl.when(unit >= early)
                def _():
                    gather_copy(k, 0, unit, order, small, False).wait_recv()

            else:
                gather_copy(k, 0, unit, order, small, False).wait_recv()
            gather_next(k, unit, order, small)
            return

        @pl.when(outer[k] if index == 2 else inner[k])
        def _():
            gather_copy(k, index, unit, order, small, False).wait_recv()
            if index < 2:
                gather_copy(k, index + 1, unit, order, small, True).start()
            if index > 0:
                gather_next(k, unit, order, small)

    def gather_drain(group, first, number, small=False):
        def sent(slot, spot, low, count):
            ref = SB.at[spot] if small else W.at[(pl.ds(low, count),) + spot]
            remote(ref, ref, ag_send.at[group, slot], ag_recv.at[0, 0], other).wait_send()

        ahead = min(early, number) if group == 0 and not small else 0
        for k in range(depth):

            def spot(value):
                return tuple(
                    slice(None) if a < k else value if a == k else digit[a] for a in range(depth)
                )

            if axes[k] == 2:
                skipped = ahead if k == 1 else 0
                if number > skipped:
                    sent(slot_of[k], spot(digit[k]), first, number - skipped)
            else:

                @pl.when(outer[k])
                def _():
                    sent(slot_of[k], spot(digit[k]), first, number)

                @pl.when(inner[k])
                def _():
                    sent(slot_of[k] + 1, spot(near[k]), first, number)
                    sent(slot_of[k], spot(three[k]), first, number)

        if ahead:
            tail = (digit[1],) + tuple(digit[2:])
            sent(plan.signals, (digit[0],) + tail, 0, ahead)

            @pl.when(outer[0])
            def _():
                sent(plan.signals + 1, (three[0],) + tail, 0, ahead)

            @pl.when(inner[0])
            def _():
                sent(plan.signals + 1, (mine_out[0],) + tail, 0, ahead)
                sent(plan.signals + 2, (far[0],) + tail, 0, ahead)

    hops = plan.slots
    leads = spread_leads(LEADS, hops)

    def gather_tick(n, carry=0):
        for index in range(hops):
            ahead = n + leads[index]

            @pl.when((ahead >= 0) & (ahead < L * NP))
            def _():
                gather_hop(index, ahead, straight, False)

        return carry

    def ready(low, high):
        lax.fori_loop(low, high, gather_tick, 0)

    gather_begin(0, small_index, straight, True)
    for unit in range(L * NP):
        gather_begin(0, unit, straight, False)
        if unit < early:
            early_own(unit, True).start()
    here = tuple(digit)
    SB[here] = small_ref[...]
    for unit in range(L * NP):
        W[(unit,) + here] = shard_ref[unit]
    before = max(max(leads), hops)
    for n in range(-before, 0):
        gather_tick(n)
        index = n + before
        if index < hops:
            gather_hop(index, small_index, straight, True)

    vec_all = SB[(slice(None),) * depth + (slice(0, rp), slice(None))]
    vec_rows = vec_all.reshape(Dp, LANES).astype(F32).T
    for layer in range(L):
        VEC[layer] = vec_rows[layer * VEC_ROWS : (layer + 1) * VEC_ROWS]
    every = L * plan.bias_cols
    shift = HD.bit_length() - 1

    def static_place(owner):
        return tuple((owner // stride) % size for stride, size in zip(plan.strides, axes))

    def column_ids(lines):
        return lax.broadcasted_iota(jnp.int32, (lines, every), 1)

    def line_ids(lines):
        return lax.broadcasted_iota(jnp.int32, (lines, every), 0)

    def group_match():
        return lax.shift_right_logical(column_ids(LANES), shift) == line_ids(LANES)

    def feature_match(lines):
        return (column_ids(lines) & (HD - 1)) == line_ids(lines)

    for owner in range(plan.count):
        held = SB[static_place(owner) + (slice(rp, rp + BIAS_ROWS), slice(None))].astype(F32)
        low = owner * plan.quarter
        TURN[low : low + plan.quarter] = held[0 : plan.quarter]
    spread = mm(TURN[0:HD].astype(BF), group_match().astype(F32).astype(BF), NN)
    bias_row = jnp.sum(jnp.where(feature_match(HD), spread, 0.0), axis=0, keepdims=True)
    for layer in range(L):
        BIAS[layer] = bias_row[:, layer * plan.bias_cols : (layer + 1) * plan.bias_cols]

    if plan.block != plan.own:
        column = lax.broadcasted_iota(jnp.int32, (1, Dp), 1)
        valid = (lax.rem(column, rp) < plan.own).astype(F32)
    else:
        valid = None

    def average(values):
        return jnp.sum(values, axis=-1, keepdims=True) * (1.0 / plan.width)

    def masked(values):
        return values if valid is None else values * valid

    def unit_of(index):
        return W[index].reshape(Dp, half)

    def pair_of(index):
        return jnp.concatenate([unit_of(index), unit_of(index + 1)], axis=1)

    def norm_forward(values, layer, which, region):
        centred = masked(values - average(values))
        inverse = lax.rsqrt(average(centred * centred) + norm_eps)
        hat = centred * inverse
        HAT[layer, which, region] = hat
        INV[layer, which, region] = inverse
        gain = VEC[layer, 2 * which : 2 * which + 1]
        shift = VEC[layer, 2 * which + 1 : 2 * which + 2]
        ACT[layer, which, region] = (hat * gain + shift).astype(BF)

    def exchange_copy(number, slot, part):
        region = pl.ds(part * chunk, chunk)
        return remote(
            XS.at[slot, region],
            XR.at[slot, region],
            x_send.at[slot, part],
            x_recv.at[number, part],
            other,
        )

    def exchange_send(number, slot, part, values):
        XS[slot, pl.ds(part * chunk, chunk)] = values.astype(BF)
        exchange_copy(number, slot, part).start()

    def exchange_sum(number, slot, part):
        exchange_copy(number, slot, part).wait_recv()
        region = pl.ds(part * chunk, chunk)
        result = XS[slot, region].astype(F32) + XR[slot, region].astype(F32)
        return result

    def exchange_done(number, slot):
        for part in range(2):
            exchange_copy(number, slot, part).wait_send()

    lane = lax.broadcasted_iota(jnp.int32, (1, LANES), 1)
    head_mask = [((lane // HD) == h).astype(F32).astype(BF) for h in range(LANES // HD)]
    scale = HD ** (-0.5)
    clips = rows // SEQ

    def landing(k, order, unit):
        if k == depth - 1:
            return lax.rem(unit, NP)
        if k > 1:
            return unit
        m = production(unit)
        return m // TURN_EVERY if order == turned else m - m // TURN_EVERY - 1

    def production(unit):
        name = lax.rem(unit, NP)
        turn = jnp.where(
            name >= 4 + UP,
            name - 4 - UP,
            jnp.where(name >= 4, name - 4 + UP, NP - 1 - name),
        )
        return (L - 1 - unit // NP) * NP + turn

    def land(k, order, slots):
        done = order[order.index(k) + 1 :]
        return tuple(slots if a == k else slice(None) for a in range(depth) if a not in done)

    def landing_ref(k, order):
        return RBt[k] if order == turned and k < 2 else RBs[k]

    def scatter_spot(k, order, value):
        done = order[order.index(k) + 1 :]
        return tuple(
            digit[a] if a in done else value if a == k else slice(None) for a in range(depth)
        )

    def scatter_copy(k, hop, unit, order, small):
        if axes[k] == 2:
            value, target, slots = 1 - digit[k], 1 - digit[k], 0
        elif hop == 0:
            value, target, slots = three[k], mine_in[k], pl.ds(0, 3)
        elif hop == 1:
            value, target, slots = far[k], far_in[k], pl.ds(3, 2)
        else:
            value, target, slots = mine_out[k], mine_out[k], 0
        spot = scatter_spot(k, order, value)
        if small:
            src, dst = SG.at[spot], RSs[k].at[land(k, order, slots)]
        else:
            src, dst = W.at[(unit,) + spot], landing_ref(k, order).at[(landing(k, order, unit),) + land(k, order, slots)]
        slot = slot_of[k] + hop % 2
        kind = 2 if small else 1 if order == turned else 0
        return remote(src, dst, rs_send.at[kind, slot], rs_recv.at[unit, slot], device(k, target))

    def scatter_begin(k, unit, order, small=False):
        if axes[k] == 2:
            scatter_copy(k, 0, unit, order, small).start()
        else:

            @pl.when(outer[k])
            def _():
                scatter_copy(k, 0, unit, order, small).start()

    def held(small, unit, spot):
        return SG[spot] if small else W[(unit,) + spot].astype(F32)

    def arrived(k, order, small, unit, slots):
        if small:
            return RSs[k][land(k, order, slots)]
        spot = (landing(k, order, unit),) + land(k, order, slots)
        return landing_ref(k, order)[spot].astype(F32)

    def keep(small, unit, spot, value):
        if small:
            SG[spot] = value
        else:
            W[(unit,) + spot] = value.astype(BF)

    def keep_copy(unit):
        return pltpu.make_async_copy(GO.at[unit], gout_ref.at[unit], go_sem.at[0])

    def finish(k, unit, order, small, slots):
        spot = scatter_spot(k, order, digit[k])
        value = held(small, unit, spot) + arrived(k, order, small, unit, slots)
        position = order.index(k)
        if position > 0:
            keep(small, unit, spot, value)
            scatter_begin(order[position - 1], unit, order, small)
        elif small:
            smallg_ref[...] = value
        else:
            GO[unit] = value
            keep_copy(unit).start()

    def add_in(k, unit, order, small, value, slots):
        spot = scatter_spot(k, order, value)
        keep(small, unit, spot, held(small, unit, spot) + arrived(k, order, small, unit, slots))

    def scatter_hop(index, unit, order, small=False):
        for k in reversed(order):
            if index < plan.hops[k]:
                break
            index -= plan.hops[k]
        if axes[k] == 2:
            scatter_copy(k, 0, unit, order, small).wait_recv()
            finish(k, unit, order, small, 0)
            return

        @pl.when(outer[k] if index == 2 else inner[k])
        def _():
            scatter_copy(k, index, unit, order, small).wait_recv()
            if index == 0:
                add_in(k, unit, order, small, three[k], pl.ds(0, 3))
                scatter_copy(k, 1, unit, order, small).start()
            elif index == 1:
                add_in(k, unit, order, small, mine_out[k], 3 + mine_out[k] - 2 * half_side[k])
                scatter_copy(k, 2, unit, order, small).start()
                finish(k, unit, order, small, 3 + digit[k] - 2 * half_side[k])
            else:
                finish(k, unit, order, small, 0)

    def scatter_drain(kind, order, number):
        def sent(k, hop, value, count):
            spot = scatter_spot(k, order, value)
            ref = SG.at[spot] if kind == 2 else W.at[(pl.ds(0, count),) + spot]
            remote(ref, ref, rs_send.at[kind, slot_of[k] + hop], rs_recv.at[0, 0], other).wait_send()

        for k in range(depth):
            if axes[k] == 2:
                if k < depth - 1 or kind != 1:
                    sent(k, 0, 1 - digit[k], L * NP if k == depth - 1 else number)
            else:

                @pl.when(outer[k])
                def _():
                    sent(k, 0, three[k], number)

                @pl.when(inner[k])
                def _():
                    sent(k, 1, far[k], number)
                    sent(k, 0, mine_out[k], number)

    block_shape = axes + (rp,)

    def put_gradient(index, value):
        W[index] = value.astype(BF).reshape(block_shape + (half,))
        scatter_begin(depth - 1, index, straight)

    def put_pair(index, value):
        put_gradient(index, value[:, :half])
        put_gradient(index + 1, value[:, half:])

    def column_sum(values):
        return jnp.sum(values, axis=0, keepdims=True)

    def down_gradient(layer, number):
        down = layer * NP + 4 + UP
        grad = mm(LOW[...], pair_of(down + number), NN) * SLOPE[layer, number // 2].astype(F32)
        low = (2 + number) * half
        BG[layer, :, low : low + 2 * half] = column_sum(grad)
        FL[number // 2] = grad.astype(BF)
        put_pair(down + number, mm(LOW[...], HIDDEN[layer, number // 2], TN))

    LOW[...] = cot_ref[...]
    VG[...] = jnp.zeros(VG.shape, F32)
    SG[...] = jnp.zeros(SG.shape, F32)

    def attend(layer):
        def one(item, _):
            pair = item // clips
            clip = lax.rem(item, clips)
            span = pl.ds(clip * SEQ, SEQ)
            query = Q[layer, pair, span]
            key = K[layer, pair, span]
            value = V[layer, pair, span]
            total = None
            for h, mask in enumerate(head_mask):
                scores = mm(query * mask, key, NT) * scale
                highest = jnp.max(scores, axis=1, keepdims=True)
                logsum = highest + jnp.log(jnp.sum(jnp.exp(scores - highest), axis=1, keepdims=True))
                kept = logsum if h == 0 else jnp.where(lane < h * HD, kept, logsum)
                weights = jnp.exp(scores - logsum).astype(BF)
                part = mm(weights, value * mask, NN)
                total = part if total is None else total + part
            LSE[layer, pair, span] = jnp.broadcast_to(kept, (SEQ, LANES))
            CTX[layer, pair, span] = total.astype(BF)
            return 0

        lax.fori_loop(0, plan.pairs * clips, one, 0)

    def context_of(layer, region=slice(None)):
        return jnp.concatenate([CTX[layer, pair, region] for pair in range(plan.pairs)], axis=1)

    def forward_layer(layer, carry):
        first = layer * NP
        up = first + 4
        down = up + UP

        @pl.when(layer == 0)
        def _():
            value = frames_ref[...].astype(F32)
            DX[...] = value
            norm_forward(value, layer, 0, slice(None))

        ready(first, first + 2)

        @pl.when(layer > 0)
        def _():
            for part in range(2):
                region = pl.ds(part * chunk, chunk)
                value = MID[region] + exchange_sum(2 * layer - 1, 1, part) + VEC[layer - 1, 5:6]
                DX[region] = value
                norm_forward(value, layer, 0, region)
            exchange_done(2 * layer - 1, 1)

        both = mm(ACT[layer, 0], pair_of(first), NN)
        for pair in range(plan.pairs):
            low = pair * LANES
            query = both[:, low : low + LANES] + BIAS[layer, :, low : low + LANES]
            Q[layer, pair] = query.astype(BF)
            K[layer, pair] = both[:, half + low : half + low + LANES].astype(BF)
        ready(first + 2, first + 3)
        values = mm(ACT[layer, 0], unit_of(first + 2), NN)
        for pair in range(plan.pairs):
            low = pair * LANES
            bias = BIAS[layer, :, half + low : half + low + LANES]
            V[layer, pair] = (values[:, low : low + LANES] + bias).astype(BF)
        attend(layer)
        ready(first + 3, first + 4)
        for part in range(2):
            region = pl.ds(part * chunk, chunk)
            heads = context_of(layer, region)
            exchange_send(2 * layer, 0, part, mm(heads, unit_of(first + 3), NT))
        ready(up, up + UP)
        for part in range(2):
            region = pl.ds(part * chunk, chunk)
            value = DX[region] + exchange_sum(2 * layer, 0, part) + VEC[layer, 4:5]
            MID[region] = value
            norm_forward(value, layer, 1, region)
        exchange_done(2 * layer, 0)
        for number in range(0, UP, 2):
            before = mm(ACT[layer, 1], pair_of(up + number), NN)
            low = (2 + number) * half
            before = before + BIAS[layer, :, low : low + 2 * half]
            bell = 0.5 * (1.0 + lax.erf(before * root_half))
            HIDDEN[layer, number // 2] = (before * bell).astype(BF)
            slope = bell + before * jnp.exp(-0.5 * before * before) * inv_root_two_pi
            SLOPE[layer, number // 2] = slope.astype(BF)
        for number in range(0, UP, 2):
            ready(down + number, down + number + 2)
            term = mm(HIDDEN[layer, number // 2], pair_of(down + number), NT)
            if number + 2 < UP:
                ACC[...] = term if number == 0 else ACC[...] + term
            else:
                whole = term + ACC[...] if UP > 2 else term

                @pl.when(layer + 1 < L)
                def _():
                    for part in range(2):
                        exchange_send(2 * layer + 1, 1, part, whole[part * chunk : (part + 1) * chunk])

                @pl.when(layer + 1 == L)
                def _():
                    LAST[...] = whole.astype(BF)

            @pl.when(layer + 1 == L)
            def _():
                gather_drain(1 + number // 2, late + number, 2)
                down_gradient(layer, number)

        return carry

    lax.fori_loop(0, L, forward_layer, 0)

    def attend_back(layer):
        def one(item, _):
            pair = item // clips
            clip = lax.rem(item, clips)
            span = pl.ds(clip * SEQ, SEQ)
            query = Q[layer, pair, span]
            key = K[layer, pair, span]
            value = V[layer, pair, span]
            upper = FL[1, span, pl.ds(pl.multiple_of(half + pair * LANES, LANES), LANES)]
            logsums = LSE[layer, pair, span]
            grad_q = grad_k = grad_v = None
            for h, mask in enumerate(head_mask):
                scores = mm(query * mask, key, NT) * scale
                probs = jnp.exp(scores - logsums[:, h * HD : h * HD + 1])
                weights = probs.astype(BF)
                up_head = upper * mask
                part_v = mm(weights, up_head, TN)
                grad_p = mm(up_head, value, NT)
                inner = jnp.sum(probs * grad_p, axis=1, keepdims=True)
                grad_s = (probs * (grad_p - inner) * scale).astype(BF)
                part_q = mm(grad_s, key * mask, NN)
                part_k = mm(grad_s, query * mask, TN)
                grad_q = part_q if grad_q is None else grad_q + part_q
                grad_k = part_k if grad_k is None else grad_k + part_k
                grad_v = part_v if grad_v is None else grad_v + part_v
            low = pl.ds(pl.multiple_of(pair * LANES, LANES), LANES)
            next_low = pl.ds(pl.multiple_of(half + pair * LANES, LANES), LANES)
            FL[0, span, low] = grad_q.astype(BF)
            FL[0, span, next_low] = grad_k.astype(BF)
            FL[1, span, low] = grad_v.astype(BF)
            sum_q = jnp.sum(grad_q, axis=0, keepdims=True)
            sum_v = jnp.sum(grad_v, axis=0, keepdims=True)

            @pl.when(clip == 0)
            def _():
                BG[layer, :, low] = sum_q
                BG[layer, :, next_low] = sum_v

            @pl.when(clip > 0)
            def _():
                BG[layer, :, low] += sum_q
                BG[layer, :, next_low] += sum_v

            return 0

        lax.fori_loop(0, plan.pairs * clips, one, 0)

    def norm_backward(upper, layer, which, region):
        hat = HAT[layer, which, region]
        scaled = upper * VEC[layer, 2 * which : 2 * which + 1]
        return INV[layer, which, region] * (
            masked(scaled - average(scaled)) - hat * average(scaled * hat)
        )

    def keep_rows(layer, line, part, value):
        if part == 0:
            VG[layer, line : line + 1] = value
        else:
            VG[layer, line : line + 1] += value

    DX[...] = cot_ref[...].astype(F32)
    VG[L - 1, 5:6] = column_sum(DX[...])
    DMID = ACC
    gather_drain(0, 0, late)
    gather_drain(group_of(0, True), 0, 1, True)

    def produced(m):
        turn = lax.rem(m, NP)
        name = jnp.where(
            turn < UP,
            4 + UP + turn,
            jnp.where(turn < 2 * UP, 4 + turn - UP, NP - 1 - turn),
        )
        return (L - 1 - m // NP) * NP + name

    def pumped(step, place, index):
        counts = [row[min(index - 1, len(row) - 1)] - max(0, index - len(row)) for row in PUMPS[place]]
        value = counts[0]
        for s in range(1, L):
            value = jnp.where(step == s, counts[min(s, len(counts) - 1)], value)
        return jnp.clip(value, 0, L * NP)

    def scatter_either(index, m):
        unit = produced(m)

        @pl.when(lax.rem(m, TURN_EVERY) != 0)
        def _():
            scatter_hop(index, unit, straight)

        @pl.when(lax.rem(m, TURN_EVERY) == 0)
        def _():
            scatter_hop(index, unit, turned)

    def pump_between(lows, highs):
        length = functools.reduce(jnp.maximum, [high - low for low, high in zip(lows, highs)])

        def one(t, carry):
            for index in range(1, hops):
                m = lows[index - 1] + t

                @pl.when(m < highs[index - 1])
                def _():
                    scatter_either(index, m)

            return carry

        lax.fori_loop(0, length, one, 0)

    def pump_to(step, place):
        if place == 0:
            before = [
                jnp.where(step == 0, 0, pumped(step - 1, len(PUMPS) - 1, index)) for index in range(1, hops)
            ]
        else:
            before = [pumped(step, place - 1, index) for index in range(1, hops)]
        pump_between(before, [pumped(step, place, index) for index in range(1, hops)])

    def rest_order():
        last = [row[-1] for row in PUMPS][-1]
        done = [min(last[min(index, 4) - 1], L * NP) for index in range(1, 5)]
        done += [0] * (hops - 5)
        if hops == 5 and sum(done) + len(REST) == 4 * L * NP:
            given = list(REST)
        else:
            done = [max(0, min(done[min(index, 4) - 1] - max(0, index - 4), L * NP)) for index in range(1, hops)]
            left = [(m + 2 * index, index) for index in range(1, hops) for m in range(done[index - 1], L * NP)]
            given = [index for _, index in sorted(left)]
        events = []
        for index in given:
            events.append((index, done[index - 1]))
            done[index - 1] += 1
        return events

    def named(m):
        name = m % NP
        name = 4 + UP + name if name < UP else 4 + name - UP if name < 2 * UP else NP - 1 - name
        return (L - 1 - m // NP) * NP + name, turned if m % TURN_EVERY == 0 else straight

    def pump_rest(aside):
        events = rest_order()
        for number, (index, m) in enumerate(events):
            unit, order = named(m)
            scatter_hop(index, unit, order)
            if m == L * NP - 1:
                scatter_hop(index, small_index, straight, True)
            if len(events) - 1 - number in aside:
                aside[len(events) - 1 - number]()

    def backward_layer(step, carry):
        layer = L - 1 - step
        first = layer * NP
        up = first + 4
        down = up + UP
        number_up = 2 * L + 2 * step

        def from_core(low, high):
            for n in range(low, high):
                turn = n - 4 - UP if n >= 4 + UP else n - 4 + UP if n >= 4 else NP - 1 - n
                scatter_hop(0, first + n, turned if turn % TURN_EVERY == 0 else straight)

        for part in range(2):
            from_core(4 + UP + part * UP // 2, 4 + UP + (part + 1) * UP // 2)
            region = pl.ds(part * chunk, chunk)
            whole = None
            for number in range(0, UP, 2):
                term = mm(FL[number // 2, region], pair_of(up + number), NT)
                whole = term if whole is None else whole + term
            exchange_send(number_up, 1, part, whole)
        pump_to(step, 0)
        for number in range(0, UP, 2):
            put_pair(up + number, mm(ACT[layer, 1], FL[number // 2], TN))
        from_core(4, 4 + UP)
        pump_to(step, 1)
        for part in range(2):
            region = pl.ds(part * chunk, chunk)
            grad = exchange_sum(number_up, 1, part)
            keep_rows(layer, 2, part, column_sum(grad * HAT[layer, 1, region]))
            keep_rows(layer, 3, part, column_sum(grad))
            grad_mid = DX[region] + norm_backward(grad, layer, 1, region)
            DMID[region] = grad_mid
            keep_rows(layer, 4, part, column_sum(grad_mid))
            LOW[region] = grad_mid.astype(BF)
        exchange_done(number_up, 1)
        heads = mm(LOW[...], unit_of(first + 3), NN)
        FL[1, :, half : 2 * half] = heads.astype(BF)
        put_gradient(first + 3, mm(LOW[...], context_of(layer), TN))
        pump_to(step, 2)
        attend_back(layer)
        for part in range(2):
            region = pl.ds(part * chunk, chunk)
            whole = mm(FL[0, region], pair_of(first), NT)
            whole = whole + mm(FL[1, region, 0:half], unit_of(first + 2), NT)
            exchange_send(number_up + 1, 0, part, whole)
        from_core(3, 4)
        pump_to(step, 3)
        put_gradient(first + 2, mm(ACT[layer, 0], FL[1, :, 0:half], TN))
        grad_qk = mm(ACT[layer, 0], FL[0], TN)
        put_gradient(first + 1, grad_qk[:, half:])
        put_gradient(first, grad_qk[:, :half])
        for n in (2, 1, 0):
            from_core(n, n + 1)
        pump_to(step, 4)

        @pl.when(step + 1 == L)
        def _():
            pack_biases()

        for part in range(2):
            region = pl.ds(part * chunk, chunk)
            grad = exchange_sum(number_up + 1, 0, part)
            keep_rows(layer, 0, part, column_sum(grad * HAT[layer, 0, region]))
            keep_rows(layer, 1, part, column_sum(grad))
            upper = DMID[region] + norm_backward(grad, layer, 0, region)
            DX[region] = upper
            LOW[region] = upper.astype(BF)
        exchange_done(number_up + 1, 0)

        @pl.when(step + 1 < L)
        def _():
            VG[layer - 1, 5:6] = column_sum(DX[...])
            for number in range(0, UP, 2):
                down_gradient(layer - 1, number)

        return carry

    def pack_biases():
        row = jnp.concatenate([BG[layer] for layer in range(L)], axis=1)
        wide = jnp.where(group_match(), row, 0.0)
        high = wide.astype(BF)
        low = (wide - high.astype(F32)).astype(BF)
        select = feature_match(LANES).astype(F32).astype(BF)
        table = (mm(high, select, NT) + mm(low, select, NT)).T
        for owner in range(plan.count):
            start = owner * plan.quarter
            spot = static_place(owner) + (slice(rp, rp + plan.quarter), slice(None))
            SG[spot] = table[start : start + plan.quarter]

    lax.fori_loop(0, L, backward_layer, 0)

    lines = [VG[layer] for layer in range(L)]
    lines.append(jnp.zeros((LANES - L * VEC_ROWS, Dp), F32))
    columns = jnp.concatenate(lines, axis=0).T.reshape(axes + (rp, LANES))
    SG[(slice(None),) * depth + (slice(0, rp), slice(None))] = columns
    scatter_begin(depth - 1, small_index, straight, True)
    for part in range(2):
        exchange_send(2 * L - 1, 1, part, LAST[pl.ds(part * chunk, chunk)])
    gin_copy = pltpu.make_async_copy(DX, gin_ref, go_sem.at[1])
    out_copy = pltpu.make_async_copy(OUT, out_ref, go_sem.at[2])
    gin_copy.start()
    scatter_hop(0, small_index, straight, True)

    def output():
        for part in range(2):
            region = pl.ds(part * chunk, chunk)
            value = MID[region] + exchange_sum(2 * L - 1, 1, part) + VEC[L - 1, 5:6]
            OUT[region] = value.astype(BF)
        out_copy.start()
        exchange_done(2 * L - 1, 1)
        gin_copy.wait()

    pump_rest({14: output})
    turned_number = -(-L * NP // TURN_EVERY)
    scatter_drain(0, straight, L * NP - turned_number)
    scatter_drain(1, turned, turned_number)
    scatter_drain(2, straight, 1)
    out_copy.wait()
    pltpu.make_async_copy(GO, gout_ref, go_sem.at[0]).wait()


PUMPS = (
    ((0, 0, 0, 0), (12, 8, 5, 1)),
    ((2, 0, 0, 0), (14, 9, 8, 1)),
    ((4, 1, 0, 0), (16, 11, 8, 6)),
    ((7, 3, 1, 0), (18, 13, 11, 6)),
    ((8, 5, 1, 0), (20, 14, 13, 9)),
)
REST = (
    1, 1, 2, 2, 2, 3, 4, 4, 4, 1, 2, 2, 2, 3, 3, 2, 3, 2, 3, 2, 1, 4, 4, 3,
    3, 3, 2, 3, 4, 3, 4, 4, 4, 4, 3, 4, 4, 4, 4, 4,
)


def run_kernel(plan, frames, cotangent, shards, small):
    L, NP, Dp, rp, rows = plan.layers, plan.units, plan.padded, plan.block, plan.rows
    axes = plan.axes
    depth = len(axes)
    half = plan.half
    UP = plan.ups // 2
    piece = 2 * half
    landings = []
    small_landings = []
    for k, size in enumerate(axes):
        turned_number = -(-L * NP // TURN_EVERY)
        number = NP if k == depth - 1 else L * NP - turned_number if k < 2 else L * NP
        slots = 1 if size == 2 else 5
        landings.append(pltpu.VMEM((number,) + axes[:k] + (slots, rp, half), BF))
        small_landings.append(pltpu.VMEM(axes[:k] + (slots, rp + BIAS_ROWS, LANES), F32))
    turned_landings = [
        pltpu.VMEM((-(-L * NP // TURN_EVERY), 1 if axes[0] == 2 else 5, axes[1], rp, half), BF),
        pltpu.VMEM((-(-L * NP // TURN_EVERY), 1 if axes[1] == 2 else 5, rp, half), BF),
    ]
    scratch = [
        pltpu.VMEM((L * NP,) + axes + (rp, half), BF),
        pltpu.VMEM(axes + (rp + BIAS_ROWS, LANES), BF),
        pltpu.VMEM((L, VEC_ROWS, Dp), F32),
        pltpu.VMEM((L, 1, plan.bias_cols), F32),
        pltpu.VMEM((2, rows, Dp), BF),
        pltpu.VMEM((2, rows, Dp), BF),
        pltpu.VMEM((rows, Dp), F32),
        pltpu.VMEM((rows, Dp), F32),
        pltpu.VMEM((rows, Dp), BF),
        pltpu.VMEM((L, 2, rows, Dp), F32),
        pltpu.VMEM((L, 2, rows, 1), F32),
        pltpu.VMEM((L, 2, rows, Dp), BF),
        pltpu.VMEM((L, plan.pairs, rows, LANES), BF),
        pltpu.VMEM((L, plan.pairs, rows, LANES), BF),
        pltpu.VMEM((L, plan.pairs, rows, LANES), BF),
        pltpu.VMEM((L, plan.pairs, rows, LANES), F32),
        pltpu.VMEM((L, plan.pairs, rows, LANES), BF),
        pltpu.VMEM((L, UP, rows, piece), BF),
        pltpu.VMEM((L, UP, rows, piece), BF),
        pltpu.VMEM((rows, Dp), F32),
        pltpu.VMEM((rows, Dp), BF),
        pltpu.VMEM((UP, rows, piece), BF),
        pltpu.VMEM((L, VEC_ROWS, Dp), F32),
        pltpu.VMEM((L, 1, plan.bias_cols), F32),
        pltpu.VMEM((HD, LANES), F32),
        pltpu.VMEM(axes + (rp + BIAS_ROWS, LANES), F32),
        landings,
        turned_landings,
        small_landings,
        pltpu.SemaphoreType.DMA((2 + plan.ups // 2, plan.signals + 3)),
        pltpu.SemaphoreType.DMA((L * NP + 1, plan.signals)),
        pltpu.SemaphoreType.DMA((max(plan.early, 1), 2)),
        pltpu.SemaphoreType.DMA((3, plan.signals)),
        pltpu.SemaphoreType.DMA((L * NP + 1, plan.signals)),
        pltpu.SemaphoreType.DMA((2, 2)),
        pltpu.SemaphoreType.DMA((4 * L, 2)),
        pltpu.VMEM((L * NP, rp, half), F32),
        pltpu.VMEM((rows, Dp), BF),
        pltpu.SemaphoreType.DMA((3,)),
    ]
    return pl.pallas_call(
        functools.partial(train_kernel, plan),
        out_shape=(
            jax.ShapeDtypeStruct((rows, Dp), BF),
            jax.ShapeDtypeStruct((rows, Dp), F32),
            jax.ShapeDtypeStruct((L * NP, rp, half), F32),
            jax.ShapeDtypeStruct((rp + BIAS_ROWS, LANES), F32),
        ),
        in_specs=[pl.BlockSpec(memory_space=pltpu.VMEM)] * 4,
        out_specs=tuple([pl.BlockSpec(memory_space=pl.ANY)] * 3 + [pl.BlockSpec(memory_space=pltpu.VMEM)]),
        scratch_shapes=scratch,
        compiler_params=pltpu.CompilerParams(
            collective_id=0, has_side_effects=True, vmem_limit_bytes=67043328
        ),
        name="train_step",
    )(frames, cotangent, shards, small)


def adamw(weight, gradient, first, second, rate, decay):
    first_new = beta_one * first + (1.0 - beta_one) * gradient
    second_new = beta_two * second + (1.0 - beta_two) * gradient * gradient
    first_hat = first_new / (1.0 - beta_one**STEP)
    second_hat = second_new / (1.0 - beta_two**STEP)
    weight_new = weight - rate * (first_hat / (jnp.sqrt(second_hat) + adam_eps) + decay * weight)
    return (weight_new, first_new, second_new)


def pad_axis(values, axis, size):
    widths = [(0, 0)] * values.ndim
    widths[axis] = (0, size - values.shape[axis])
    return jnp.pad(values, widths)


def on_device(count, frames, cotangent, *tensors):
    masters, firsts, seconds = tensors[:7], tensors[7:14], tensors[14:21]
    w_qkv, w_out, w_up, w_down, b_qv, b_up, vectors = masters
    L = w_qkv.shape[0]
    rows, width = frames.shape
    half = w_qkv.shape[3]
    hidden = w_up.shape[2]
    plan = Plan(count, rows, width, half, hidden, L)
    own, rp, UP = plan.own, plan.block, plan.ups

    def spread_features(values):
        if rp == own:
            return values
        return pad_axis(values.reshape(rows, count, own), 2, rp).reshape(rows, plan.padded)

    def gather_features(values):
        if rp == own:
            return values
        return values.reshape(rows, count, rp)[:, :, :own].reshape(rows, width)

    low_qkv = w_qkv.astype(BF).reshape(L, own, 3 * half)
    low_out = w_out.astype(BF).transpose(0, 2, 1)
    low_up = w_up.astype(BF)
    low_down = w_down.astype(BF).transpose(0, 2, 1)
    parts = [low_qkv[:, :, n * half : (n + 1) * half] for n in range(3)] + [low_out]
    parts += [low_up[:, :, n * half : (n + 1) * half] for n in range(UP)]
    parts += [low_down[:, :, n * half : (n + 1) * half] for n in range(UP)]
    shards = jnp.stack(parts, axis=1).reshape(L * plan.units, own, half)
    shards = pad_axis(shards, 1, rp)

    quarter = plan.quarter
    vec_part = pad_axis(vectors.astype(BF).transpose(2, 0, 1), 2, VEC_ROWS).reshape(own, L * VEC_ROWS)
    bias_part = jnp.concatenate(
        [b_qv.astype(BF).reshape(L, -1, quarter), b_up.astype(BF).reshape(L, -1, quarter)], axis=1
    )
    groups = bias_part.shape[1]
    bias_part = bias_part.transpose(2, 0, 1).reshape(quarter, L * groups)
    small = jnp.concatenate(
        [
            pad_axis(pad_axis(vec_part, 1, LANES), 0, rp),
            pad_axis(pad_axis(bias_part, 1, LANES), 0, BIAS_ROWS),
        ],
        axis=0,
    )

    output, grad_input, wide, small_grad = run_kernel(
        plan, spread_features(frames), spread_features(cotangent), shards, small
    )

    wide = wide.reshape(L, plan.units, rp, half)[:, :, :own]
    grad_qkv = jnp.stack([wide[:, n] for n in range(3)], axis=2)
    grad_out = wide[:, 3].transpose(0, 2, 1)
    grad_up = jnp.concatenate([wide[:, 4 + n] for n in range(UP)], axis=2)
    grad_down = jnp.concatenate([wide[:, 4 + UP + n] for n in range(UP)], axis=2).transpose(0, 2, 1)
    vec_grad = small_grad[:own, : L * VEC_ROWS].reshape(own, L, VEC_ROWS)[:, :, : vectors.shape[1]]
    grad_vec = vec_grad.transpose(1, 2, 0)
    bias_grad = small_grad[rp : rp + quarter, : L * groups].reshape(quarter, L, groups)
    bias_grad = bias_grad.transpose(1, 2, 0)
    split = b_qv.shape[1] * b_qv.shape[2]
    grad_bqv = bias_grad[:, :split].reshape(b_qv.shape)
    grad_bup = bias_grad[:, split:]
    grads = (grad_qkv, grad_out, grad_up, grad_down, grad_bqv, grad_bup, grad_vec)
    rates = (rate_matrix,) * 4 + (rate_vector,) * 3
    decays = (decay_rate,) * 4 + (0.0,) * 3
    updated = [
        adamw(masters[n], grads[n], firsts[n], seconds[n], rates[n], decays[n]) for n in range(7)
    ]
    return (
        (gather_features(output), gather_features(grad_input))
        + grads
        + tuple(updated[n][0] for n in range(7))
        + tuple(updated[n][1] for n in range(7))
        + tuple(updated[n][2] for n in range(7))
    )


def solution(mesh):
    tensors = (
        P(None, "fsdp", None, "tp"),
        P(None, "tp", "fsdp"),
        P(None, "fsdp", "tp"),
        P(None, "tp", "fsdp"),
        P(None, None, "tp", "fsdp"),
        P(None, "tp", "fsdp"),
        P(None, None, "fsdp"),
    )
    rows = (P("fsdp", None), P("fsdp", None))
    return jax.shard_map(
        functools.partial(on_device, mesh.shape["fsdp"]),
        mesh=mesh,
        in_specs=rows + tensors * 3,
        out_specs=rows + tensors * 4,
        check_vma=False,
    )
```
